32 devices in a mesh: grp: 4 (over z), pen: 8 (over y, x, core).
Axes of the slice: x: 2, y: 2, z: 4, core: 2. Of those that a mesh axis runs over, the one named last changes fastest.
Arguments:
- cell_offsets: int32 [2, 1048576], P(None, ('grp', 'pen')), may hold values from 0 to 1
- cell_z: int32 [1048576], P(('grp', 'pen')), may hold values from 0 to 255
- frac: float32 [3, 1048576], P(None, ('grp', 'pen')), may hold values from 0 to 1
- charges: float32 [1048576], P(('grp', 'pen')), may hold values from -4 to 4
- tile_counts: int32 [16384], P(('grp', 'pen')), may hold values from 16 to 64, as said below
Outputs:
- forces: float32 [3, 1048576], P(None, ('grp', 'pen'))
- energy: float32 [], replicated
The draws below stay inside these ranges and needn't reach their ends.
Inputs may be any that keep to these rules, and one draw needn't show every extreme that they name: `tile_counts`: live slots of each tile; some tile holds 64.
All inputs are finite; a program needn't handle non-finite values.
Results may differ from the reference program's by a relative error of at most 0.0003.
Values sent between devices are 32-bit elements; how exact they have to be, the bound alone decides.
A program may use at most 256 MiB of HBM per device.

```python
import math
import jax
import jax.numpy as jnp
from jax import lax

KX = 256
KY = 256
KZ = 256
SLOTS = 64
TILES = 16384
ATOMS = 1048576
N_GRP = 4
N_PEN = 8


def draw_tile_counts(key, part):
    counts = jax.random.randint(key, (TILES,), max(1, SLOTS // 4), SLOTS + 1)
    filled = jax.random.randint(jax.random.fold_in(key, 7), (), 0, TILES)
    return counts.at[filled].set(SLOTS).astype(jnp.int32)


def place_ends(drawn, key, low, top_value):
    dims = drawn.shape
    spot = [jax.random.randint(jax.random.fold_in(key, axis), (), 0, dims[axis]) for axis in range(len(dims))]
    drawn = drawn.at[tuple(spot)].set(low)
    longest = dims.index(max(dims))
    spot[longest] = (spot[longest] + 1) % dims[longest]
    return drawn.at[tuple(spot)].set(top_value)


def steps_of(own_key, shape, cuts, least, high):
    gain, own = 1.0, jax.random.fold_in(own_key, 6)
    for axis_at, shards_of in cuts:
        steps = jnp.exp(jax.random.uniform(jax.random.fold_in(own, axis_at), (shards_of,), jnp.float32, least / len(cuts), high / len(cuts)))
        gain = gain * jnp.repeat(steps, shape[axis_at] // shards_of).reshape([-1 if axis == axis_at else 1 for axis in range(len(shape))])
    return gain


def scatter_about(stream_key, shape, width, limit, shards=(), kind=jnp.bfloat16):
    array = jax.random.normal(stream_key, shape, jnp.float32) * width
    if len(shards) > 0:
        array = steps_of(stream_key, shape, shards, -0.22, 0.18) * array
    return jnp.clip(array, min=-limit, max=limit).astype(kind)


def setup_inputs(seed: int = 0) -> dict:
    arg_keys = jax.random.split(jax.random.key(seed), 6)
    return {
        "cell_offsets": place_ends(jax.random.randint(arg_keys[0], (2, ATOMS), 0, 2), jax.random.fold_in(arg_keys[0], 1), 0, 1).astype(jnp.int32),
        "cell_z": place_ends(jax.random.randint(arg_keys[1], (ATOMS,), 0, KZ), jax.random.fold_in(arg_keys[1], 1), 0, KZ - 1).astype(jnp.int32),
        "frac": jnp.clip(1.0 * jax.random.uniform(arg_keys[2], (3, ATOMS), jnp.float32) ** steps_of(arg_keys[2], (3, ATOMS), ((1, 32),), -0.2, 0.2), 0.0, 1.0),
        "charges": scatter_about(arg_keys[3], (ATOMS,), 1.0, 4.0, ((0, 32),), jnp.float32),
        "tile_counts": draw_tile_counts(jax.random.fold_in(arg_keys[5], 71), 0),
    }


ewald_split = 0.6


def spline_rows(fracs):
    values = [jnp.ones_like(fracs)]
    fifth = values
    for order in range(2, 7):
        nxt = []
        for j in range(order):
            term = jnp.zeros_like(fracs)
            if j >= 1:
                term = term + values[j - 1] * (fracs + order - 1 - j)
            if j <= order - 2:
                term = term + values[j] * (1.0 - fracs + j)
            nxt.append(term / (order - 1))
        if order == 5:
            fifth = nxt
        values = nxt
    slopes = []
    for j in range(6):
        term = jnp.zeros_like(fracs)
        if j >= 1:
            term = term + fifth[j - 1]
        if j <= 4:
            term = term - fifth[j]
        slopes.append(term)
    return values, slopes


def tile_weights(offsets, zcell, fracs, charge, counts, size_z):
    slots = charge.shape[-1]
    live = (jnp.arange(slots, dtype=jnp.int32) < counts[..., None]).astype(jnp.float32)
    live_q = charge * live
    theta_x, slope_x = spline_rows(fracs[0])
    theta_y, slope_y = spline_rows(fracs[1])
    theta_z, slope_z = spline_rows(fracs[2])
    footing = jnp.arange(8, dtype=jnp.int32)[:, None]
    cells = jnp.arange(size_z, dtype=jnp.int32)
    weight_x = 0.0
    grade_x = 0.0
    weight_y = 0.0
    grade_y = 0.0
    weight_z = 0.0
    grade_z = 0.0
    for j in range(6):
        hit_x = (footing == offsets[0][..., None, :] + j).astype(jnp.float32)
        hit_y = (footing == offsets[1][..., None, :] + j).astype(jnp.float32)
        hit_z = (cells == (zcell[..., :, None] + j) % size_z).astype(jnp.float32)
        weight_x = weight_x + theta_x[j][..., None, :] * hit_x
        grade_x = grade_x + slope_x[j][..., None, :] * hit_x
        weight_y = weight_y + theta_y[j][..., None, :] * hit_y
        grade_y = grade_y + slope_y[j][..., None, :] * hit_y
        weight_z = weight_z + theta_z[j][..., :, None] * hit_z
        grade_z = grade_z + slope_z[j][..., :, None] * hit_z
    return weight_x, grade_x, weight_y, grade_y, weight_z, grade_z, live_q


def modulus(index, length):
    coeffs = (1.0 / 120.0, 26.0 / 120.0, 66.0 / 120.0, 26.0 / 120.0, 1.0 / 120.0)
    real_part = 0.0
    imag_part = 0.0
    for j in range(5):
        angle = ((index * j) % length).astype(jnp.float32) * (2.0 * math.pi / length)
        real_part = real_part + coeffs[j] * jnp.cos(angle)
        imag_part = imag_part + coeffs[j] * jnp.sin(angle)
    return real_part * real_part + imag_part * imag_part


def influence(index_x, index_y, index_z):
    freq_x = jnp.where(2 * index_x < KX, index_x, index_x - KX).astype(jnp.float32) / KX
    freq_y = jnp.where(2 * index_y < KY, index_y, index_y - KY).astype(jnp.float32) / KY
    freq_z = jnp.where(2 * index_z < KZ, index_z, index_z - KZ).astype(jnp.float32) / KZ
    square = freq_x * freq_x + freq_y * freq_y + freq_z * freq_z
    safe = jnp.where(square > 0, square, 1.0)
    volume = float(KX * KY * KZ)
    value = jnp.exp(-(math.pi ** 2) * safe / (ewald_split ** 2)) / (math.pi * volume * safe)
    value = value / (modulus(index_x, KX) * modulus(index_y, KY) * modulus(index_z, KZ))
    return jnp.where(square > 0, value, 0.0)


def reference(cell_offsets, cell_z, frac, charges, tile_counts):
    tiles_x = KX // N_GRP // 2
    tiles_y = KY // N_PEN // 2
    rows_x = KX // 2
    rows_y = KY // 2
    highest = lax.Precision.HIGHEST

    def arrange(arr):
        lead = arr.shape[:-1]
        count = len(lead)
        shaped = arr.reshape(lead + (N_GRP, N_PEN, tiles_x, tiles_y, SLOTS))
        order = tuple(range(count)) + (count, count + 2, count + 1, count + 3, count + 4)
        return jnp.transpose(shaped, order).reshape(lead + (rows_x, rows_y, SLOTS))

    offsets = jnp.moveaxis(arrange(cell_offsets), 1, 0)
    fracs = jnp.moveaxis(arrange(frac), 1, 0)
    zcell = arrange(cell_z)
    charge = arrange(charges)
    counts = jnp.transpose(tile_counts.reshape(N_GRP, N_PEN, tiles_x, tiles_y), (0, 2, 1, 3)).reshape(rows_x, rows_y)
    row_ids = jnp.arange(rows_x, dtype=jnp.int32)
    eight = jnp.arange(8, dtype=jnp.int32)

    def spread_row(grid, inputs):
        offs, zrow, frow, qrow, crow, row = inputs
        weight_x, grade_x, weight_y, grade_y, weight_z, grade_z, live_q = tile_weights(offs, zrow, frow, qrow, crow, KZ)
        pair = (weight_x[:, :, None, :] * weight_y[:, None, :, :] * live_q[:, None, None, :]).reshape(rows_y, 64, SLOTS)
        spread = jnp.einsum("tfs,tsz->tfz", pair, weight_z, precision=highest).reshape(rows_y, 8, 4, 2, KZ)
        slab = 0.0
        for j in range(4):
            part = jnp.transpose(spread[:, :, j], (1, 0, 2, 3))
            slab = slab + jnp.roll(part, j, axis=1).reshape(8, KY, KZ)
        targets = (2 * row + eight) % KX
        return grid.at[targets].add(slab), None

    start = jnp.zeros((KX, KY, KZ), jnp.float32)
    charge_mesh, _ = lax.scan(spread_row, start, (offsets, zcell, fracs, charge, counts, row_ids))
    spectrum = jnp.fft.fftn(charge_mesh)
    index_x = jnp.arange(KX, dtype=jnp.int32)[:, None, None]
    index_y = jnp.arange(KY, dtype=jnp.int32)[None, :, None]
    index_z = jnp.arange(KZ, dtype=jnp.int32)[None, None, :]
    kernel = influence(index_x, index_y, index_z)
    power = jnp.real(spectrum) ** 2 + jnp.imag(spectrum) ** 2
    energy = 0.5 * jnp.sum(kernel * power)
    potential = jnp.real(jnp.fft.ifftn(kernel * spectrum)) * float(KX * KY * KZ)

    def interp_row(carry, inputs):
        offs, zrow, frow, qrow, crow, row = inputs
        weight_x, grade_x, weight_y, grade_y, weight_z, grade_z, live_q = tile_weights(offs, zrow, frow, qrow, crow, KZ)
        rows = jnp.take(potential, (2 * row + eight) % KX, axis=0)
        parts = []
        for j in range(4):
            parts.append(jnp.roll(rows, -2 * j, axis=1).reshape(8, rows_y, 2, KZ))
        footing = jnp.transpose(jnp.stack(parts, axis=0), (2, 1, 0, 3, 4)).reshape(rows_y, 64, KZ)
        main = jnp.einsum("tfz,tsz->tfs", footing, weight_z, precision=highest).reshape(rows_y, 8, 8, SLOTS)
        tilt = jnp.einsum("tfz,tsz->tfs", footing, grade_z, precision=highest).reshape(rows_y, 8, 8, SLOTS)
        force_x = -live_q * jnp.einsum("txs,tys,txys->ts", grade_x, weight_y, main, precision=highest)
        force_y = -live_q * jnp.einsum("txs,tys,txys->ts", weight_x, grade_y, main, precision=highest)
        force_z = -live_q * jnp.einsum("txs,tys,txys->ts", weight_x, weight_y, tilt, precision=highest)
        return carry, jnp.stack([force_x, force_y, force_z], axis=0)

    _, stacked = lax.scan(interp_row, 0.0, (offsets, zcell, fracs, charge, counts, row_ids))
    forces = stacked.reshape(N_GRP, tiles_x, 3, N_PEN, tiles_y, SLOTS)
    forces = jnp.transpose(forces, (2, 0, 3, 1, 4, 5)).reshape(3, ATOMS)
    return forces, (energy / ATOMS).astype(jnp.float32)
```

```python
import functools
import math

import jax
import jax.numpy as jnp
import numpy as np
from jax import lax
from jax.experimental import pallas as pl
from jax.experimental.pallas import tpu as pltpu
from jax.sharding import PartitionSpec as P

KX = 256
KY = 256
KZ = 256
ATOMS = 1048576


ewald_split = 0.6
highest = lax.Precision.HIGH


def shifted(block, axis, distance):
    devices = range(lax.axis_size(axis))
    route = [((i - distance) % len(devices), i) for i in devices]
    return lax.ppermute(block, axis, route)


def spline_rows(fracs):
    values = [jnp.ones_like(fracs)]
    fifth = values
    for order in range(2, 7):
        nxt = []
        for j in range(order):
            term = jnp.zeros_like(fracs)
            if j >= 1:
                term = values[j - 1] * (fracs + order - 1 - j)
            if j <= order - 2:
                term = term + values[j] * (1.0 - fracs + j)
            nxt.append(term / (order - 1))
        if order == 5:
            fifth = nxt
        values = nxt
    slopes = []
    for j in range(6):
        term = jnp.zeros_like(fracs)
        if j >= 1:
            term = fifth[j - 1]
        if j <= 4:
            term = term - fifth[j]
        slopes.append(term)
    return (values, slopes)


def select_rows(distance, values):
    total = jnp.zeros(distance.shape, jnp.float32)
    for j in range(6):
        total = jnp.where(distance == j, values[j], total)
    return total


def select_pair(distance, values, grades):
    total = jnp.zeros(distance.shape, jnp.float32)
    slope = jnp.zeros(distance.shape, jnp.float32)
    for j in range(6):
        hit = distance == j
        total = jnp.where(hit, values[j], total)
        slope = jnp.where(hit, grades[j], slope)
    return (total, slope)


def split(values):
    high = values.astype(jnp.bfloat16)
    low = (values - high.astype(jnp.float32)).astype(jnp.bfloat16)
    return (high, low)


def product(high, low, other, dims):
    other_high, other_low = split(other)
    rows = high.shape[0]
    both = lax.dot_general(
        jnp.concatenate([high, low], axis=0), other_high, dims, preferred_element_type=jnp.float32
    )
    rest = lax.dot_general(high, other_low, dims, preferred_element_type=jnp.float32)
    return both[:rows] + both[rows:] + rest


def row_of(values, i):
    return [value[i : i + 1] for value in values]


def y_offset(offset, slots):
    lane = lax.broadcasted_iota(jnp.int32, offset.shape, 1)
    return offset + 2 * (lane // slots)


def spread_kernel(per_row, slots, off_ref, z_ref, frac_ref, q_ref, grid_ref):
    width = z_ref.shape[1]
    size_z = grid_ref.shape[2]
    grid_ref[...] = jnp.zeros_like(grid_ref)

    def step(outer, carry):
        rows = pl.ds(pl.multiple_of(outer * 8, 8), 8)
        theta_x, _ = spline_rows(frac_ref[0, rows, :])
        theta_y, _ = spline_rows(frac_ref[1, rows, :])
        theta_z, _ = spline_rows(frac_ref[2, rows, :])
        charge = q_ref[rows, :]
        theta_x = [theta * charge for theta in theta_x]
        off_x = off_ref[0, rows, :]
        off_y = y_offset(off_ref[1, rows, :], slots)
        base = z_ref[rows, :]
        eight = lax.broadcasted_iota(jnp.int32, (8, width), 0)
        sixteen = lax.broadcasted_iota(jnp.int32, (16, width), 0)
        cells = lax.broadcasted_iota(jnp.int32, (size_z, width), 0)
        for i in range(8):
            weight_x = select_rows(eight - off_x[i : i + 1], row_of(theta_x, i))
            weight_y = select_rows(sixteen - off_y[i : i + 1], row_of(theta_y, i))
            weight_z = select_rows(
                (cells - base[i : i + 1]) & (size_z - 1), row_of(theta_z, i)
            )
            pair = jnp.concatenate([weight_x[k : k + 1] * weight_y for k in range(8)], axis=0)
            high, low = split(pair)
            out = product(high, low, weight_z, (((1,), (1,)), ((), ())))
            first = 2 * (outer * (8 // per_row) + i // per_row)
            y0 = 8 * (i % per_row)
            for k in range(8):
                grid_ref[first + k, y0 : y0 + 16, :] += out[16 * k : 16 * k + 16]
        return carry

    lax.fori_loop(0, z_ref.shape[0] // 8, step, 0)


def interp_kernel(
    per_row, slots, off_ref, z_ref, frac_ref, q_ref, pot_ref, up_ref, side_ref, out_ref, ext_ref
):
    width = z_ref.shape[1]
    size_z = pot_ref.shape[2]
    block_x, block_y = pot_ref.shape[0], pot_ref.shape[1]
    ext_ref[:block_x, :block_y] = pot_ref[...]
    ext_ref[block_x : block_x + 5, :block_y] = up_ref[...]
    ext_ref[block_x + 5 :, :block_y] = jnp.zeros((3, block_y, size_z), jnp.float32)
    ext_ref[: block_x + 5, block_y:] = side_ref[...]
    ext_ref[block_x + 5 :, block_y:] = jnp.zeros((3, 8, size_z), jnp.float32)

    def step(outer, carry):
        rows = pl.ds(pl.multiple_of(outer * 8, 8), 8)
        theta_x, slope_x = spline_rows(frac_ref[0, rows, :])
        theta_y, slope_y = spline_rows(frac_ref[1, rows, :])
        theta_z, slope_z = spline_rows(frac_ref[2, rows, :])
        off_x = off_ref[0, rows, :]
        off_y = y_offset(off_ref[1, rows, :], slots)
        base = z_ref[rows, :]
        eight = lax.broadcasted_iota(jnp.int32, (8, width), 0)
        sixteen = lax.broadcasted_iota(jnp.int32, (16, width), 0)
        cells = lax.broadcasted_iota(jnp.int32, (size_z, width), 0)
        dims = (((1,), (0,)), ((), ()))
        forces = [[], [], []]
        for i in range(8):
            weight_x, grade_x = select_pair(
                eight - off_x[i : i + 1], row_of(theta_x, i), row_of(slope_x, i)
            )
            weight_y, grade_y = select_pair(
                sixteen - off_y[i : i + 1], row_of(theta_y, i), row_of(slope_y, i)
            )
            weight_z, grade_z = select_pair(
                (cells - base[i : i + 1]) & (size_z - 1), row_of(theta_z, i), row_of(slope_z, i)
            )
            first = 2 * (outer * (8 // per_row) + i // per_row)
            y0 = 8 * (i % per_row)
            footing = jnp.concatenate(
                [ext_ref[first + k, y0 : y0 + 16, :] for k in range(8)], axis=0
            )
            high, low = split(footing)
            main = product(high, low, weight_z, dims)
            tilt = product(high, low, grade_z, dims)
            along_x = 0.0
            along_y = 0.0
            along_z = 0.0
            for k in range(8):
                piece = main[16 * k : 16 * k + 16]
                along_x = along_x + grade_x[k : k + 1] * piece
                along_y = along_y + weight_x[k : k + 1] * piece
                along_z = along_z + weight_x[k : k + 1] * tilt[16 * k : 16 * k + 16]
            forces[0].append(jnp.sum(along_x * weight_y, axis=0, keepdims=True))
            forces[1].append(jnp.sum(along_y * grade_y, axis=0, keepdims=True))
            forces[2].append(jnp.sum(along_z * weight_y, axis=0, keepdims=True))
        minus_q = -q_ref[rows, :]
        for d in range(3):
            out_ref[d, rows, :] = minus_q * jnp.concatenate(forces[d], axis=0)
        return carry

    lax.fori_loop(0, z_ref.shape[0] // 8, step, 0)


def modulus(index, length):
    coeffs = (1.0 / 120.0, 26.0 / 120.0, 66.0 / 120.0, 26.0 / 120.0, 1.0 / 120.0)
    real_part = 0.0
    imag_part = 0.0
    for j in range(5):
        angle = (index * j % length).astype(jnp.float32) * (2.0 * math.pi / length)
        real_part = real_part + coeffs[j] * jnp.cos(angle)
        imag_part = imag_part + coeffs[j] * jnp.sin(angle)
    return real_part * real_part + imag_part * imag_part


def influence(index_x, index_y, index_z):
    freq_x = jnp.where(2 * index_x < KX, index_x, index_x - KX).astype(jnp.float32) / KX
    freq_y = jnp.where(2 * index_y < KY, index_y, index_y - KY).astype(jnp.float32) / KY
    freq_z = jnp.where(2 * index_z < KZ, index_z, index_z - KZ).astype(jnp.float32) / KZ
    square = freq_x * freq_x + freq_y * freq_y + freq_z * freq_z
    safe = jnp.where(square > 0, square, 1.0)
    volume = float(KX * KY * KZ)
    value = jnp.exp(-math.pi**2 * safe / ewald_split**2) / (math.pi * volume * safe)
    value = value / (modulus(index_x, KX) * modulus(index_y, KY) * modulus(index_z, KZ))
    return jnp.where(square > 0, value, 0.0)


def waves(index, length):
    angle = (index % length) * (2.0 * math.pi / length)
    return (np.cos(angle), np.sin(angle))


def z_table(groups):
    planes = KZ // (2 * groups)
    frequency = np.arange(KZ // 2).reshape(groups, planes)
    cos, sin = waves(frequency[..., None] * np.arange(KZ), KZ)
    table = np.stack([cos, -sin], axis=1)
    table[0, 1, 0] = waves(np.arange(KZ) * (KZ // 2), KZ)[0]
    weight = np.full((groups, 2, planes), 2.0)
    weight[0, :, 0] = 1.0
    table = table.reshape(KZ, KZ)
    return (table.astype(np.float32), (table * weight.reshape(KZ, 1)).astype(np.float32))


def block_table(frequency, length, groups):
    position = np.arange(length)
    cos, sin = waves(frequency[..., None] * position, length)
    shape = (frequency.shape[0], frequency.shape[1], groups, length // groups)
    cos, sin = cos.reshape(shape), sin.reshape(shape)
    real_row = np.stack([cos, sin], axis=3)
    imag_row = np.stack([-sin, cos], axis=3)
    table = np.stack([real_row, imag_row], axis=1)
    return table.reshape(2 * length, 2 * length).astype(np.float32)


def y_frequency(groups):
    first = np.arange(KY // 2).reshape(groups, -1)
    second = np.where(first == 0, KY // 2, (KY - first) % KY)
    return np.concatenate([first, second], axis=1)


def partner_of(me, d, count):
    if count & (count - 1):
        return lax.rem(me + d, count)
    peer = me
    bit = 1
    while bit < count:
        if d & bit:
            peer = peer + bit - 2 * bit * lax.rem(lax.div(me, bit), 2)
        bit = 2 * bit
    return peer


def exchange_kernel(axis, count, *refs):
    arrays = (len(refs) - 3) // 2
    sources, targets = refs[:arrays], refs[arrays : 2 * arrays]
    send_sem, recv_sem, own_sem = refs[2 * arrays :]
    me = lax.axis_index(axis)
    barrier = pltpu.get_barrier_semaphore()
    for d in range(1, count):
        pl.semaphore_signal(
            barrier,
            inc=1,
            device_id={axis: partner_of(me, d, count)},
            device_id_type=pl.DeviceIdType.MESH,
        )
    pl.semaphore_wait(barrier, count - 1)
    copies = []
    for k in range(arrays):
        for d in range(1, count):
            peer = partner_of(me, d, count)
            copies.append(
                pltpu.make_async_remote_copy(
                    src_ref=sources[k].at[peer],
                    dst_ref=targets[k].at[me],
                    send_sem=send_sem.at[k, d],
                    recv_sem=recv_sem.at[k, d],
                    device_id={axis: peer},
                    device_id_type=pl.DeviceIdType.MESH,
                )
            )
        copies.append(
            pltpu.make_async_copy(sources[k].at[me], targets[k].at[me], own_sem.at[k])
        )
    for copy in copies:
        copy.start()
    for copy in copies:
        copy.wait()


def exchange(arrays, axis, number):
    count = lax.axis_size(axis)
    vmem = pl.BlockSpec(memory_space=pltpu.VMEM)
    return pl.pallas_call(
        functools.partial(exchange_kernel, axis, count),
        out_shape=[jax.ShapeDtypeStruct(array.shape, array.dtype) for array in arrays],
        in_specs=[vmem] * len(arrays),
        out_specs=[vmem] * len(arrays),
        scratch_shapes=[
            pltpu.SemaphoreType.DMA((len(arrays), count)),
            pltpu.SemaphoreType.DMA((len(arrays), count)),
            pltpu.SemaphoreType.DMA((len(arrays),)),
        ],
        compiler_params=pltpu.CompilerParams(collective_id=number, has_side_effects=True),
        name="exchange" + str(number),
    )(*arrays)


def dot(left, right, left_dim, right_dim):
    dims = (((left_dim,), (right_dim,)), ((), ()))
    return lax.dot_general(
        left, right, dims, precision=highest, preferred_element_type=jnp.float32
    )


def spectrum_of(grid, block_x, block_y):
    grp, pen = lax.axis_size("grp"), lax.axis_size("pen")
    planes = KZ // (2 * pen)
    lines = KY // grp
    half = lines // 2
    forward_z, backward_z = z_table(pen)
    order_y = y_frequency(grp)
    table_y = block_table(order_y, KY, pen)
    table_x = block_table(np.arange(KX)[None], KX, grp)
    lines_z = dot(forward_z, grid.reshape(block_x * block_y, KZ), 1, 1)
    lines_z = lines_z.reshape(pen, 2, planes, block_x, block_y).transpose(0, 1, 4, 2, 3)
    (columns,) = exchange(
        [lines_z.reshape(pen, 2 * block_y, planes * block_x)], "pen", 1
    )
    lines_y = dot(table_y, columns.reshape(2 * KY, planes * block_x), 1, 0)
    lines_y = lines_y.reshape(grp, 2, lines, planes, block_x).transpose(0, 1, 4, 3, 2)
    (rows,) = exchange([lines_y.reshape(grp, 2 * block_x, planes * lines)], "grp", 2)
    rows = rows.reshape(grp, 2, block_x, planes * lines)
    at_grp, at_pen = lax.axis_index("grp"), lax.axis_index("pen")
    packed = rows[..., :lines]
    alone = (at_grp == 0) & (jnp.arange(lines) % half == 0)
    partner = jnp.where(
        alone, packed, jnp.concatenate([packed[..., half:], packed[..., :half]], axis=-1)
    )
    a, b = packed[:, :1], packed[:, 1:]
    c, d = partner[:, :1], partner[:, 1:]
    whole = jnp.concatenate([a + c, b - d], axis=1) * 0.5
    midway = jnp.concatenate([b + d, c - a], axis=1) * 0.5
    origin = at_pen == 0
    whole = jnp.where(origin, whole, packed)
    midway = jnp.where(origin, midway, 0.0)
    total_lanes = (planes + 1) * lines
    full = jnp.concatenate([whole, rows[..., lines:], midway], axis=-1)
    spectrum = dot(table_x, full.reshape(2 * KX, total_lanes), 1, 0)
    spectrum = spectrum.reshape(2, KX, total_lanes)
    index_x = jnp.arange(KX, dtype=jnp.int32)[:, None]
    slot = jnp.arange(planes + 1, dtype=jnp.int32)
    index_z = jnp.where(slot < planes, at_pen * planes + slot, KZ // 2)
    plane_weight = jnp.where(
        slot < planes,
        jnp.where(origin & (slot == 0), 1.0, 2.0),
        jnp.where(origin, 1.0, 0.0),
    )
    index_z = jnp.repeat(index_z, lines)[None, :]
    plane_weight = jnp.repeat(plane_weight, lines)[None, :]
    index_y = lax.dynamic_index_in_dim(jnp.asarray(order_y, jnp.int32), at_grp, 0, False)
    index_y = jnp.tile(index_y, planes + 1)[None, :]
    kernel = influence(index_x, index_y, index_z)
    power = spectrum[0] * spectrum[0] + spectrum[1] * spectrum[1]
    spectral = 0.5 * jnp.sum(plane_weight * kernel * power)
    scaled = (spectrum * kernel).reshape(2 * KX, total_lanes)
    returning = dot(table_x, scaled, 0, 0).reshape(grp, 2, block_x, total_lanes)
    midway = returning[..., planes * lines :]
    turned = jnp.concatenate([-midway[:, 1:], midway[:, :1]], axis=1)
    returning = jnp.concatenate(
        [returning[..., :lines] + turned, returning[..., lines : planes * lines]], axis=-1
    )
    rows, sums = exchange(
        [
            returning.reshape(grp, 2 * block_x, planes * lines),
            jnp.broadcast_to(spectral, (grp, 8, 128)),
        ],
        "grp",
        3,
    )
    spectral = jnp.sum(sums[:, 0, 0])
    rows = rows.reshape(grp, 2, block_x, planes, lines).transpose(0, 1, 4, 3, 2)
    columns = dot(table_y, rows.reshape(2 * KY, planes * block_x), 0, 0)
    columns, sums = exchange(
        [
            columns.reshape(pen, 2 * block_y, planes * block_x),
            jnp.broadcast_to(spectral, (pen, 8, 128)),
        ],
        "pen",
        4,
    )
    spectral = jnp.sum(sums[:, 0, 0])
    home = columns.reshape(pen, 2, block_y, planes, block_x).transpose(0, 1, 3, 4, 2)
    potential = dot(home.reshape(KZ, block_x * block_y), backward_z, 0, 0)
    return (potential.reshape(block_x, block_y, KZ), spectral)


def cas_table(length):
    position = np.arange(length)
    cos, sin = waves(position[:, None] * position, length)
    return cos + sin


def halves(table):
    high = table.astype(jnp.bfloat16)
    low = (table - high.astype(np.float64)).astype(jnp.bfloat16)
    return (high, low)


def spline_factor(length):
    index = np.arange(length)
    freq = np.where(2 * index < length, index, index - length) / length
    coeffs = np.array([1.0, 26.0, 66.0, 26.0, 1.0]) / 120.0
    phase = np.exp(2j * np.pi * index[:, None] * np.arange(5) / length)
    modulus_square = np.abs(phase @ coeffs) ** 2
    square = freq**2
    factor = np.exp(-(math.pi**2) * square / ewald_split**2) / modulus_square
    return (factor.astype(np.float32), square.astype(np.float32))


def dot3(left, right, left_dim, right_dim):
    dims = (((left_dim,), (right_dim,)), ((), ()))
    one = functools.partial(
        lax.dot_general, dimension_numbers=dims, preferred_element_type=jnp.float32
    )
    return one(left[0], right[0]) + one(left[0], right[1]) + one(left[1], right[0])


def regroup(tiles, width):
    lane = lax.broadcasted_iota(jnp.int32, tiles[0].shape, 1) // width
    bit = 1
    while bit < len(tiles):
        keep = (lane // bit) % 2 == 0
        mixed = list(tiles)
        for i in range(len(tiles)):
            if not i & bit:
                first, second = tiles[i], tiles[i + bit]
                mixed[i] = jnp.where(keep, first, pltpu.roll(second, bit * width, 1))
                mixed[i + bit] = jnp.where(
                    keep, pltpu.roll(first, 128 - bit * width, 1), second
                )
        tiles = mixed
        bit = 2 * bit
    return tiles


def slab_kernel(
    grp, pen, grid_ref, cas_hi, cas_lo, into_hi, into_lo, back_hi, back_lo,
    factor_row, factor_col, square_row, square_col, pot_ref, energy_ref,
    send, recv, send_back, recv_back, work, sums, part,
    send_sem, recv_sem, back_send_sem, back_recv_sem, sum_send_sem, sum_recv_sem,
):
    count = grp * pen
    block_x, block_y = grid_ref.shape[0], grid_ref.shape[1]
    fan = 128 // block_y
    tiles = block_x // fan
    half = pen // fan
    at_grp, at_pen = lax.axis_index("grp"), lax.axis_index("pen")
    me = at_grp * pen + at_pen

    def peer_of(d):
        peer = partner_of(me, d, count)
        return (peer, {"grp": peer // pen, "pen": peer % pen})

    barrier = pltpu.get_barrier_semaphore()
    for d in range(1, count):
        pl.semaphore_signal(
            barrier, inc=1, device_id=peer_of(d)[1], device_id_type=pl.DeviceIdType.MESH
        )
    cas = (cas_hi[...], cas_lo[...])

    def along_z(i, carry):
        rows = grid_ref[pl.ds(2 * fan * i, 2 * fan)].reshape(256, KZ)
        out = dot3(cas, split(rows), 1, 1)
        for t in range(2):
            send[:, 2 * i + t] = out[:, 128 * t : 128 * t + 128].reshape(count, 8, 128)
        return carry

    lax.fori_loop(0, tiles // 2, along_z, 0)
    pl.semaphore_wait(barrier, count - 1)

    def copy_of(d, source, target, sems):
        peer, where = peer_of(d)
        return pltpu.make_async_remote_copy(
            src_ref=source(peer),
            dst_ref=target.at[me],
            send_sem=sems[0].at[d],
            recv_sem=sems[1].at[d],
            device_id=where,
            device_id_type=pl.DeviceIdType.MESH,
        )

    out_copies = {
        d: copy_of(d, lambda p: send.at[p], recv, (send_sem, recv_sem))
        for d in range(1, count)
    }
    for d in reversed(range(1, count)):
        out_copies[d].start()
    recv[me] = send[me]

    def along_y(t):
        g = partner_of(at_grp, t, grp)
        groups = [[] for _ in range(fan)]
        for h in range(half):
            loaded = [
                recv[g * pen + h * fan + k].reshape(8 * tiles, 128) for k in range(fan)
            ]
            for k, tile in enumerate(regroup(loaded, block_y)):
                groups[k].append(tile)
        for k in range(fan):
            rows = jnp.concatenate(groups[k], axis=1)
            out = dot3(split(rows), cas, 1, 0)
            start = pl.multiple_of((g * fan + k) * 8 * tiles, 128)
            for h in range(2):
                work[pl.ds(start + h * 8 * KX, 8 * tiles), :] = out[:, 128 * h : 128 * h + 128]

    for t in range(grp):
        for e in range(pen):
            if t * pen + e:
                out_copies[t * pen + e].wait_recv()
        along_y(t)

    scale = 1.0 / (math.pi * KX * KY * KZ)
    first = pl.multiple_of(8 * me, 8)
    factor_z = factor_col[pl.ds(first, 8), :]
    square_z = square_col[pl.ds(first, 8), :]
    pick = lax.broadcasted_iota(jnp.int32, (8, 1), 0)

    def along_x(f, total):
        fz = jnp.sum(jnp.where(pick == f, factor_z, 0.0), axis=0, keepdims=True) * scale
        sz = jnp.sum(jnp.where(pick == f, square_z, 0.0), axis=0, keepdims=True)
        rows = jnp.concatenate(
            [work[pl.ds(f + h * 8 * KX, KX, stride=8), :] for h in range(2)], axis=1
        )
        spectrum = dot3((into_hi[...], into_lo[...]), split(rows), 1, 0)
        square = square_col[...] + (square_row[...] + sz)
        safe = jnp.where(square > 0, square, 1.0)
        kernel = factor_col[...] * (factor_row[...] * fz) / safe
        kernel = jnp.where(square > 0, kernel, 0.0)
        scaled = kernel * spectrum
        total = total + jnp.sum(scaled * spectrum, axis=0, keepdims=True)
        out = dot3((back_hi[...], back_lo[...]), split(scaled), 1, 0)
        for h in range(2):
            work[pl.ds(f + h * 8 * KX, KX, stride=8), :] = out[:, 128 * h : 128 * h + 128]
        return total

    total = lax.fori_loop(0, 8, along_x, jnp.zeros((1, KY), jnp.float32))
    part[...] = jnp.broadcast_to(0.5 * jnp.sum(total, axis=1, keepdims=True), (1, 128))
    sums[me] = part[...]

    back_copies = {
        d: copy_of(d, lambda p: send_back.at[p], recv_back, (back_send_sem, back_recv_sem))
        for d in range(1, count)
    }
    sum_copies = {
        d: copy_of(d, lambda p: part, sums, (sum_send_sem, sum_recv_sem))
        for d in range(1, count)
    }
    for t in reversed(range(grp)):
        g = partner_of(at_grp, t, grp)
        groups = [[] for _ in range(half)]
        for k in range(fan):
            start = pl.multiple_of((g * fan + k) * 8 * tiles, 128)
            rows = jnp.concatenate(
                [work[pl.ds(start + h * 8 * KX, 8 * tiles), :] for h in range(2)], axis=1
            )
            out = dot3(split(rows), cas, 1, 0)
            for h in range(half):
                groups[h].append(out[:, 128 * h : 128 * h + 128])
        for h in range(half):
            for k, tile in enumerate(regroup(groups[h], block_y)):
                send_back[g * pen + h * fan + k] = tile.reshape(tiles, 8, 128)
        for e in reversed(range(pen)):
            if t * pen + e:
                back_copies[t * pen + e].start()
    for d in range(1, count):
        sum_copies[d].start()
    recv_back[me] = send_back[me]
    for d in range(1, count):
        back_copies[d].wait_recv()

    def home_z(i, carry):
        rows = jnp.concatenate(
            [recv_back[:, 2 * i + t].reshape(KZ, 128) for t in range(2)], axis=1
        )
        out = dot3(split(jnp.transpose(rows)), cas, 1, 0)
        pot_ref[pl.ds(2 * fan * i, 2 * fan)] = out.reshape(2 * fan, block_y, KZ)
        return carry

    lax.fori_loop(0, tiles // 2, home_z, 0)
    for d in range(1, count):
        sum_copies[d].wait_recv()
    energy_ref[...] = jnp.sum(sums[...], axis=0)
    for d in range(1, count):
        out_copies[d].wait_send()
        back_copies[d].wait_send()
        sum_copies[d].wait_send()


def slab_potential(grid, grp, pen):
    count = grp * pen
    block_x, block_y = grid.shape[0], grid.shape[1]
    fan = 128 // block_y
    tiles = block_x // fan
    cas = cas_table(KZ)
    order = np.arange(KX).reshape(grp, tiles, fan).transpose(0, 2, 1).reshape(KX)
    factor, square = spline_factor(KX)
    tables = [*halves(cas), *halves(cas[:, order]), *halves(cas[order, :])]
    tables += [factor[None, :], factor[:, None], square[None, :], square[:, None]]
    tables = [jnp.asarray(table) for table in tables]
    vmem = pl.BlockSpec(memory_space=pltpu.VMEM)
    blocks = pltpu.VMEM((count, tiles, 8, 128), jnp.float32)
    potential, energy = pl.pallas_call(
        functools.partial(slab_kernel, grp, pen),
        out_shape=[
            jax.ShapeDtypeStruct(grid.shape, jnp.float32),
            jax.ShapeDtypeStruct((1, 128), jnp.float32),
        ],
        in_specs=[vmem] * (1 + len(tables)),
        out_specs=[vmem] * 2,
        scratch_shapes=[
            blocks, blocks, blocks, blocks,
            pltpu.VMEM((16 * KX, 128), jnp.float32),
            pltpu.VMEM((count, 1, 128), jnp.float32),
            pltpu.VMEM((1, 128), jnp.float32),
        ] + [pltpu.SemaphoreType.DMA((count,))] * 6,
        compiler_params=pltpu.CompilerParams(
            collective_id=1, has_side_effects=True, vmem_limit_bytes=60 * 1024 * 1024
        ),
        name="slab",
    )(grid, *tables)
    return (potential, energy[0, 0])


def slab_fits(grp, pen, block_x, block_y):
    fan = 128 // block_y
    return (
        grp * pen * 8 == KZ and KX == KY and KY == KZ and pen % fan == 0
        and block_x % (2 * fan) == 0 and KZ == 256
    )


def local(cell_offsets, cell_z, frac, charges, tile_counts):
    block_x = KX // lax.axis_size("grp")
    block_y = KY // lax.axis_size("pen")
    tiles = tile_counts.shape[0]
    slots = charges.shape[0] // tiles
    width = 4 * slots
    groups = tiles // 4
    per_row = block_y // 8
    live = jnp.arange(slots, dtype=jnp.int32)[None, :] < tile_counts[:, None]
    live_q = (charges.reshape(tiles, slots) * live.astype(jnp.float32)).reshape(groups, width)
    offsets = cell_offsets.reshape(2, groups, width)
    zcell = cell_z.reshape(groups, width)
    fracs = frac.reshape(3, groups, width)
    vmem = pl.BlockSpec(memory_space=pltpu.VMEM)
    params = pltpu.CompilerParams(vmem_limit_bytes=60 * 1024 * 1024)
    padded = pl.pallas_call(
        functools.partial(spread_kernel, per_row, slots),
        out_shape=jax.ShapeDtypeStruct((block_x + 8, block_y + 8, KZ), jnp.float32),
        in_specs=[vmem] * 4,
        out_specs=vmem,
        compiler_params=params,
        name="spread",
    )(offsets, zcell, fracs, live_q)
    rim_y = shifted(padded[: block_x + 5, block_y : block_y + 5], "pen", 1)
    merged = padded[: block_x + 5, :block_y].at[:, :5].add(rim_y)
    rim_x = shifted(merged[block_x : block_x + 5], "grp", 1)
    grid = merged[:block_x] + jnp.pad(rim_x, ((0, block_x - 5), (0, 0), (0, 0)))
    grp, pen = lax.axis_size("grp"), lax.axis_size("pen")
    if slab_fits(grp, pen, block_x, block_y):
        potential, total = slab_potential(grid, grp, pen)
    else:
        potential, total = spectrum_of(grid, block_x, block_y)
    upper = shifted(potential[:5], "grp", -1)
    ext_x = jnp.concatenate([potential[:, :5], upper[:, :5]], axis=0)
    beside = shifted(ext_x, "pen", -1)
    beside = jnp.pad(beside, ((0, 0), (0, 3), (0, 0)))
    forces = pl.pallas_call(
        functools.partial(interp_kernel, per_row, slots),
        out_shape=jax.ShapeDtypeStruct((3, groups, width), jnp.float32),
        in_specs=[vmem] * 7,
        out_specs=vmem,
        scratch_shapes=[pltpu.VMEM((block_x + 8, block_y + 8, KZ), jnp.float32)],
        compiler_params=params,
        name="interp",
    )(offsets, zcell, fracs, live_q, potential, upper, beside)
    return (forces.reshape(3, groups * width), total / ATOMS)


def solution(mesh):
    in_specs = (
        P(None, ("grp", "pen")),
        P(("grp", "pen")),
        P(None, ("grp", "pen")),
        P(("grp", "pen")),
        P(("grp", "pen")),
    )
    out_specs = (P(None, ("grp", "pen")), P())
    return jax.shard_map(local, mesh=mesh, in_specs=in_specs, out_specs=out_specs, check_vma=False)
```

```python
import functools
import math

import jax
import jax.numpy as jnp
import numpy as np
from jax import lax
from jax.experimental import pallas as pl
from jax.experimental.pallas import tpu as pltpu
from jax.sharding import PartitionSpec as P

KX = 256
KY = 256
KZ = 256
ATOMS = 1048576


ewald_split = 0.6
highest = lax.Precision.HIGH


def shifted(block, axis, distance):
    devices = range(lax.axis_size(axis))
    route = [((i - distance) % len(devices), i) for i in devices]
    return lax.ppermute(block, axis, route)


def spline_rows(fracs):
    values = [jnp.ones_like(fracs)]
    fifth = values
    for order in range(2, 7):
        nxt = []
        for j in range(order):
            term = jnp.zeros_like(fracs)
            if j >= 1:
                term = values[j - 1] * (fracs + order - 1 - j)
            if j <= order - 2:
                term = term + values[j] * (1.0 - fracs + j)
            nxt.append(term / (order - 1))
        if order == 5:
            fifth = nxt
        values = nxt
    slopes = []
    for j in range(6):
        term = jnp.zeros_like(fracs)
        if j >= 1:
            term = fifth[j - 1]
        if j <= 4:
            term = term - fifth[j]
        slopes.append(term)
    return (values, slopes)


def split(values):
    high = values.astype(jnp.bfloat16)
    low = (values - high.astype(jnp.float32)).astype(jnp.bfloat16)
    return (high, low)


def shift_rows(values, offset):
    none = jnp.zeros_like(values[0])
    return [
        jnp.where(offset == 0, first, second)
        for first, second in zip(values + [none], [none] + values)
    ]


def store_weights(outer, slots, off_ref, frac_ref, charge, x_ref, y_ref, z_ref, which):
    groups, width = off_ref.shape[1], off_ref.shape[2]
    rows = pl.ds(pl.multiple_of(outer * 8, 8), 8)
    lane_tile = lax.broadcasted_iota(jnp.int32, (8, width), 1) // slots
    along_x = spline_rows(frac_ref[0, rows, :])[which]
    along_y = spline_rows(frac_ref[1, rows, :])[which]
    along_z = spline_rows(frac_ref[2, rows, :])[which]
    if charge is not None:
        along_x = [value * charge for value in along_x]
    for k, value in enumerate(shift_rows(along_x, off_ref[0, rows, :])):
        x_ref[k, rows, :] = value
    for k, value in enumerate(along_z):
        z_ref[k, rows, :] = value
    near = shift_rows(along_y, off_ref[1, rows, :])
    none = jnp.zeros_like(near[0])
    for r in range(16):
        value = none
        for tile in range(4):
            if 0 <= r - 2 * tile < 7:
                value = jnp.where(lane_tile == tile, near[r - 2 * tile], value)
        for h in range(width // 128):
            start = (h * groups + outer * 8) * 16 + r
            y_ref[pl.ds(start, 8, stride=16), :] = value[:, 128 * h : 128 * h + 128]


def rows_of_y(y_ref, group, groups, width):
    parts = []
    for h in range(width // 128):
        start = pl.multiple_of((h * groups + group) * 16, 16)
        parts.append(y_ref[pl.ds(start, 16), :])
    return jnp.concatenate(parts, axis=1)


def z_window(base, values):
    fine = lax.broadcasted_iota(jnp.int32, (32, base.shape[1]), 0) - (base & 15)
    total = jnp.zeros(fine.shape, jnp.float32)
    for j in range(6):
        total = jnp.where(fine == j, values[j], total)
    return split(total)


def z_masks(base):
    coarse = jnp.broadcast_to(base // 16, (16, base.shape[1])).astype(jnp.int16)
    return [coarse == jnp.int16(k) for k in range(16)]


def z_weights(masks, window):
    halves_of = []
    for part in window:
        lower, upper = part[:16], part[16:]
        none = jnp.zeros_like(lower)
        blocks = []
        for k in range(16):
            block = jnp.where(masks[k - 1], upper, none)
            blocks.append(jnp.where(masks[k], lower, block))
        halves_of.append(jnp.concatenate(blocks, axis=0))
    return halves_of


def dot3(left, right, left_dim, right_dim):
    dims = (((left_dim,), (right_dim,)), ((), ()))
    one = functools.partial(
        lax.dot_general, dimension_numbers=dims, preferred_element_type=jnp.float32
    )
    return one(left[0], right[0]) + one(left[0], right[1]) + one(left[1], right[0])


def spread_row(a, per_row, cell_ref, x_ref, y_ref, z_ref, grid_ref):
    groups, width = cell_ref.shape
    outs = []
    for b in range(per_row):
        group = a * per_row + b
        base = cell_ref[pl.ds(group, 1), :]
        values = [z_ref[j, pl.ds(group, 1), :] for j in range(6)]
        weights = z_weights(z_masks(base), z_window(base, values))
        along_y = rows_of_y(y_ref, group, groups, width)
        pair = [x_ref[k, pl.ds(group, 1), :] * along_y for k in range(7)]
        outs.append(dot3(split(jnp.concatenate(pair, axis=0)), weights, 1, 1))
    for k in range(7):
        for t in range(per_row + 1):
            value = 0.0
            if t < per_row:
                value = outs[t][16 * k : 16 * k + 8]
            if t >= 1:
                value = value + outs[t - 1][16 * k + 8 : 16 * k + 16]
            grid_ref[2 * a + k, 8 * t : 8 * t + 8, :] += value


def interp_row(a, per_row, cell_ref, q_ref, plain, slope, ext_ref, out_ref):
    groups, width = cell_ref.shape
    for b in range(per_row):
        group = a * per_row + b
        row = pl.ds(group, 1)
        base = cell_ref[row, :]
        masks = z_masks(base)
        footing = jnp.concatenate(
            [ext_ref[2 * a + k, 8 * b : 8 * b + 16, :] for k in range(7)], axis=0
        )
        footing = split(footing)
        both = []
        for refs in (plain, slope):
            window = z_window(base, [refs[2][j, row, :] for j in range(6)])
            both.append(dot3(footing, z_weights(masks, window), 1, 0))
        main, tilt = both
        along_x = 0.0
        along_y = 0.0
        along_z = 0.0
        for k in range(7):
            weight, grade = plain[0][k, row, :], slope[0][k, row, :]
            piece = main[16 * k : 16 * k + 16]
            along_x = along_x + grade * piece
            along_y = along_y + weight * piece
            along_z = along_z + weight * tilt[16 * k : 16 * k + 16]
        weight_y = rows_of_y(plain[1], group, groups, width)
        grade_y = rows_of_y(slope[1], group, groups, width)
        minus_q = -q_ref[row, :]
        pieces = (along_x * weight_y, along_y * grade_y, along_z * weight_y)
        for d, piece in enumerate(pieces):
            out_ref[d, row, :] = minus_q * jnp.sum(piece, axis=0, keepdims=True)


def weight_scratch(groups, width):
    return [
        pltpu.VMEM((7, groups, width), jnp.float32),
        pltpu.VMEM((groups * 16 * (width // 128), 128), jnp.float32),
        pltpu.VMEM((6, groups, width), jnp.float32),
    ]


def spread_kernel(per_row, slots, off_ref, z_ref, frac_ref, q_ref, grid_ref, *weights):
    grid_ref[...] = jnp.zeros_like(grid_ref)
    groups = z_ref.shape[0]

    def prepare(outer, carry):
        rows = pl.ds(pl.multiple_of(outer * 8, 8), 8)
        store_weights(outer, slots, off_ref, frac_ref, q_ref[rows, :], *weights, 0)
        return carry

    def step(a, carry):
        spread_row(a, per_row, z_ref, *weights, grid_ref)
        return carry

    lax.fori_loop(0, groups // 8, prepare, 0)
    lax.fori_loop(0, groups // per_row, step, 0)


def interp_kernel(
    per_row, slots, off_ref, z_ref, frac_ref, q_ref, pot_ref, up_ref, side_ref, out_ref,
    ext_ref, *weights
):
    groups = z_ref.shape[0]
    size_z = pot_ref.shape[2]
    block_x, block_y = pot_ref.shape[0], pot_ref.shape[1]
    ext_ref[:block_x, :block_y] = pot_ref[...]
    ext_ref[block_x : block_x + 5, :block_y] = up_ref[...]
    ext_ref[block_x + 5 :, :block_y] = jnp.zeros((3, block_y, size_z), jnp.float32)
    ext_ref[: block_x + 5, block_y:] = side_ref[...]
    ext_ref[block_x + 5 :, block_y:] = jnp.zeros((3, 8, size_z), jnp.float32)

    def prepare(outer, carry):
        store_weights(outer, slots, off_ref, frac_ref, None, *weights[:3], 0)
        store_weights(outer, slots, off_ref, frac_ref, None, *weights[3:], 1)
        return carry

    def step(a, carry):
        interp_row(a, per_row, z_ref, q_ref, weights[:3], weights[3:], ext_ref, out_ref)
        return carry

    lax.fori_loop(0, groups // 8, prepare, 0)
    lax.fori_loop(0, groups // per_row, step, 0)


def modulus(index, length):
    coeffs = (1.0 / 120.0, 26.0 / 120.0, 66.0 / 120.0, 26.0 / 120.0, 1.0 / 120.0)
    real_part = 0.0
    imag_part = 0.0
    for j in range(5):
        angle = (index * j % length).astype(jnp.float32) * (2.0 * math.pi / length)
        real_part = real_part + coeffs[j] * jnp.cos(angle)
        imag_part = imag_part + coeffs[j] * jnp.sin(angle)
    return real_part * real_part + imag_part * imag_part


def influence(index_x, index_y, index_z):
    freq_x = jnp.where(2 * index_x < KX, index_x, index_x - KX).astype(jnp.float32) / KX
    freq_y = jnp.where(2 * index_y < KY, index_y, index_y - KY).astype(jnp.float32) / KY
    freq_z = jnp.where(2 * index_z < KZ, index_z, index_z - KZ).astype(jnp.float32) / KZ
    square = freq_x * freq_x + freq_y * freq_y + freq_z * freq_z
    safe = jnp.where(square > 0, square, 1.0)
    volume = float(KX * KY * KZ)
    value = jnp.exp(-math.pi**2 * safe / ewald_split**2) / (math.pi * volume * safe)
    value = value / (modulus(index_x, KX) * modulus(index_y, KY) * modulus(index_z, KZ))
    return jnp.where(square > 0, value, 0.0)


def waves(index, length):
    angle = (index % length) * (2.0 * math.pi / length)
    return (np.cos(angle), np.sin(angle))


def z_table(groups):
    planes = KZ // (2 * groups)
    frequency = np.arange(KZ // 2).reshape(groups, planes)
    cos, sin = waves(frequency[..., None] * np.arange(KZ), KZ)
    table = np.stack([cos, -sin], axis=1)
    table[0, 1, 0] = waves(np.arange(KZ) * (KZ // 2), KZ)[0]
    weight = np.full((groups, 2, planes), 2.0)
    weight[0, :, 0] = 1.0
    table = table.reshape(KZ, KZ)
    return (table.astype(np.float32), (table * weight.reshape(KZ, 1)).astype(np.float32))


def block_table(frequency, length, groups):
    position = np.arange(length)
    cos, sin = waves(frequency[..., None] * position, length)
    shape = (frequency.shape[0], frequency.shape[1], groups, length // groups)
    cos, sin = cos.reshape(shape), sin.reshape(shape)
    real_row = np.stack([cos, sin], axis=3)
    imag_row = np.stack([-sin, cos], axis=3)
    table = np.stack([real_row, imag_row], axis=1)
    return table.reshape(2 * length, 2 * length).astype(np.float32)


def y_frequency(groups):
    first = np.arange(KY // 2).reshape(groups, -1)
    second = np.where(first == 0, KY // 2, (KY - first) % KY)
    return np.concatenate([first, second], axis=1)


def partner_of(me, d, count):
    if count & (count - 1):
        return lax.rem(me + d, count)
    peer = me
    bit = 1
    while bit < count:
        if d & bit:
            peer = peer + bit - 2 * bit * lax.rem(lax.div(me, bit), 2)
        bit = 2 * bit
    return peer


def exchange_kernel(axis, count, *refs):
    arrays = (len(refs) - 3) // 2
    sources, targets = refs[:arrays], refs[arrays : 2 * arrays]
    send_sem, recv_sem, own_sem = refs[2 * arrays :]
    me = lax.axis_index(axis)
    barrier = pltpu.get_barrier_semaphore()
    for d in range(1, count):
        pl.semaphore_signal(
            barrier,
            inc=1,
            device_id={axis: partner_of(me, d, count)},
            device_id_type=pl.DeviceIdType.MESH,
        )
    pl.semaphore_wait(barrier, count - 1)
    copies = []
    for k in range(arrays):
        for d in range(1, count):
            peer = partner_of(me, d, count)
            copies.append(
                pltpu.make_async_remote_copy(
                    src_ref=sources[k].at[peer],
                    dst_ref=targets[k].at[me],
                    send_sem=send_sem.at[k, d],
                    recv_sem=recv_sem.at[k, d],
                    device_id={axis: peer},
                    device_id_type=pl.DeviceIdType.MESH,
                )
            )
        copies.append(
            pltpu.make_async_copy(sources[k].at[me], targets[k].at[me], own_sem.at[k])
        )
    for copy in copies:
        copy.start()
    for copy in copies:
        copy.wait()


def exchange(arrays, axis, number):
    count = lax.axis_size(axis)
    vmem = pl.BlockSpec(memory_space=pltpu.VMEM)
    return pl.pallas_call(
        functools.partial(exchange_kernel, axis, count),
        out_shape=[jax.ShapeDtypeStruct(array.shape, array.dtype) for array in arrays],
        in_specs=[vmem] * len(arrays),
        out_specs=[vmem] * len(arrays),
        scratch_shapes=[
            pltpu.SemaphoreType.DMA((len(arrays), count)),
            pltpu.SemaphoreType.DMA((len(arrays), count)),
            pltpu.SemaphoreType.DMA((len(arrays),)),
        ],
        compiler_params=pltpu.CompilerParams(collective_id=number, has_side_effects=True),
        name="exchange" + str(number),
    )(*arrays)


def dot(left, right, left_dim, right_dim):
    dims = (((left_dim,), (right_dim,)), ((), ()))
    return lax.dot_general(
        left, right, dims, precision=highest, preferred_element_type=jnp.float32
    )


def spectrum_of(grid, block_x, block_y):
    grp, pen = lax.axis_size("grp"), lax.axis_size("pen")
    planes = KZ // (2 * pen)
    lines = KY // grp
    half = lines // 2
    forward_z, backward_z = z_table(pen)
    order_y = y_frequency(grp)
    table_y = block_table(order_y, KY, pen)
    table_x = block_table(np.arange(KX)[None], KX, grp)
    lines_z = dot(forward_z, grid.reshape(block_x * block_y, KZ), 1, 1)
    lines_z = lines_z.reshape(pen, 2, planes, block_x, block_y).transpose(0, 1, 4, 2, 3)
    (columns,) = exchange(
        [lines_z.reshape(pen, 2 * block_y, planes * block_x)], "pen", 1
    )
    lines_y = dot(table_y, columns.reshape(2 * KY, planes * block_x), 1, 0)
    lines_y = lines_y.reshape(grp, 2, lines, planes, block_x).transpose(0, 1, 4, 3, 2)
    (rows,) = exchange([lines_y.reshape(grp, 2 * block_x, planes * lines)], "grp", 2)
    rows = rows.reshape(grp, 2, block_x, planes * lines)
    at_grp, at_pen = lax.axis_index("grp"), lax.axis_index("pen")
    packed = rows[..., :lines]
    alone = (at_grp == 0) & (jnp.arange(lines) % half == 0)
    partner = jnp.where(
        alone, packed, jnp.concatenate([packed[..., half:], packed[..., :half]], axis=-1)
    )
    a, b = packed[:, :1], packed[:, 1:]
    c, d = partner[:, :1], partner[:, 1:]
    whole = jnp.concatenate([a + c, b - d], axis=1) * 0.5
    midway = jnp.concatenate([b + d, c - a], axis=1) * 0.5
    origin = at_pen == 0
    whole = jnp.where(origin, whole, packed)
    midway = jnp.where(origin, midway, 0.0)
    total_lanes = (planes + 1) * lines
    full = jnp.concatenate([whole, rows[..., lines:], midway], axis=-1)
    spectrum = dot(table_x, full.reshape(2 * KX, total_lanes), 1, 0)
    spectrum = spectrum.reshape(2, KX, total_lanes)
    index_x = jnp.arange(KX, dtype=jnp.int32)[:, None]
    slot = jnp.arange(planes + 1, dtype=jnp.int32)
    index_z = jnp.where(slot < planes, at_pen * planes + slot, KZ // 2)
    plane_weight = jnp.where(
        slot < planes,
        jnp.where(origin & (slot == 0), 1.0, 2.0),
        jnp.where(origin, 1.0, 0.0),
    )
    index_z = jnp.repeat(index_z, lines)[None, :]
    plane_weight = jnp.repeat(plane_weight, lines)[None, :]
    index_y = lax.dynamic_index_in_dim(jnp.asarray(order_y, jnp.int32), at_grp, 0, False)
    index_y = jnp.tile(index_y, planes + 1)[None, :]
    kernel = influence(index_x, index_y, index_z)
    power = spectrum[0] * spectrum[0] + spectrum[1] * spectrum[1]
    spectral = 0.5 * jnp.sum(plane_weight * kernel * power)
    scaled = (spectrum * kernel).reshape(2 * KX, total_lanes)
    returning = dot(table_x, scaled, 0, 0).reshape(grp, 2, block_x, total_lanes)
    midway = returning[..., planes * lines :]
    turned = jnp.concatenate([-midway[:, 1:], midway[:, :1]], axis=1)
    returning = jnp.concatenate(
        [returning[..., :lines] + turned, returning[..., lines : planes * lines]], axis=-1
    )
    rows, sums = exchange(
        [
            returning.reshape(grp, 2 * block_x, planes * lines),
            jnp.broadcast_to(spectral, (grp, 8, 128)),
        ],
        "grp",
        3,
    )
    spectral = jnp.sum(sums[:, 0, 0])
    rows = rows.reshape(grp, 2, block_x, planes, lines).transpose(0, 1, 4, 3, 2)
    columns = dot(table_y, rows.reshape(2 * KY, planes * block_x), 0, 0)
    columns, sums = exchange(
        [
            columns.reshape(pen, 2 * block_y, planes * block_x),
            jnp.broadcast_to(spectral, (pen, 8, 128)),
        ],
        "pen",
        4,
    )
    spectral = jnp.sum(sums[:, 0, 0])
    home = columns.reshape(pen, 2, block_y, planes, block_x).transpose(0, 1, 3, 4, 2)
    potential = dot(home.reshape(KZ, block_x * block_y), backward_z, 0, 0)
    return (potential.reshape(block_x, block_y, KZ), spectral)


def cas_table(length):
    position = np.arange(length)
    cos, sin = waves(position[:, None] * position, length)
    return cos + sin


def halves(table):
    high = table.astype(jnp.bfloat16)
    low = (table - high.astype(np.float64)).astype(jnp.bfloat16)
    return (high, low)


def spline_factor(length):
    index = np.arange(length)
    freq = np.where(2 * index < length, index, index - length) / length
    coeffs = np.array([1.0, 26.0, 66.0, 26.0, 1.0]) / 120.0
    phase = np.exp(2j * np.pi * index[:, None] * np.arange(5) / length)
    modulus_square = np.abs(phase @ coeffs) ** 2
    square = freq**2
    factor = np.exp(-(math.pi**2) * square / ewald_split**2) / modulus_square
    return (factor.astype(np.float32), square.astype(np.float32))


def regroup(tiles, width):
    lane = lax.broadcasted_iota(jnp.int32, tiles[0].shape, 1) // width
    bit = 1
    while bit < len(tiles):
        keep = (lane // bit) % 2 == 0
        mixed = list(tiles)
        for i in range(len(tiles)):
            if not i & bit:
                first, second = tiles[i], tiles[i + bit]
                mixed[i] = jnp.where(keep, first, pltpu.roll(second, bit * width, 1))
                mixed[i + bit] = jnp.where(
                    keep, pltpu.roll(first, 128 - bit * width, 1), second
                )
        tiles = mixed
        bit = 2 * bit
    return tiles


def slab_kernel(
    grp, pen, grid_ref, cas_hi, cas_lo, into_hi, into_lo, back_hi, back_lo,
    factor_row, factor_col, square_row, square_col, pot_ref, energy_ref,
    send, recv, send_back, recv_back, work, sums, part,
    send_sem, recv_sem, back_send_sem, back_recv_sem, sum_send_sem, sum_recv_sem,
):
    count = grp * pen
    block_x, block_y = grid_ref.shape[0], grid_ref.shape[1]
    fan = 128 // block_y
    tiles = block_x // fan
    half = pen // fan
    at_grp, at_pen = lax.axis_index("grp"), lax.axis_index("pen")
    me = at_grp * pen + at_pen

    def peer_of(d):
        peer = partner_of(me, d, count)
        return (peer, {"grp": peer // pen, "pen": peer % pen})

    barrier = pltpu.get_barrier_semaphore()
    for d in range(1, count):
        pl.semaphore_signal(
            barrier, inc=1, device_id=peer_of(d)[1], device_id_type=pl.DeviceIdType.MESH
        )
    cas = (cas_hi[...], cas_lo[...])

    def along_z(i, carry):
        rows = grid_ref[pl.ds(2 * fan * i, 2 * fan)].reshape(256, KZ)
        out = dot3(cas, split(rows), 1, 1)
        for t in range(2):
            send[:, 2 * i + t] = out[:, 128 * t : 128 * t + 128].reshape(count, 8, 128)
        return carry

    lax.fori_loop(0, tiles // 2, along_z, 0)
    pl.semaphore_wait(barrier, count - 1)

    def copy_of(d, source, target, sems):
        peer, where = peer_of(d)
        return pltpu.make_async_remote_copy(
            src_ref=source(peer),
            dst_ref=target.at[me],
            send_sem=sems[0].at[d],
            recv_sem=sems[1].at[d],
            device_id=where,
            device_id_type=pl.DeviceIdType.MESH,
        )

    out_copies = {
        d: copy_of(d, lambda p: send.at[p], recv, (send_sem, recv_sem))
        for d in range(1, count)
    }
    for d in reversed(range(1, count)):
        out_copies[d].start()
    recv[me] = send[me]

    def along_y(t):
        g = partner_of(at_grp, t, grp)
        groups = [[] for _ in range(fan)]
        for h in range(half):
            loaded = [
                recv[g * pen + h * fan + k].reshape(8 * tiles, 128) for k in range(fan)
            ]
            for k, tile in enumerate(regroup(loaded, block_y)):
                groups[k].append(tile)
        for k in range(fan):
            rows = jnp.concatenate(groups[k], axis=1)
            out = dot3(split(rows), cas, 1, 0)
            start = pl.multiple_of((g * fan + k) * 8 * tiles, 128)
            for h in range(2):
                work[pl.ds(start + h * 8 * KX, 8 * tiles), :] = out[:, 128 * h : 128 * h + 128]

    for t in range(grp):
        for e in range(pen):
            if t * pen + e:
                out_copies[t * pen + e].wait_recv()
        along_y(t)

    scale = 1.0 / (math.pi * KX * KY * KZ)
    first = pl.multiple_of(8 * me, 8)
    factor_z = factor_col[pl.ds(first, 8), :]
    square_z = square_col[pl.ds(first, 8), :]
    pick = lax.broadcasted_iota(jnp.int32, (8, 1), 0)

    def along_x(f, total):
        fz = jnp.sum(jnp.where(pick == f, factor_z, 0.0), axis=0, keepdims=True) * scale
        sz = jnp.sum(jnp.where(pick == f, square_z, 0.0), axis=0, keepdims=True)
        rows = jnp.concatenate(
            [work[pl.ds(f + h * 8 * KX, KX, stride=8), :] for h in range(2)], axis=1
        )
        spectrum = dot3((into_hi[...], into_lo[...]), split(rows), 1, 0)
        square = square_col[...] + (square_row[...] + sz)
        safe = jnp.where(square > 0, square, 1.0)
        kernel = factor_col[...] * (factor_row[...] * fz) / safe
        kernel = jnp.where(square > 0, kernel, 0.0)
        scaled = kernel * spectrum
        total = total + jnp.sum(scaled * spectrum, axis=0, keepdims=True)
        out = dot3((back_hi[...], back_lo[...]), split(scaled), 1, 0)
        for h in range(2):
            work[pl.ds(f + h * 8 * KX, KX, stride=8), :] = out[:, 128 * h : 128 * h + 128]
        return total

    total = lax.fori_loop(0, 8, along_x, jnp.zeros((1, KY), jnp.float32))
    part[...] = jnp.broadcast_to(0.5 * jnp.sum(total, axis=1, keepdims=True), (1, 128))
    sums[me] = part[...]

    back_copies = {
        d: copy_of(d, lambda p: send_back.at[p], recv_back, (back_send_sem, back_recv_sem))
        for d in range(1, count)
    }
    sum_copies = {
        d: copy_of(d, lambda p: part, sums, (sum_send_sem, sum_recv_sem))
        for d in range(1, count)
    }
    for t in reversed(range(grp)):
        g = partner_of(at_grp, t, grp)
        groups = [[] for _ in range(half)]
        for k in range(fan):
            start = pl.multiple_of((g * fan + k) * 8 * tiles, 128)
            rows = jnp.concatenate(
                [work[pl.ds(start + h * 8 * KX, 8 * tiles), :] for h in range(2)], axis=1
            )
            out = dot3(split(rows), cas, 1, 0)
            for h in range(half):
                groups[h].append(out[:, 128 * h : 128 * h + 128])
        for h in range(half):
            for k, tile in enumerate(regroup(groups[h], block_y)):
                send_back[g * pen + h * fan + k] = tile.reshape(tiles, 8, 128)
        for e in reversed(range(pen)):
            if t * pen + e:
                back_copies[t * pen + e].start()
    for d in range(1, count):
        sum_copies[d].start()
    recv_back[me] = send_back[me]
    for d in range(1, count):
        back_copies[d].wait_recv()

    def home_z(i, carry):
        rows = jnp.concatenate(
            [recv_back[:, 2 * i + t].reshape(KZ, 128) for t in range(2)], axis=1
        )
        out = dot3(split(jnp.transpose(rows)), cas, 1, 0)
        pot_ref[pl.ds(2 * fan * i, 2 * fan)] = out.reshape(2 * fan, block_y, KZ)
        return carry

    lax.fori_loop(0, tiles // 2, home_z, 0)
    for d in range(1, count):
        sum_copies[d].wait_recv()
    energy_ref[...] = jnp.sum(sums[...], axis=0)
    for d in range(1, count):
        out_copies[d].wait_send()
        back_copies[d].wait_send()
        sum_copies[d].wait_send()


def slab_potential(grid, grp, pen):
    count = grp * pen
    block_x, block_y = grid.shape[0], grid.shape[1]
    fan = 128 // block_y
    tiles = block_x // fan
    cas = cas_table(KZ)
    order = np.arange(KX).reshape(grp, tiles, fan).transpose(0, 2, 1).reshape(KX)
    factor, square = spline_factor(KX)
    tables = [*halves(cas), *halves(cas[:, order]), *halves(cas[order, :])]
    tables += [factor[None, :], factor[:, None], square[None, :], square[:, None]]
    tables = [jnp.asarray(table) for table in tables]
    vmem = pl.BlockSpec(memory_space=pltpu.VMEM)
    blocks = pltpu.VMEM((count, tiles, 8, 128), jnp.float32)
    potential, energy = pl.pallas_call(
        functools.partial(slab_kernel, grp, pen),
        out_shape=[
            jax.ShapeDtypeStruct(grid.shape, jnp.float32),
            jax.ShapeDtypeStruct((1, 128), jnp.float32),
        ],
        in_specs=[vmem] * (1 + len(tables)),
        out_specs=[vmem] * 2,
        scratch_shapes=[
            blocks, blocks, blocks, blocks,
            pltpu.VMEM((16 * KX, 128), jnp.float32),
            pltpu.VMEM((count, 1, 128), jnp.float32),
            pltpu.VMEM((1, 128), jnp.float32),
        ] + [pltpu.SemaphoreType.DMA((count,))] * 6,
        compiler_params=pltpu.CompilerParams(
            collective_id=1, has_side_effects=True, vmem_limit_bytes=60 * 1024 * 1024
        ),
        name="slab",
    )(grid, *tables)
    return (potential, energy[0, 0])


def slab_fits(grp, pen, block_x, block_y):
    fan = 128 // block_y
    return (
        grp * pen * 8 == KZ and KX == KY and KY == KZ and pen % fan == 0
        and block_x % (2 * fan) == 0 and KZ == 256
    )


def local(cell_offsets, cell_z, frac, charges, tile_counts):
    block_x = KX // lax.axis_size("grp")
    block_y = KY // lax.axis_size("pen")
    tiles = tile_counts.shape[0]
    slots = charges.shape[0] // tiles
    width = 4 * slots
    groups = tiles // 4
    per_row = block_y // 8
    live = jnp.arange(slots, dtype=jnp.int32)[None, :] < tile_counts[:, None]
    live_q = (charges.reshape(tiles, slots) * live.astype(jnp.float32)).reshape(groups, width)
    offsets = cell_offsets.reshape(2, groups, width)
    zcell = cell_z.reshape(groups, width)
    fracs = frac.reshape(3, groups, width)
    vmem = pl.BlockSpec(memory_space=pltpu.VMEM)
    params = pltpu.CompilerParams(vmem_limit_bytes=60 * 1024 * 1024)
    padded = pl.pallas_call(
        functools.partial(spread_kernel, per_row, slots),
        out_shape=jax.ShapeDtypeStruct((block_x + 8, block_y + 8, KZ), jnp.float32),
        in_specs=[vmem] * 4,
        out_specs=vmem,
        scratch_shapes=weight_scratch(groups, width),
        compiler_params=params,
        name="spread",
    )(offsets, zcell, fracs, live_q)
    rim_y = shifted(padded[: block_x + 5, block_y : block_y + 5], "pen", 1)
    merged = padded[: block_x + 5, :block_y].at[:, :5].add(rim_y)
    rim_x = shifted(merged[block_x : block_x + 5], "grp", 1)
    grid = merged[:block_x] + jnp.pad(rim_x, ((0, block_x - 5), (0, 0), (0, 0)))
    grp, pen = lax.axis_size("grp"), lax.axis_size("pen")
    if slab_fits(grp, pen, block_x, block_y):
        potential, total = slab_potential(grid, grp, pen)
    else:
        potential, total = spectrum_of(grid, block_x, block_y)
    upper = shifted(potential[:5], "grp", -1)
    ext_x = jnp.concatenate([potential[:, :5], upper[:, :5]], axis=0)
    beside = shifted(ext_x, "pen", -1)
    beside = jnp.pad(beside, ((0, 0), (0, 3), (0, 0)))
    forces = pl.pallas_call(
        functools.partial(interp_kernel, per_row, slots),
        out_shape=jax.ShapeDtypeStruct((3, groups, width), jnp.float32),
        in_specs=[vmem] * 7,
        out_specs=vmem,
        scratch_shapes=[pltpu.VMEM((block_x + 8, block_y + 8, KZ), jnp.float32)]
        + 2 * weight_scratch(groups, width),
        compiler_params=params,
        name="interp",
    )(offsets, zcell, fracs, live_q, potential, upper, beside)
    return (forces.reshape(3, groups * width), total / ATOMS)


def solution(mesh):
    in_specs = (
        P(None, ("grp", "pen")),
        P(("grp", "pen")),
        P(None, ("grp", "pen")),
        P(("grp", "pen")),
        P(("grp", "pen")),
    )
    out_specs = (P(None, ("grp", "pen")), P())
    return jax.shard_map(local, mesh=mesh, in_specs=in_specs, out_specs=out_specs, check_vma=False)
```

```python
import functools
import math

import jax
import jax.numpy as jnp
import numpy as np
from jax import lax
from jax.experimental import pallas as pl
from jax.experimental.pallas import tpu as pltpu
from jax.sharding import PartitionSpec as P

KX = 256
KY = 256
KZ = 256
ATOMS = 1048576


ewald_split = 0.6
highest = lax.Precision.HIGH


def shifted(block, axis, distance):
    devices = range(lax.axis_size(axis))
    route = [((i - distance) % len(devices), i) for i in devices]
    return lax.ppermute(block, axis, route)


def spline_rows(fracs):
    values = [jnp.ones_like(fracs)]
    fifth = values
    for order in range(2, 7):
        nxt = []
        for j in range(order):
            term = jnp.zeros_like(fracs)
            if j >= 1:
                term = values[j - 1] * (fracs + order - 1 - j)
            if j <= order - 2:
                term = term + values[j] * (1.0 - fracs + j)
            nxt.append(term / (order - 1))
        if order == 5:
            fifth = nxt
        values = nxt
    slopes = []
    for j in range(6):
        term = jnp.zeros_like(fracs)
        if j >= 1:
            term = fifth[j - 1]
        if j <= 4:
            term = term - fifth[j]
        slopes.append(term)
    return (values, slopes)


def split(values):
    high = values.astype(jnp.bfloat16)
    low = (values - high.astype(jnp.float32)).astype(jnp.bfloat16)
    return (high, low)


def shift_rows(values, offset):
    none = jnp.zeros_like(values[0])
    return [
        jnp.where(offset == 0, first, second)
        for first, second in zip(values + [none], [none] + values)
    ]


def store_weights(outer, slots, off_ref, frac_ref, x_ref, y_ref, z_ref, which):
    groups, width = off_ref.shape[1], off_ref.shape[2]
    rows = pl.ds(pl.multiple_of(outer * 8, 8), 8)
    lane_tile = lax.broadcasted_iota(jnp.int32, (8, width), 1) // slots
    along_x = spline_rows(frac_ref[0, rows, :])[which]
    along_y = spline_rows(frac_ref[1, rows, :])[which]
    along_z = spline_rows(frac_ref[2, rows, :])[which]
    for k, value in enumerate(shift_rows(along_x, off_ref[0, rows, :])):
        x_ref[k, rows, :] = value
    for k, value in enumerate(along_z):
        z_ref[k, rows, :] = value
    near = shift_rows(along_y, off_ref[1, rows, :])
    none = jnp.zeros_like(near[0])
    for r in range(16):
        value = none
        for tile in range(4):
            if 0 <= r - 2 * tile < 7:
                value = jnp.where(lane_tile == tile, near[r - 2 * tile], value)
        for h in range(width // 128):
            start = (h * groups + outer * 8) * 16 + r
            y_ref[pl.ds(start, 8, stride=16), :] = value[:, 128 * h : 128 * h + 128]


def rows_of_y(y_ref, group, groups, width):
    parts = []
    for h in range(width // 128):
        start = pl.multiple_of((h * groups + group) * 16, 16)
        parts.append(y_ref[pl.ds(start, 16), :])
    return jnp.concatenate(parts, axis=1)


def z_window(base, values):
    fine = lax.broadcasted_iota(jnp.int32, (32, base.shape[1]), 0) - (base & 15)
    total = jnp.zeros(fine.shape, jnp.float32)
    for j in range(6):
        total = jnp.where(fine == j, values[j], total)
    return split(total)


def z_masks(base):
    coarse = jnp.broadcast_to(base // 16, (16, base.shape[1])).astype(jnp.int16)
    return [coarse == jnp.int16(k) for k in range(16)]


def z_weights(masks, window):
    halves_of = []
    for part in window:
        lower, upper = part[:16], part[16:]
        none = jnp.zeros_like(lower)
        blocks = []
        for k in range(16):
            block = jnp.where(masks[k - 1], upper, none)
            blocks.append(jnp.where(masks[k], lower, block))
        halves_of.append(jnp.concatenate(blocks, axis=0))
    return halves_of


def dot3(left, right, left_dim, right_dim):
    dims = (((left_dim,), (right_dim,)), ((), ()))
    one = functools.partial(
        lax.dot_general, dimension_numbers=dims, preferred_element_type=jnp.float32
    )
    return one(left[0], right[0]) + one(left[0], right[1]) + one(left[1], right[0])


def spread_row(a, per_row, cell_ref, q_ref, x_ref, y_ref, z_ref, grid_ref):
    groups, width = cell_ref.shape
    outs = []
    for b in range(per_row):
        group = a * per_row + b
        base = cell_ref[pl.ds(group, 1), :]
        values = [z_ref[j, pl.ds(group, 1), :] for j in range(6)]
        weights = z_weights(z_masks(base), z_window(base, values))
        along_y = rows_of_y(y_ref, group, groups, width) * q_ref[pl.ds(group, 1), :]
        pair = [x_ref[k, pl.ds(group, 1), :] * along_y for k in range(7)]
        outs.append(dot3(split(jnp.concatenate(pair, axis=0)), weights, 1, 1))
    for k in range(7):
        for t in range(per_row + 1):
            value = 0.0
            if t < per_row:
                value = outs[t][16 * k : 16 * k + 8]
            if t >= 1:
                value = value + outs[t - 1][16 * k + 8 : 16 * k + 16]
            grid_ref[2 * a + k, 8 * t : 8 * t + 8, :] += value


def interp_row(a, per_row, cell_ref, q_ref, plain, slope, ext_ref, out_ref):
    groups, width = cell_ref.shape
    for b in range(per_row):
        group = a * per_row + b
        row = pl.ds(group, 1)
        base = cell_ref[row, :]
        masks = z_masks(base)
        footing = jnp.concatenate(
            [ext_ref[2 * a + k, 8 * b : 8 * b + 16, :] for k in range(7)], axis=0
        )
        footing = split(footing)
        both = []
        for refs in (plain, slope):
            window = z_window(base, [refs[2][j, row, :] for j in range(6)])
            both.append(dot3(footing, z_weights(masks, window), 1, 0))
        main, tilt = both
        along_x = 0.0
        along_y = 0.0
        along_z = 0.0
        for k in range(7):
            weight, grade = plain[0][k, row, :], slope[0][k, row, :]
            piece = main[16 * k : 16 * k + 16]
            along_x = along_x + grade * piece
            along_y = along_y + weight * piece
            along_z = along_z + weight * tilt[16 * k : 16 * k + 16]
        weight_y = rows_of_y(plain[1], group, groups, width)
        grade_y = rows_of_y(slope[1], group, groups, width)
        minus_q = -q_ref[row, :]
        pieces = (along_x * weight_y, along_y * grade_y, along_z * weight_y)
        for d, piece in enumerate(pieces):
            out_ref[d, row, :] = minus_q * jnp.sum(piece, axis=0, keepdims=True)


def weight_scratch(groups, width):
    return [
        pltpu.VMEM((7, groups, width), jnp.float32),
        pltpu.VMEM((groups * 16 * (width // 128), 128), jnp.float32),
        pltpu.VMEM((6, groups, width), jnp.float32),
    ]


def spread_kernel(per_row, slots, off_ref, z_ref, frac_ref, q_ref, grid_ref, *weights):
    grid_ref[...] = jnp.zeros_like(grid_ref)
    groups = z_ref.shape[0]

    def prepare(outer, carry):
        store_weights(outer, slots, off_ref, frac_ref, *weights, 0)
        return carry

    def step(a, carry):
        spread_row(a, per_row, z_ref, q_ref, *weights, grid_ref)
        return carry

    lax.fori_loop(0, groups // 8, prepare, 0)
    lax.fori_loop(0, groups // per_row, step, 0)


def interp_kernel(
    per_row, slots, off_ref, z_ref, frac_ref, q_ref, pot_ref, up_ref, side_ref, out_ref,
    ext_ref, *weights
):
    groups = z_ref.shape[0]
    size_z = pot_ref.shape[2]
    block_x, block_y = pot_ref.shape[0], pot_ref.shape[1]
    ext_ref[:block_x, :block_y] = pot_ref[...]
    ext_ref[block_x : block_x + 5, :block_y] = up_ref[...]
    ext_ref[block_x + 5 :, :block_y] = jnp.zeros((3, block_y, size_z), jnp.float32)
    ext_ref[: block_x + 5, block_y:] = side_ref[...]
    ext_ref[block_x + 5 :, block_y:] = jnp.zeros((3, 8, size_z), jnp.float32)

    def prepare(outer, carry):
        store_weights(outer, slots, off_ref, frac_ref, *weights[:3], 0)
        store_weights(outer, slots, off_ref, frac_ref, *weights[3:], 1)
        return carry

    def step(a, carry):
        interp_row(a, per_row, z_ref, q_ref, weights[:3], weights[3:], ext_ref, out_ref)
        return carry

    lax.fori_loop(0, groups // 8, prepare, 0)
    lax.fori_loop(0, groups // per_row, step, 0)


def modulus(index, length):
    coeffs = (1.0 / 120.0, 26.0 / 120.0, 66.0 / 120.0, 26.0 / 120.0, 1.0 / 120.0)
    real_part = 0.0
    imag_part = 0.0
    for j in range(5):
        angle = (index * j % length).astype(jnp.float32) * (2.0 * math.pi / length)
        real_part = real_part + coeffs[j] * jnp.cos(angle)
        imag_part = imag_part + coeffs[j] * jnp.sin(angle)
    return real_part * real_part + imag_part * imag_part


def influence(index_x, index_y, index_z):
    freq_x = jnp.where(2 * index_x < KX, index_x, index_x - KX).astype(jnp.float32) / KX
    freq_y = jnp.where(2 * index_y < KY, index_y, index_y - KY).astype(jnp.float32) / KY
    freq_z = jnp.where(2 * index_z < KZ, index_z, index_z - KZ).astype(jnp.float32) / KZ
    square = freq_x * freq_x + freq_y * freq_y + freq_z * freq_z
    safe = jnp.where(square > 0, square, 1.0)
    volume = float(KX * KY * KZ)
    value = jnp.exp(-math.pi**2 * safe / ewald_split**2) / (math.pi * volume * safe)
    value = value / (modulus(index_x, KX) * modulus(index_y, KY) * modulus(index_z, KZ))
    return jnp.where(square > 0, value, 0.0)


def waves(index, length):
    angle = (index % length) * (2.0 * math.pi / length)
    return (np.cos(angle), np.sin(angle))


def z_table(groups):
    planes = KZ // (2 * groups)
    frequency = np.arange(KZ // 2).reshape(groups, planes)
    cos, sin = waves(frequency[..., None] * np.arange(KZ), KZ)
    table = np.stack([cos, -sin], axis=1)
    table[0, 1, 0] = waves(np.arange(KZ) * (KZ // 2), KZ)[0]
    weight = np.full((groups, 2, planes), 2.0)
    weight[0, :, 0] = 1.0
    table = table.reshape(KZ, KZ)
    return (table.astype(np.float32), (table * weight.reshape(KZ, 1)).astype(np.float32))


def block_table(frequency, length, groups):
    position = np.arange(length)
    cos, sin = waves(frequency[..., None] * position, length)
    shape = (frequency.shape[0], frequency.shape[1], groups, length // groups)
    cos, sin = cos.reshape(shape), sin.reshape(shape)
    real_row = np.stack([cos, sin], axis=3)
    imag_row = np.stack([-sin, cos], axis=3)
    table = np.stack([real_row, imag_row], axis=1)
    return table.reshape(2 * length, 2 * length).astype(np.float32)


def y_frequency(groups):
    first = np.arange(KY // 2).reshape(groups, -1)
    second = np.where(first == 0, KY // 2, (KY - first) % KY)
    return np.concatenate([first, second], axis=1)


def partner_of(me, d, count):
    if count & (count - 1):
        return lax.rem(me + d, count)
    peer = me
    bit = 1
    while bit < count:
        if d & bit:
            peer = peer + bit - 2 * bit * lax.rem(lax.div(me, bit), 2)
        bit = 2 * bit
    return peer


def exchange_kernel(axis, count, *refs):
    arrays = (len(refs) - 3) // 2
    sources, targets = refs[:arrays], refs[arrays : 2 * arrays]
    send_sem, recv_sem, own_sem = refs[2 * arrays :]
    me = lax.axis_index(axis)
    barrier = pltpu.get_barrier_semaphore()
    for d in range(1, count):
        pl.semaphore_signal(
            barrier,
            inc=1,
            device_id={axis: partner_of(me, d, count)},
            device_id_type=pl.DeviceIdType.MESH,
        )
    pl.semaphore_wait(barrier, count - 1)
    copies = []
    for k in range(arrays):
        for d in range(1, count):
            peer = partner_of(me, d, count)
            copies.append(
                pltpu.make_async_remote_copy(
                    src_ref=sources[k].at[peer],
                    dst_ref=targets[k].at[me],
                    send_sem=send_sem.at[k, d],
                    recv_sem=recv_sem.at[k, d],
                    device_id={axis: peer},
                    device_id_type=pl.DeviceIdType.MESH,
                )
            )
        copies.append(
            pltpu.make_async_copy(sources[k].at[me], targets[k].at[me], own_sem.at[k])
        )
    for copy in copies:
        copy.start()
    for copy in copies:
        copy.wait()


def exchange(arrays, axis, number):
    count = lax.axis_size(axis)
    vmem = pl.BlockSpec(memory_space=pltpu.VMEM)
    return pl.pallas_call(
        functools.partial(exchange_kernel, axis, count),
        out_shape=[jax.ShapeDtypeStruct(array.shape, array.dtype) for array in arrays],
        in_specs=[vmem] * len(arrays),
        out_specs=[vmem] * len(arrays),
        scratch_shapes=[
            pltpu.SemaphoreType.DMA((len(arrays), count)),
            pltpu.SemaphoreType.DMA((len(arrays), count)),
            pltpu.SemaphoreType.DMA((len(arrays),)),
        ],
        compiler_params=pltpu.CompilerParams(collective_id=number, has_side_effects=True),
        name="exchange" + str(number),
    )(*arrays)


def dot(left, right, left_dim, right_dim):
    dims = (((left_dim,), (right_dim,)), ((), ()))
    return lax.dot_general(
        left, right, dims, precision=highest, preferred_element_type=jnp.float32
    )


def spectrum_of(grid, block_x, block_y):
    grp, pen = lax.axis_size("grp"), lax.axis_size("pen")
    planes = KZ // (2 * pen)
    lines = KY // grp
    half = lines // 2
    forward_z, backward_z = z_table(pen)
    order_y = y_frequency(grp)
    table_y = block_table(order_y, KY, pen)
    table_x = block_table(np.arange(KX)[None], KX, grp)
    lines_z = dot(forward_z, grid.reshape(block_x * block_y, KZ), 1, 1)
    lines_z = lines_z.reshape(pen, 2, planes, block_x, block_y).transpose(0, 1, 4, 2, 3)
    (columns,) = exchange(
        [lines_z.reshape(pen, 2 * block_y, planes * block_x)], "pen", 1
    )
    lines_y = dot(table_y, columns.reshape(2 * KY, planes * block_x), 1, 0)
    lines_y = lines_y.reshape(grp, 2, lines, planes, block_x).transpose(0, 1, 4, 3, 2)
    (rows,) = exchange([lines_y.reshape(grp, 2 * block_x, planes * lines)], "grp", 2)
    rows = rows.reshape(grp, 2, block_x, planes * lines)
    at_grp, at_pen = lax.axis_index("grp"), lax.axis_index("pen")
    packed = rows[..., :lines]
    alone = (at_grp == 0) & (jnp.arange(lines) % half == 0)
    partner = jnp.where(
        alone, packed, jnp.concatenate([packed[..., half:], packed[..., :half]], axis=-1)
    )
    a, b = packed[:, :1], packed[:, 1:]
    c, d = partner[:, :1], partner[:, 1:]
    whole = jnp.concatenate([a + c, b - d], axis=1) * 0.5
    midway = jnp.concatenate([b + d, c - a], axis=1) * 0.5
    origin = at_pen == 0
    whole = jnp.where(origin, whole, packed)
    midway = jnp.where(origin, midway, 0.0)
    total_lanes = (planes + 1) * lines
    full = jnp.concatenate([whole, rows[..., lines:], midway], axis=-1)
    spectrum = dot(table_x, full.reshape(2 * KX, total_lanes), 1, 0)
    spectrum = spectrum.reshape(2, KX, total_lanes)
    index_x = jnp.arange(KX, dtype=jnp.int32)[:, None]
    slot = jnp.arange(planes + 1, dtype=jnp.int32)
    index_z = jnp.where(slot < planes, at_pen * planes + slot, KZ // 2)
    plane_weight = jnp.where(
        slot < planes,
        jnp.where(origin & (slot == 0), 1.0, 2.0),
        jnp.where(origin, 1.0, 0.0),
    )
    index_z = jnp.repeat(index_z, lines)[None, :]
    plane_weight = jnp.repeat(plane_weight, lines)[None, :]
    index_y = lax.dynamic_index_in_dim(jnp.asarray(order_y, jnp.int32), at_grp, 0, False)
    index_y = jnp.tile(index_y, planes + 1)[None, :]
    kernel = influence(index_x, index_y, index_z)
    power = spectrum[0] * spectrum[0] + spectrum[1] * spectrum[1]
    spectral = 0.5 * jnp.sum(plane_weight * kernel * power)
    scaled = (spectrum * kernel).reshape(2 * KX, total_lanes)
    returning = dot(table_x, scaled, 0, 0).reshape(grp, 2, block_x, total_lanes)
    midway = returning[..., planes * lines :]
    turned = jnp.concatenate([-midway[:, 1:], midway[:, :1]], axis=1)
    returning = jnp.concatenate(
        [returning[..., :lines] + turned, returning[..., lines : planes * lines]], axis=-1
    )
    rows, sums = exchange(
        [
            returning.reshape(grp, 2 * block_x, planes * lines),
            jnp.broadcast_to(spectral, (grp, 8, 128)),
        ],
        "grp",
        3,
    )
    spectral = jnp.sum(sums[:, 0, 0])
    rows = rows.reshape(grp, 2, block_x, planes, lines).transpose(0, 1, 4, 3, 2)
    columns = dot(table_y, rows.reshape(2 * KY, planes * block_x), 0, 0)
    columns, sums = exchange(
        [
            columns.reshape(pen, 2 * block_y, planes * block_x),
            jnp.broadcast_to(spectral, (pen, 8, 128)),
        ],
        "pen",
        4,
    )
    spectral = jnp.sum(sums[:, 0, 0])
    home = columns.reshape(pen, 2, block_y, planes, block_x).transpose(0, 1, 3, 4, 2)
    potential = dot(home.reshape(KZ, block_x * block_y), backward_z, 0, 0)
    return (potential.reshape(block_x, block_y, KZ), spectral)


def cas_table(length):
    position = np.arange(length)
    cos, sin = waves(position[:, None] * position, length)
    return cos + sin


def halves(table):
    high = table.astype(jnp.bfloat16)
    low = (table - high.astype(np.float64)).astype(jnp.bfloat16)
    return (high, low)


def spline_factor(length):
    index = np.arange(length)
    freq = np.where(2 * index < length, index, index - length) / length
    coeffs = np.array([1.0, 26.0, 66.0, 26.0, 1.0]) / 120.0
    phase = np.exp(2j * np.pi * index[:, None] * np.arange(5) / length)
    modulus_square = np.abs(phase @ coeffs) ** 2
    square = freq**2
    factor = np.exp(-(math.pi**2) * square / ewald_split**2) / modulus_square
    return (factor.astype(np.float32), square.astype(np.float32))


def regroup(tiles, width):
    lane = lax.broadcasted_iota(jnp.int32, tiles[0].shape, 1) // width
    bit = 1
    while bit < len(tiles):
        keep = (lane // bit) % 2 == 0
        mixed = list(tiles)
        for i in range(len(tiles)):
            if not i & bit:
                first, second = tiles[i], tiles[i + bit]
                mixed[i] = jnp.where(keep, first, pltpu.roll(second, bit * width, 1))
                mixed[i + bit] = jnp.where(
                    keep, pltpu.roll(first, 128 - bit * width, 1), second
                )
        tiles = mixed
        bit = 2 * bit
    return tiles


def whole_kernel(
    grp, pen, slots, off_ref, cell_ref, frac_ref, q_ref, cas_hi, cas_lo, into_hi, into_lo,
    back_hi, back_lo, factor_row, factor_col, square_row, square_col, out_ref, energy_ref,
    pad, ext, plain_x, plain_y, plain_z, slope_x, slope_y, slope_z,
    send, recv, send_back, recv_back, work, sums, part,
    rim_side, rim_up, rim_corner, halo_side, halo_up, halo_corner,
    out_send, out_recv, back_send, back_recv, sum_send, sum_recv,
    side_send, side_recv, halo_send, halo_recv, edge_send, edge_recv,
):
    count = grp * pen
    slabs, blocks = send.shape[0], send.shape[2]
    groups = cell_ref.shape[0]
    block_x, block_y = KX // grp, KY // pen
    tile_rows = block_x // 2
    per_row = groups // tile_rows
    fan = 128 // block_y
    depth = block_x // slabs
    step = depth // 2
    half = pen // fan
    lines = 8 * blocks
    at_grp, at_pen = lax.axis_index("grp"), lax.axis_index("pen")
    me = at_grp * pen + at_pen
    plain = (plain_x, plain_y, plain_z)
    slope = (slope_x, slope_y, slope_z)
    cas = (cas_hi[...], cas_lo[...])

    def device(d_grp, d_pen):
        return {
            "grp": lax.rem(at_grp + d_grp + grp, grp),
            "pen": lax.rem(at_pen + d_pen + pen, pen),
        }

    def remote(source, target, sems, where):
        return pltpu.make_async_remote_copy(
            src_ref=source, dst_ref=target, send_sem=sems[0], recv_sem=sems[1],
            device_id=where, device_id_type=pl.DeviceIdType.MESH,
        )

    def peer_of(d):
        peer = lax.rem(me + d, count)
        return (peer, {"grp": lax.div(peer, pen), "pen": lax.rem(peer, pen)})

    def fan_out(make):
        def one(e, carry):
            make(1 + lax.rem(e + pen - 1, count - 1)).start()
            return carry

        lax.fori_loop(0, count - 1, one, 0)

    def fan_wait(make, receiving):
        def one(d, carry):
            copy = make(d)
            copy.wait_recv() if receiving else copy.wait_send()
            return carry

        lax.fori_loop(1, count, one, 0)

    def out_copy(s):
        def make(d):
            peer, where = peer_of(d)
            sems = (out_send.at[s, d], out_recv.at[s, d])
            return remote(send.at[s, peer], recv.at[s, me], sems, where)

        return make

    def back_copy(s):
        def make(d):
            peer, where = peer_of(d)
            sems = (back_send.at[s, d], back_recv.at[s, d])
            return remote(send_back.at[s, peer], recv_back.at[s, me], sems, where)

        return make

    def sum_copy(d):
        return remote(part, sums.at[me], (sum_send.at[d], sum_recv.at[d]), peer_of(d)[1])

    def slab_rows(s):
        return pl.ds(s * depth, depth)

    def side_rim(s):
        source = pad.at[slab_rows(s), pl.ds(block_y, 8), :]
        return remote(source, rim_side.at[s], (side_send.at[s], side_recv.at[s]), device(0, 1))

    def edge_rims():
        source = pad.at[pl.ds(block_x, 5)]
        return [
            remote(
                source.at[:, pl.ds(0, block_y), :], rim_up,
                (edge_send.at[0], edge_recv.at[0]), device(1, 0),
            ),
            remote(
                source.at[:, pl.ds(block_y, 8), :], rim_corner,
                (edge_send.at[1], edge_recv.at[1]), device(1, 1),
            ),
        ]

    def side_halo(s):
        source = ext.at[slab_rows(s), pl.ds(0, 8), :]
        return remote(source, halo_side.at[s], (halo_send.at[s], halo_recv.at[s]), device(0, -1))

    def edge_halos():
        source = ext.at[pl.ds(0, 5)]
        return [
            remote(
                source.at[:, pl.ds(0, block_y), :], halo_up,
                (edge_send.at[2], edge_recv.at[2]), device(-1, 0),
            ),
            remote(
                source.at[:, pl.ds(0, 8), :], halo_corner,
                (edge_send.at[3], edge_recv.at[3]), device(-1, -1),
            ),
        ]

    barrier = pltpu.get_barrier_semaphore()

    def greet(d, carry):
        pl.semaphore_signal(
            barrier, inc=1, device_id=peer_of(d)[1], device_id_type=pl.DeviceIdType.MESH
        )
        return carry

    lax.fori_loop(1, count, greet, 0)
    pad[...] = jnp.zeros_like(pad)

    def prepare(outer, carry):
        store_weights(outer, slots, off_ref, frac_ref, *plain, 0)
        return carry

    lax.fori_loop(0, groups // 8, prepare, 0)
    pl.semaphore_wait(barrier, count - 1)

    def ship(s):
        side_rim(s).wait_recv()
        pad[slab_rows(s), pl.ds(0, 8), :] += rim_side[s]

    def transform_out(s):
        def along_z(i, carry):
            rows = pad[pl.ds(s * depth + 2 * fan * i, 2 * fan), pl.ds(0, block_y), :]
            out = dot3(cas, split(rows.reshape(256, KZ)), 1, 1)
            for t in range(2):
                block = out[:, 128 * t : 128 * t + 128].reshape(count, 8, 128)
                send[s, :, 2 * i + t] = block
            return carry

        lax.fori_loop(0, blocks // 2, along_z, 0)
        fan_out(out_copy(s))
        recv[s, me] = send[s, me]

    def spread_step(i, carry):
        a = tile_rows - 1 - i
        spread_row(a, per_row, cell_ref, q_ref, *plain, pad)

        @pl.when(((lax.rem(a + 3, step) == 0) & (a + 3 < tile_rows)) | (a == 0))
        def _():
            side_rim(lax.div(a + 3, step)).start()

        @pl.when(a == tile_rows - step - 3)
        def _():
            for copy in edge_rims():
                copy.start()

        @pl.when((lax.rem(a + 7, step) == 0) & (a + 7 < tile_rows))
        def _():
            s = lax.div(a + 7, step)
            ship(s)
            transform_out(s)

        return carry

    lax.fori_loop(0, tile_rows, spread_step, 0)
    for copy in edge_rims():
        copy.wait_recv()
    ship(0)
    pad[:5, :block_y, :] += rim_up[...]
    pad[:5, :8, :] += rim_corner[...]
    transform_out(0)

    def prepare_slopes(outer, carry):
        store_weights(outer, slots, off_ref, frac_ref, *slope, 1)
        return carry

    lax.fori_loop(0, groups // 8, prepare_slopes, 0)

    def along_y(i, carry):
        s = slabs - 1 - i
        fan_wait(out_copy(s), True)
        rows = []
        for g in range(grp):
            parts = [[] for _ in range(fan)]
            for h in range(half):
                loaded = [
                    recv[s, g * pen + h * fan + k].reshape(lines, 128) for k in range(fan)
                ]
                for k, tile in enumerate(regroup(loaded, block_y)):
                    parts[k].append(tile)
            rows += [jnp.concatenate(part, axis=1) for part in parts]
        out = dot3(split(jnp.concatenate(rows, axis=0)), cas, 1, 0)
        span = grp * fan * lines
        for h in range(2):
            start = pl.multiple_of(s * span + h * 8 * KX, 128)
            work[pl.ds(start, span), :] = out[:, 128 * h : 128 * h + 128]
        return carry

    lax.fori_loop(0, slabs, along_y, 0)

    scale = 1.0 / (math.pi * KX * KY * KZ)
    first = pl.multiple_of(8 * me, 8)
    factor_z = factor_col[pl.ds(first, 8), :]
    square_z = square_col[pl.ds(first, 8), :]
    pick = lax.broadcasted_iota(jnp.int32, (8, 1), 0)

    def along_x(f, total):
        fz = jnp.sum(jnp.where(pick == f, factor_z, 0.0), axis=0, keepdims=True) * scale
        sz = jnp.sum(jnp.where(pick == f, square_z, 0.0), axis=0, keepdims=True)
        rows = jnp.concatenate(
            [work[pl.ds(f + h * 8 * KX, KX, stride=8), :] for h in range(2)], axis=1
        )
        spectrum = dot3((into_hi[...], into_lo[...]), split(rows), 1, 0)
        square = square_col[...] + (square_row[...] + sz)
        safe = jnp.where(square > 0, square, 1.0)
        kernel = factor_col[...] * (factor_row[...] * fz) / safe
        kernel = jnp.where(square > 0, kernel, 0.0)
        scaled = kernel * spectrum
        total = total + jnp.sum(scaled * spectrum, axis=0, keepdims=True)
        out = dot3((back_hi[...], back_lo[...]), split(scaled), 1, 0)
        for h in range(2):
            work[pl.ds(f + h * 8 * KX, KX, stride=8), :] = out[:, 128 * h : 128 * h + 128]
        return total

    total = lax.fori_loop(0, 8, along_x, jnp.zeros((1, KY), jnp.float32))
    part[...] = jnp.broadcast_to(0.5 * jnp.sum(total, axis=1, keepdims=True), (1, 128))
    sums[me] = part[...]

    def back_y(s, carry):
        span = grp * fan * lines
        rows = jnp.concatenate(
            [
                work[pl.ds(pl.multiple_of(s * span + h * 8 * KX, 128), span), :]
                for h in range(2)
            ],
            axis=1,
        )
        out = dot3(split(rows), cas, 1, 0)
        for g in range(grp):
            for h in range(half):
                parts = []
                for k in range(fan):
                    start = (g * fan + k) * lines
                    parts.append(out[start : start + lines, 128 * h : 128 * h + 128])
                for k, tile in enumerate(regroup(parts, block_y)):
                    send_back[s, g * pen + h * fan + k] = tile.reshape(blocks, 8, 128)
        fan_out(back_copy(s))
        recv_back[s, me] = send_back[s, me]
        return carry

    lax.fori_loop(0, slabs, back_y, 0)
    fan_out(sum_copy)

    def home(s, carry):
        fan_wait(back_copy(s), True)

        def home_z(i, inner):
            rows = jnp.concatenate(
                [recv_back[s, :, 2 * i + t].reshape(KZ, 128) for t in range(2)], axis=1
            )
            out = dot3(split(jnp.transpose(rows)), cas, 1, 0)
            where = pl.ds(s * depth + 2 * fan * i, 2 * fan)
            ext[where, pl.ds(0, block_y), :] = out.reshape(2 * fan, block_y, KZ)
            return inner

        lax.fori_loop(0, blocks // 2, home_z, 0)
        side_halo(s).start()
        return carry

    home(0, 0)
    for copy in edge_halos():
        copy.start()
    home(1, 0)

    def join_halo(s):
        side_halo(s).wait_recv()
        ext[slab_rows(s), pl.ds(block_y, 8), :] = halo_side[s]

    join_halo(0)

    def interp_step(a, carry):
        @pl.when((lax.rem(a, step) == 0) & (a >= step) & (a < tile_rows - step))
        def _():
            home(lax.div(a, step) + 1, 0)

        @pl.when((lax.rem(a + 3, step) == 0) & (a + 3 < tile_rows))
        def _():
            join_halo(lax.div(a + 3, step))

        @pl.when(a == tile_rows - 3)
        def _():
            for copy in edge_halos():
                copy.wait_recv()
            ext[pl.ds(block_x, 5), pl.ds(0, block_y), :] = halo_up[...]
            ext[pl.ds(block_x, 5), pl.ds(block_y, 8), :] = halo_corner[...]

        interp_row(a, per_row, cell_ref, q_ref, plain, slope, ext, out_ref)
        return carry

    lax.fori_loop(0, tile_rows, interp_step, 0)
    fan_wait(sum_copy, True)
    energy_ref[...] = jnp.sum(sums[...], axis=0)
    fan_wait(sum_copy, False)

    def drain(s, carry):
        fan_wait(out_copy(s), False)
        fan_wait(back_copy(s), False)
        side_rim(s).wait_send()
        side_halo(s).wait_send()
        return carry

    lax.fori_loop(0, slabs, drain, 0)
    for copy in edge_rims() + edge_halos():
        copy.wait_send()


def whole_program(offsets, zcell, fracs, live_q, slots, grp, pen, slabs):
    count = grp * pen
    groups, width = zcell.shape
    block_x, block_y = KX // grp, KY // pen
    fan = 128 // block_y
    blocks = block_x // fan // slabs
    depth = block_x // slabs
    cas = cas_table(KZ)
    order = np.arange(KX).reshape(grp, slabs, blocks, fan).transpose(1, 0, 3, 2).reshape(KX)
    factor, square = spline_factor(KX)
    tables = [*halves(cas), *halves(cas[:, order]), *halves(cas[order, :])]
    tables += [factor[None, :], factor[:, None], square[None, :], square[:, None]]
    tables = [jnp.asarray(table) for table in tables]
    vmem = pl.BlockSpec(memory_space=pltpu.VMEM)

    def held(*shape):
        return pltpu.VMEM(shape, jnp.float32)

    traffic = held(slabs, count, blocks, 8, 128)
    dma = pltpu.SemaphoreType.DMA
    forces, energy = pl.pallas_call(
        functools.partial(whole_kernel, grp, pen, slots),
        out_shape=[
            jax.ShapeDtypeStruct((3, groups, width), jnp.float32),
            jax.ShapeDtypeStruct((1, 128), jnp.float32),
        ],
        in_specs=[vmem] * (4 + len(tables)),
        out_specs=[vmem] * 2,
        scratch_shapes=[
            held(block_x + 8, block_y + 8, KZ),
            held(block_x + 8, block_y + 8, KZ),
            *weight_scratch(groups, width),
            *weight_scratch(groups, width),
            traffic, traffic, traffic, traffic,
            held(16 * KX, 128),
            held(count, 1, 128),
            held(1, 128),
            held(slabs, depth, 8, KZ), held(5, block_y, KZ), held(5, 8, KZ),
            held(slabs, depth, 8, KZ), held(5, block_y, KZ), held(5, 8, KZ),
            dma((slabs, count)), dma((slabs, count)),
            dma((slabs, count)), dma((slabs, count)),
            dma((count,)), dma((count,)),
            dma((slabs,)), dma((slabs,)), dma((slabs,)), dma((slabs,)),
            dma((4,)), dma((4,)),
        ],
        compiler_params=pltpu.CompilerParams(
            collective_id=1, has_side_effects=True, vmem_limit_bytes=60 * 1024 * 1024
        ),
        name="whole",
    )(offsets, zcell, fracs, live_q, *tables)
    return (forces, energy[0, 0])


def slab_fits(grp, pen, slabs, block_x, block_y, per_row):
    fan = 128 // block_y
    return (
        grp * pen * 8 == KZ and KX == KY and KY == KZ and KZ == 256 and pen % fan == 0
        and block_x == 16 * slabs and 16 % (2 * fan) == 0 and per_row * 8 == block_y
    )


def local(cell_offsets, cell_z, frac, charges, tile_counts):
    block_x = KX // lax.axis_size("grp")
    block_y = KY // lax.axis_size("pen")
    tiles = tile_counts.shape[0]
    slots = charges.shape[0] // tiles
    width = 4 * slots
    groups = tiles // 4
    per_row = block_y // 8
    live = jnp.arange(slots, dtype=jnp.int32)[None, :] < tile_counts[:, None]
    live_q = (charges.reshape(tiles, slots) * live.astype(jnp.float32)).reshape(groups, width)
    offsets = cell_offsets.reshape(2, groups, width)
    zcell = cell_z.reshape(groups, width)
    fracs = frac.reshape(3, groups, width)
    grp, pen = lax.axis_size("grp"), lax.axis_size("pen")
    if slab_fits(grp, pen, 4, block_x, block_y, per_row):
        forces, total = whole_program(offsets, zcell, fracs, live_q, slots, grp, pen, 4)
        return (forces.reshape(3, groups * width), total / ATOMS)
    vmem = pl.BlockSpec(memory_space=pltpu.VMEM)
    params = pltpu.CompilerParams(vmem_limit_bytes=60 * 1024 * 1024)
    padded = pl.pallas_call(
        functools.partial(spread_kernel, per_row, slots),
        out_shape=jax.ShapeDtypeStruct((block_x + 8, block_y + 8, KZ), jnp.float32),
        in_specs=[vmem] * 4,
        out_specs=vmem,
        scratch_shapes=weight_scratch(groups, width),
        compiler_params=params,
        name="spread",
    )(offsets, zcell, fracs, live_q)
    rim_y = shifted(padded[: block_x + 5, block_y : block_y + 5], "pen", 1)
    merged = padded[: block_x + 5, :block_y].at[:, :5].add(rim_y)
    rim_x = shifted(merged[block_x : block_x + 5], "grp", 1)
    grid = merged[:block_x] + jnp.pad(rim_x, ((0, block_x - 5), (0, 0), (0, 0)))
    potential, total = spectrum_of(grid, block_x, block_y)
    upper = shifted(potential[:5], "grp", -1)
    ext_x = jnp.concatenate([potential[:, :5], upper[:, :5]], axis=0)
    beside = shifted(ext_x, "pen", -1)
    beside = jnp.pad(beside, ((0, 0), (0, 3), (0, 0)))
    forces = pl.pallas_call(
        functools.partial(interp_kernel, per_row, slots),
        out_shape=jax.ShapeDtypeStruct((3, groups, width), jnp.float32),
        in_specs=[vmem] * 7,
        out_specs=vmem,
        scratch_shapes=[pltpu.VMEM((block_x + 8, block_y + 8, KZ), jnp.float32)]
        + 2 * weight_scratch(groups, width),
        compiler_params=params,
        name="interp",
    )(offsets, zcell, fracs, live_q, potential, upper, beside)
    return (forces.reshape(3, groups * width), total / ATOMS)


def solution(mesh):
    in_specs = (
        P(None, ("grp", "pen")),
        P(("grp", "pen")),
        P(None, ("grp", "pen")),
        P(("grp", "pen")),
        P(("grp", "pen")),
    )
    out_specs = (P(None, ("grp", "pen")), P())
    return jax.shard_map(local, mesh=mesh, in_specs=in_specs, out_specs=out_specs, check_vma=False)
```

```python
import functools
import math

import jax
import jax.numpy as jnp
import numpy as np
from jax import lax
from jax.experimental import pallas as pl
from jax.experimental.pallas import tpu as pltpu
from jax.sharding import PartitionSpec as P

KX = 256
KY = 256
KZ = 256
ATOMS = 1048576


ewald_split = 0.6
highest = lax.Precision.HIGH


def shifted(block, axis, distance):
    devices = range(lax.axis_size(axis))
    route = [((i - distance) % len(devices), i) for i in devices]
    return lax.ppermute(block, axis, route)


def spline_rows(fracs):
    values = [jnp.ones_like(fracs)]
    fifth = values
    for order in range(2, 7):
        nxt = []
        for j in range(order):
            term = jnp.zeros_like(fracs)
            if j >= 1:
                term = values[j - 1] * (fracs + order - 1 - j)
            if j <= order - 2:
                term = term + values[j] * (1.0 - fracs + j)
            nxt.append(term / (order - 1))
        if order == 5:
            fifth = nxt
        values = nxt
    slopes = []
    for j in range(6):
        term = jnp.zeros_like(fracs)
        if j >= 1:
            term = fifth[j - 1]
        if j <= 4:
            term = term - fifth[j]
        slopes.append(term)
    return (values, slopes)


def split(values):
    high = values.astype(jnp.bfloat16)
    low = (values - high.astype(jnp.float32)).astype(jnp.bfloat16)
    return (high, low)


def shift_rows(values, offset):
    none = jnp.zeros_like(values[0])
    return [
        jnp.where(offset == 0, first, second)
        for first, second in zip(values + [none], [none] + values)
    ]


def store_weights(outer, slots, off_ref, frac_ref, x_ref, y_ref, z_ref, which):
    groups, width = off_ref.shape[1], off_ref.shape[2]
    rows = pl.ds(pl.multiple_of(outer * 8, 8), 8)
    lane_tile = lax.broadcasted_iota(jnp.int32, (8, width), 1) // slots
    along_x = spline_rows(frac_ref[0, rows, :])[which]
    along_y = spline_rows(frac_ref[1, rows, :])[which]
    along_z = spline_rows(frac_ref[2, rows, :])[which]
    for k, value in enumerate(shift_rows(along_x, off_ref[0, rows, :])):
        x_ref[k, rows, :] = value
    for k, value in enumerate(along_z):
        z_ref[k, rows, :] = value
    near = shift_rows(along_y, off_ref[1, rows, :])
    none = jnp.zeros_like(near[0])
    for r in range(16):
        value = none
        for tile in range(4):
            if 0 <= r - 2 * tile < 7:
                value = jnp.where(lane_tile == tile, near[r - 2 * tile], value)
        for h in range(width // 128):
            start = (h * groups + outer * 8) * 16 + r
            y_ref[pl.ds(start, 8, stride=16), :] = value[:, 128 * h : 128 * h + 128]


def rows_of_y(y_ref, group, groups, width):
    parts = []
    for h in range(width // 128):
        start = pl.multiple_of((h * groups + group) * 16, 16)
        parts.append(y_ref[pl.ds(start, 16), :])
    return jnp.concatenate(parts, axis=1)


def z_window(base, values):
    fine = lax.broadcasted_iota(jnp.int32, (32, base.shape[1]), 0) - (base & 15)
    total = jnp.zeros(fine.shape, jnp.float32)
    for j in range(6):
        total = jnp.where(fine == j, values[j], total)
    return split(total)


def z_masks(base):
    coarse = jnp.broadcast_to(base // 16, (16, base.shape[1])).astype(jnp.int16)
    return [coarse == jnp.int16(k) for k in range(16)]


def z_weights(masks, window):
    halves_of = []
    for part in window:
        lower, upper = part[:16], part[16:]
        none = jnp.zeros_like(lower)
        blocks = []
        for k in range(16):
            block = jnp.where(masks[k - 1], upper, none)
            blocks.append(jnp.where(masks[k], lower, block))
        halves_of.append(jnp.concatenate(blocks, axis=0))
    return halves_of


def dot3(left, right, left_dim, right_dim):
    dims = (((left_dim,), (right_dim,)), ((), ()))
    one = functools.partial(
        lax.dot_general, dimension_numbers=dims, preferred_element_type=jnp.float32
    )
    return one(left[0], right[0]) + one(left[0], right[1]) + one(left[1], right[0])


def stacked_dot(left, right, left_dim, right_dim):
    dims = (((left_dim,), (right_dim,)), ((), ()))
    one = functools.partial(
        lax.dot_general, dimension_numbers=dims, preferred_element_type=jnp.float32
    )
    rows = left[0].shape[0]
    both = one(jnp.concatenate(left, axis=0), right[0])
    return both[:rows] + both[rows:] + one(left[0], right[1])


def spread_row(a, per_row, cell_ref, q_ref, x_ref, y_ref, z_ref, grid_ref):
    groups, width = cell_ref.shape
    outs = []
    for b in range(per_row):
        group = a * per_row + b
        base = cell_ref[pl.ds(group, 1), :]
        values = [z_ref[j, pl.ds(group, 1), :] for j in range(6)]
        weights = z_weights(z_masks(base), z_window(base, values))
        along_y = rows_of_y(y_ref, group, groups, width) * q_ref[pl.ds(group, 1), :]
        pair = [x_ref[k, pl.ds(group, 1), :] * along_y for k in range(7)]
        outs.append(stacked_dot(split(jnp.concatenate(pair, axis=0)), weights, 1, 1))
    for k in range(7):
        for t in range(per_row + 1):
            value = 0.0
            if t < per_row:
                value = outs[t][16 * k : 16 * k + 8]
            if t >= 1:
                value = value + outs[t - 1][16 * k + 8 : 16 * k + 16]
            grid_ref[2 * a + k, 8 * t : 8 * t + 8, :] += value


def interp_row(a, per_row, cell_ref, q_ref, plain, slope, ext_ref, out_ref):
    groups, width = cell_ref.shape
    for b in range(per_row):
        group = a * per_row + b
        row = pl.ds(group, 1)
        base = cell_ref[row, :]
        masks = z_masks(base)
        footing = jnp.concatenate(
            [ext_ref[2 * a + k, 8 * b : 8 * b + 16, :] for k in range(7)], axis=0
        )
        footing = split(footing)
        both = []
        for refs in (plain, slope):
            window = z_window(base, [refs[2][j, row, :] for j in range(6)])
            both.append(dot3(footing, z_weights(masks, window), 1, 0))
        main, tilt = both
        along_x = 0.0
        along_y = 0.0
        along_z = 0.0
        for k in range(7):
            weight, grade = plain[0][k, row, :], slope[0][k, row, :]
            piece = main[16 * k : 16 * k + 16]
            along_x = along_x + grade * piece
            along_y = along_y + weight * piece
            along_z = along_z + weight * tilt[16 * k : 16 * k + 16]
        weight_y = rows_of_y(plain[1], group, groups, width)
        grade_y = rows_of_y(slope[1], group, groups, width)
        minus_q = -q_ref[row, :]
        pieces = (along_x * weight_y, along_y * grade_y, along_z * weight_y)
        sums = [jnp.sum(piece, axis=0, keepdims=True) for piece in pieces]
        lanes = pl.ds(pl.multiple_of(group * width, width), width)
        out_ref[:, lanes] = minus_q * jnp.concatenate(sums, axis=0)


def weight_scratch(groups, width):
    return [
        pltpu.VMEM((7, groups, width), jnp.float32),
        pltpu.VMEM((groups * 16 * (width // 128), 128), jnp.float32),
        pltpu.VMEM((6, groups, width), jnp.float32),
    ]


def spread_kernel(per_row, slots, off_ref, z_ref, frac_ref, q_ref, grid_ref, *weights):
    grid_ref[...] = jnp.zeros_like(grid_ref)
    groups = z_ref.shape[0]

    def prepare(outer, carry):
        store_weights(outer, slots, off_ref, frac_ref, *weights, 0)
        return carry

    def step(a, carry):
        spread_row(a, per_row, z_ref, q_ref, *weights, grid_ref)
        return carry

    lax.fori_loop(0, groups // 8, prepare, 0)
    lax.fori_loop(0, groups // per_row, step, 0)


def interp_kernel(
    per_row, slots, off_ref, z_ref, frac_ref, q_ref, pot_ref, up_ref, side_ref, out_ref,
    ext_ref, *weights
):
    groups = z_ref.shape[0]
    size_z = pot_ref.shape[2]
    block_x, block_y = pot_ref.shape[0], pot_ref.shape[1]
    ext_ref[:block_x, :block_y] = pot_ref[...]
    ext_ref[block_x : block_x + 5, :block_y] = up_ref[...]
    ext_ref[block_x + 5 :, :block_y] = jnp.zeros((3, block_y, size_z), jnp.float32)
    ext_ref[: block_x + 5, block_y:] = side_ref[...]
    ext_ref[block_x + 5 :, block_y:] = jnp.zeros((3, 8, size_z), jnp.float32)

    def prepare(outer, carry):
        store_weights(outer, slots, off_ref, frac_ref, *weights[:3], 0)
        store_weights(outer, slots, off_ref, frac_ref, *weights[3:], 1)
        return carry

    def step(a, carry):
        interp_row(a, per_row, z_ref, q_ref, weights[:3], weights[3:], ext_ref, out_ref)
        return carry

    lax.fori_loop(0, groups // 8, prepare, 0)
    lax.fori_loop(0, groups // per_row, step, 0)


def modulus(index, length):
    coeffs = (1.0 / 120.0, 26.0 / 120.0, 66.0 / 120.0, 26.0 / 120.0, 1.0 / 120.0)
    real_part = 0.0
    imag_part = 0.0
    for j in range(5):
        angle = (index * j % length).astype(jnp.float32) * (2.0 * math.pi / length)
        real_part = real_part + coeffs[j] * jnp.cos(angle)
        imag_part = imag_part + coeffs[j] * jnp.sin(angle)
    return real_part * real_part + imag_part * imag_part


def influence(index_x, index_y, index_z):
    freq_x = jnp.where(2 * index_x < KX, index_x, index_x - KX).astype(jnp.float32) / KX
    freq_y = jnp.where(2 * index_y < KY, index_y, index_y - KY).astype(jnp.float32) / KY
    freq_z = jnp.where(2 * index_z < KZ, index_z, index_z - KZ).astype(jnp.float32) / KZ
    square = freq_x * freq_x + freq_y * freq_y + freq_z * freq_z
    safe = jnp.where(square > 0, square, 1.0)
    volume = float(KX * KY * KZ)
    value = jnp.exp(-math.pi**2 * safe / ewald_split**2) / (math.pi * volume * safe)
    value = value / (modulus(index_x, KX) * modulus(index_y, KY) * modulus(index_z, KZ))
    return jnp.where(square > 0, value, 0.0)


def waves(index, length):
    angle = (index % length) * (2.0 * math.pi / length)
    return (np.cos(angle), np.sin(angle))


def z_table(groups):
    planes = KZ // (2 * groups)
    frequency = np.arange(KZ // 2).reshape(groups, planes)
    cos, sin = waves(frequency[..., None] * np.arange(KZ), KZ)
    table = np.stack([cos, -sin], axis=1)
    table[0, 1, 0] = waves(np.arange(KZ) * (KZ // 2), KZ)[0]
    weight = np.full((groups, 2, planes), 2.0)
    weight[0, :, 0] = 1.0
    table = table.reshape(KZ, KZ)
    return (table.astype(np.float32), (table * weight.reshape(KZ, 1)).astype(np.float32))


def block_table(frequency, length, groups):
    position = np.arange(length)
    cos, sin = waves(frequency[..., None] * position, length)
    shape = (frequency.shape[0], frequency.shape[1], groups, length // groups)
    cos, sin = cos.reshape(shape), sin.reshape(shape)
    real_row = np.stack([cos, sin], axis=3)
    imag_row = np.stack([-sin, cos], axis=3)
    table = np.stack([real_row, imag_row], axis=1)
    return table.reshape(2 * length, 2 * length).astype(np.float32)


def y_frequency(groups):
    first = np.arange(KY // 2).reshape(groups, -1)
    second = np.where(first == 0, KY // 2, (KY - first) % KY)
    return np.concatenate([first, second], axis=1)


def partner_of(me, d, count):
    if count & (count - 1):
        return lax.rem(me + d, count)
    peer = me
    bit = 1
    while bit < count:
        if d & bit:
            peer = peer + bit - 2 * bit * lax.rem(lax.div(me, bit), 2)
        bit = 2 * bit
    return peer


def exchange_kernel(axis, count, *refs):
    arrays = (len(refs) - 3) // 2
    sources, targets = refs[:arrays], refs[arrays : 2 * arrays]
    send_sem, recv_sem, own_sem = refs[2 * arrays :]
    me = lax.axis_index(axis)
    barrier = pltpu.get_barrier_semaphore()
    for d in range(1, count):
        pl.semaphore_signal(
            barrier,
            inc=1,
            device_id={axis: partner_of(me, d, count)},
            device_id_type=pl.DeviceIdType.MESH,
        )
    pl.semaphore_wait(barrier, count - 1)
    copies = []
    for k in range(arrays):
        for d in range(1, count):
            peer = partner_of(me, d, count)
            copies.append(
                pltpu.make_async_remote_copy(
                    src_ref=sources[k].at[peer],
                    dst_ref=targets[k].at[me],
                    send_sem=send_sem.at[k, d],
                    recv_sem=recv_sem.at[k, d],
                    device_id={axis: peer},
                    device_id_type=pl.DeviceIdType.MESH,
                )
            )
        copies.append(
            pltpu.make_async_copy(sources[k].at[me], targets[k].at[me], own_sem.at[k])
        )
    for copy in copies:
        copy.start()
    for copy in copies:
        copy.wait()


def exchange(arrays, axis, number):
    count = lax.axis_size(axis)
    vmem = pl.BlockSpec(memory_space=pltpu.VMEM)
    return pl.pallas_call(
        functools.partial(exchange_kernel, axis, count),
        out_shape=[jax.ShapeDtypeStruct(array.shape, array.dtype) for array in arrays],
        in_specs=[vmem] * len(arrays),
        out_specs=[vmem] * len(arrays),
        scratch_shapes=[
            pltpu.SemaphoreType.DMA((len(arrays), count)),
            pltpu.SemaphoreType.DMA((len(arrays), count)),
            pltpu.SemaphoreType.DMA((len(arrays),)),
        ],
        compiler_params=pltpu.CompilerParams(collective_id=number, has_side_effects=True),
        name="exchange" + str(number),
    )(*arrays)


def dot(left, right, left_dim, right_dim):
    dims = (((left_dim,), (right_dim,)), ((), ()))
    return lax.dot_general(
        left, right, dims, precision=highest, preferred_element_type=jnp.float32
    )


def spectrum_of(grid, block_x, block_y):
    grp, pen = lax.axis_size("grp"), lax.axis_size("pen")
    planes = KZ // (2 * pen)
    lines = KY // grp
    half = lines // 2
    forward_z, backward_z = z_table(pen)
    order_y = y_frequency(grp)
    table_y = block_table(order_y, KY, pen)
    table_x = block_table(np.arange(KX)[None], KX, grp)
    lines_z = dot(forward_z, grid.reshape(block_x * block_y, KZ), 1, 1)
    lines_z = lines_z.reshape(pen, 2, planes, block_x, block_y).transpose(0, 1, 4, 2, 3)
    (columns,) = exchange(
        [lines_z.reshape(pen, 2 * block_y, planes * block_x)], "pen", 1
    )
    lines_y = dot(table_y, columns.reshape(2 * KY, planes * block_x), 1, 0)
    lines_y = lines_y.reshape(grp, 2, lines, planes, block_x).transpose(0, 1, 4, 3, 2)
    (rows,) = exchange([lines_y.reshape(grp, 2 * block_x, planes * lines)], "grp", 2)
    rows = rows.reshape(grp, 2, block_x, planes * lines)
    at_grp, at_pen = lax.axis_index("grp"), lax.axis_index("pen")
    packed = rows[..., :lines]
    alone = (at_grp == 0) & (jnp.arange(lines) % half == 0)
    partner = jnp.where(
        alone, packed, jnp.concatenate([packed[..., half:], packed[..., :half]], axis=-1)
    )
    a, b = packed[:, :1], packed[:, 1:]
    c, d = partner[:, :1], partner[:, 1:]
    whole = jnp.concatenate([a + c, b - d], axis=1) * 0.5
    midway = jnp.concatenate([b + d, c - a], axis=1) * 0.5
    origin = at_pen == 0
    whole = jnp.where(origin, whole, packed)
    midway = jnp.where(origin, midway, 0.0)
    total_lanes = (planes + 1) * lines
    full = jnp.concatenate([whole, rows[..., lines:], midway], axis=-1)
    spectrum = dot(table_x, full.reshape(2 * KX, total_lanes), 1, 0)
    spectrum = spectrum.reshape(2, KX, total_lanes)
    index_x = jnp.arange(KX, dtype=jnp.int32)[:, None]
    slot = jnp.arange(planes + 1, dtype=jnp.int32)
    index_z = jnp.where(slot < planes, at_pen * planes + slot, KZ // 2)
    plane_weight = jnp.where(
        slot < planes,
        jnp.where(origin & (slot == 0), 1.0, 2.0),
        jnp.where(origin, 1.0, 0.0),
    )
    index_z = jnp.repeat(index_z, lines)[None, :]
    plane_weight = jnp.repeat(plane_weight, lines)[None, :]
    index_y = lax.dynamic_index_in_dim(jnp.asarray(order_y, jnp.int32), at_grp, 0, False)
    index_y = jnp.tile(index_y, planes + 1)[None, :]
    kernel = influence(index_x, index_y, index_z)
    power = spectrum[0] * spectrum[0] + spectrum[1] * spectrum[1]
    spectral = 0.5 * jnp.sum(plane_weight * kernel * power)
    scaled = (spectrum * kernel).reshape(2 * KX, total_lanes)
    returning = dot(table_x, scaled, 0, 0).reshape(grp, 2, block_x, total_lanes)
    midway = returning[..., planes * lines :]
    turned = jnp.concatenate([-midway[:, 1:], midway[:, :1]], axis=1)
    returning = jnp.concatenate(
        [returning[..., :lines] + turned, returning[..., lines : planes * lines]], axis=-1
    )
    rows, sums = exchange(
        [
            returning.reshape(grp, 2 * block_x, planes * lines),
            jnp.broadcast_to(spectral, (grp, 8, 128)),
        ],
        "grp",
        3,
    )
    spectral = jnp.sum(sums[:, 0, 0])
    rows = rows.reshape(grp, 2, block_x, planes, lines).transpose(0, 1, 4, 3, 2)
    columns = dot(table_y, rows.reshape(2 * KY, planes * block_x), 0, 0)
    columns, sums = exchange(
        [
            columns.reshape(pen, 2 * block_y, planes * block_x),
            jnp.broadcast_to(spectral, (pen, 8, 128)),
        ],
        "pen",
        4,
    )
    spectral = jnp.sum(sums[:, 0, 0])
    home = columns.reshape(pen, 2, block_y, planes, block_x).transpose(0, 1, 3, 4, 2)
    potential = dot(home.reshape(KZ, block_x * block_y), backward_z, 0, 0)
    return (potential.reshape(block_x, block_y, KZ), spectral)


def cas_table(length):
    position = np.arange(length)
    cos, sin = waves(position[:, None] * position, length)
    return cos + sin


def halves(table):
    high = table.astype(jnp.bfloat16)
    low = (table - high.astype(np.float64)).astype(jnp.bfloat16)
    return (high, low)


def spline_factor(length):
    index = np.arange(length)
    freq = np.where(2 * index < length, index, index - length) / length
    coeffs = np.array([1.0, 26.0, 66.0, 26.0, 1.0]) / 120.0
    phase = np.exp(2j * np.pi * index[:, None] * np.arange(5) / length)
    modulus_square = np.abs(phase @ coeffs) ** 2
    square = freq**2
    factor = np.exp(-(math.pi**2) * square / ewald_split**2) / modulus_square
    return (factor.astype(np.float32), square.astype(np.float32))


def regroup(tiles, width):
    lane = lax.broadcasted_iota(jnp.int32, tiles[0].shape, 1) // width
    bit = 1
    while bit < len(tiles):
        keep = (lane // bit) % 2 == 0
        mixed = list(tiles)
        for i in range(len(tiles)):
            if not i & bit:
                first, second = tiles[i], tiles[i + bit]
                mixed[i] = jnp.where(keep, first, pltpu.roll(second, bit * width, 1))
                mixed[i + bit] = jnp.where(
                    keep, pltpu.roll(first, 128 - bit * width, 1), second
                )
        tiles = mixed
        bit = 2 * bit
    return tiles


def whole_kernel(
    grp, pen, slots, sizes, off_ref, cell_ref, frac_ref, q_ref, cas_hi, cas_lo, into_hi, into_lo,
    back_hi, back_lo, factor_row, factor_col, square_row, square_col, out_ref, energy_ref,
    pad, ext, plain_x, plain_y, plain_z, slope_x, slope_y, slope_z,
    send, recv, send_back, recv_back, work, sums, part,
    rim_side, rim_up, rim_corner, halo_side, halo_up, halo_corner,
    out_send, out_recv, back_send, back_recv, sum_send, sum_recv,
    side_send, side_recv, halo_send, halo_recv, edge_send, edge_recv,
):
    count = grp * pen
    slabs = len(sizes)
    starts = [sum(sizes[:s]) for s in range(slabs)]
    groups = cell_ref.shape[0]
    block_x, block_y = KX // grp, KY // pen
    tile_rows = block_x // 2
    per_row = groups // tile_rows
    fan = 128 // block_y
    half = pen // fan
    at_grp, at_pen = lax.axis_index("grp"), lax.axis_index("pen")
    me = at_grp * pen + at_pen
    plain = (plain_x, plain_y, plain_z)
    slope = (slope_x, slope_y, slope_z)
    cas = (cas_hi[...], cas_lo[...])

    def device(d_grp, d_pen):
        return {
            "grp": lax.rem(at_grp + d_grp + grp, grp),
            "pen": lax.rem(at_pen + d_pen + pen, pen),
        }

    def remote(source, target, sems, where):
        return pltpu.make_async_remote_copy(
            src_ref=source, dst_ref=target, send_sem=sems[0], recv_sem=sems[1],
            device_id=where, device_id_type=pl.DeviceIdType.MESH,
        )

    def peer_of(d):
        peer = lax.rem(me + d, count)
        return (peer, {"grp": lax.div(peer, pen), "pen": lax.rem(peer, pen)})

    def fan_out(make):
        def one(e, carry):
            make(1 + lax.rem(e + pen - 1, count - 1)).start()
            return carry

        lax.fori_loop(0, count - 1, one, 0)

    def fan_wait(make, receiving):
        def one(d, carry):
            copy = make(d)
            copy.wait_recv() if receiving else copy.wait_send()
            return carry

        lax.fori_loop(1, count, one, 0)

    def slab_copy(s, source, target, sems):
        part_of = pl.ds(starts[s], sizes[s])

        def make(d):
            peer, where = peer_of(d)
            pair = (sems[0].at[s, d], sems[1].at[s, d])
            return remote(source.at[peer, part_of], target.at[me, part_of], pair, where)

        return make

    def out_copy(s):
        return slab_copy(s, send, recv, (out_send, out_recv))

    def back_copy(s):
        return slab_copy(s, send_back, recv_back, (back_send, back_recv))

    def sum_copy(d):
        return remote(part, sums.at[me], (sum_send.at[d], sum_recv.at[d]), peer_of(d)[1])

    def slab_rows(s):
        return pl.ds(starts[s] * fan, sizes[s] * fan)

    def side_rim(s):
        source = pad.at[slab_rows(s), pl.ds(block_y, 8), :]
        return remote(source, rim_side.at[slab_rows(s)], (side_send.at[s], side_recv.at[s]), device(0, 1))

    def edge_rims():
        source = pad.at[pl.ds(block_x, 5)]
        return [
            remote(
                source.at[:, pl.ds(0, block_y), :], rim_up,
                (edge_send.at[0], edge_recv.at[0]), device(1, 0),
            ),
            remote(
                source.at[:, pl.ds(block_y, 8), :], rim_corner,
                (edge_send.at[1], edge_recv.at[1]), device(1, 1),
            ),
        ]

    def side_halo(s):
        source = ext.at[slab_rows(s), pl.ds(0, 8), :]
        return remote(source, halo_side.at[slab_rows(s)], (halo_send.at[s], halo_recv.at[s]), device(0, -1))

    def edge_halos():
        source = ext.at[pl.ds(0, 5)]
        return [
            remote(
                source.at[:, pl.ds(0, block_y), :], halo_up,
                (edge_send.at[2], edge_recv.at[2]), device(-1, 0),
            ),
            remote(
                source.at[:, pl.ds(0, 8), :], halo_corner,
                (edge_send.at[3], edge_recv.at[3]), device(-1, -1),
            ),
        ]

    barrier = pltpu.get_barrier_semaphore()

    def greet(d, carry):
        pl.semaphore_signal(
            barrier, inc=1, device_id=peer_of(d)[1], device_id_type=pl.DeviceIdType.MESH
        )
        return carry

    lax.fori_loop(1, count, greet, 0)
    pad[...] = jnp.zeros_like(pad)

    pl.semaphore_wait(barrier, count - 1)

    def ship(s):
        side_rim(s).wait_recv()
        pad[slab_rows(s), pl.ds(0, 8), :] += rim_side[slab_rows(s)]

    def transform_out(s):
        def along_z(i, carry):
            tile = starts[s] + 2 * i
            rows = pad[pl.ds(tile * fan, 2 * fan), pl.ds(0, block_y), :]
            out = dot3(cas, split(rows.reshape(256, KZ)), 1, 1)
            for t in range(2):
                block = out[:, 128 * t : 128 * t + 128].reshape(count, 8, 128)
                send[:, tile + t] = block
            return carry

        lax.fori_loop(0, sizes[s] // 2, along_z, 0)
        fan_out(out_copy(s))
        own = pl.ds(starts[s], sizes[s])
        recv[me, own] = send[me, own]

    ready = [max((start * fan - 5) // 2, 0) for start in starts]
    rows_per_outer = 8 // per_row

    def spread_step(i, carry):
        a = tile_rows - 1 - i

        @pl.when(lax.rem(i, rows_per_outer) == 0)
        def _():
            outer = lax.div(a, rows_per_outer)
            store_weights(outer, slots, off_ref, frac_ref, *plain, 0)

        spread_row(a, per_row, cell_ref, q_ref, *plain, pad)

        @pl.when(a == tile_rows - 3)
        def _():
            for copy in edge_rims():
                copy.start()

        for s in range(slabs):

            @pl.when(a == ready[s])
            def _(s=s):
                side_rim(s).start()

            if s:

                @pl.when(a == max(ready[s] - 5, 0))
                def _(s=s):
                    ship(s)
                    transform_out(s)

        return carry

    lax.fori_loop(0, tile_rows, spread_step, 0)
    for copy in edge_rims():
        copy.wait_recv()
    ship(0)
    pad[:5, :block_y, :] += rim_up[...]
    pad[:5, :8, :] += rim_corner[...]
    transform_out(0)

    def prepare_slopes(outer, carry):
        store_weights(outer, slots, off_ref, frac_ref, *slope, 1)
        return carry

    lax.fori_loop(0, groups // 8, prepare_slopes, 0)

    def slab_lines(s, h):
        span = sizes[s] * 8 * KX // (block_x // fan)
        return pl.ds(starts[s] * 8 * KX // (block_x // fan) + h * 8 * KX, span)

    for s in reversed(range(slabs)):
        fan_wait(out_copy(s), True)
        rows = []
        own = pl.ds(starts[s], sizes[s])
        for g in range(grp):
            parts = [[] for _ in range(fan)]
            for h in range(half):
                loaded = [
                    recv[g * pen + h * fan + k, own].reshape(8 * sizes[s], 128)
                    for k in range(fan)
                ]
                for k, tile in enumerate(regroup(loaded, block_y)):
                    parts[k].append(tile)
            rows += [jnp.concatenate(pieces, axis=1) for pieces in parts]
        out = dot3(split(jnp.concatenate(rows, axis=0)), cas, 1, 0)
        for h in range(2):
            work[slab_lines(s, h), :] = out[:, 128 * h : 128 * h + 128]

    scale = 1.0 / (math.pi * KX * KY * KZ)
    first = pl.multiple_of(8 * me, 8)
    factor_z = factor_col[pl.ds(first, 8), :]
    square_z = square_col[pl.ds(first, 8), :]
    pick = lax.broadcasted_iota(jnp.int32, (8, 1), 0)

    def along_x(i, total):
        for f in (2 * i, 2 * i + 1):
            chosen = pick == f
            fz = jnp.sum(jnp.where(chosen, factor_z, 0.0), axis=0, keepdims=True) * scale
            sz = jnp.sum(jnp.where(chosen, square_z, 0.0), axis=0, keepdims=True)
            rows = jnp.concatenate(
                [work[pl.ds(f + h * 8 * KX, KX, stride=8), :] for h in range(2)], axis=1
            )
            spectrum = dot3((into_hi[...], into_lo[...]), split(rows), 1, 0)
            square = square_col[...] + (square_row[...] + sz)
            safe = jnp.where(square > 0, square, 1.0)
            kernel = factor_col[...] * (factor_row[...] * fz) / safe
            kernel = jnp.where(square > 0, kernel, 0.0)
            scaled = kernel * spectrum
            total = total + jnp.sum(scaled * spectrum, axis=0, keepdims=True)
            out = dot3((back_hi[...], back_lo[...]), split(scaled), 1, 0)
            for h in range(2):
                rows = pl.ds(f + h * 8 * KX, KX, stride=8)
                work[rows, :] = out[:, 128 * h : 128 * h + 128]
        return total

    total = lax.fori_loop(0, 4, along_x, jnp.zeros((1, KY), jnp.float32))
    part[...] = jnp.broadcast_to(0.5 * jnp.sum(total, axis=1, keepdims=True), (1, 128))
    sums[me] = part[...]

    for s in range(slabs):
        rows = jnp.concatenate([work[slab_lines(s, h), :] for h in range(2)], axis=1)
        out = dot3(split(rows), cas, 1, 0)
        lines = 8 * sizes[s]
        own = pl.ds(starts[s], sizes[s])
        for g in range(grp):
            for h in range(half):
                parts = []
                for k in range(fan):
                    start = (g * fan + k) * lines
                    parts.append(out[start : start + lines, 128 * h : 128 * h + 128])
                for k, tile in enumerate(regroup(parts, block_y)):
                    send_back[g * pen + h * fan + k, own] = tile.reshape(sizes[s], 8, 128)
        fan_out(back_copy(s))
        recv_back[me, own] = send_back[me, own]
    fan_out(sum_copy)

    def home(s):
        fan_wait(back_copy(s), True)

        def home_z(i, inner):
            tile = starts[s] + 2 * i
            rows = jnp.concatenate(
                [recv_back[:, tile + t].reshape(KZ, 128) for t in range(2)], axis=1
            )
            out = dot3(split(jnp.transpose(rows)), cas, 1, 0)
            where = pl.ds(tile * fan, 2 * fan)
            ext[where, pl.ds(0, block_y), :] = out.reshape(2 * fan, block_y, KZ)
            return inner

        lax.fori_loop(0, sizes[s] // 2, home_z, 0)
        side_halo(s).start()

    def join_halo(s):
        side_halo(s).wait_recv()
        ext[slab_rows(s), pl.ds(block_y, 8), :] = halo_side[slab_rows(s)]

    home(0)
    for copy in edge_halos():
        copy.start()
    join_halo(0)
    needed = [max((start * fan - 5) // 2, 0) for start in starts]
    early = [0] + [min(needed[s], 3) for s in range(1, slabs)]
    early[-1] = min(needed[-1], 5)

    def interp_step(a, carry):
        for s in range(1, slabs):

            @pl.when(a == needed[s] - early[s])
            def _(s=s):
                home(s)

            @pl.when(a == needed[s])
            def _(s=s):
                join_halo(s)

        @pl.when(a == tile_rows - 3)
        def _():
            for copy in edge_halos():
                copy.wait_recv()
            ext[pl.ds(block_x, 5), pl.ds(0, block_y), :] = halo_up[...]
            ext[pl.ds(block_x, 5), pl.ds(block_y, 8), :] = halo_corner[...]

        interp_row(a, per_row, cell_ref, q_ref, plain, slope, ext, out_ref)
        return carry

    lax.fori_loop(0, tile_rows, interp_step, 0)
    fan_wait(sum_copy, True)
    energy_ref[...] = jnp.sum(sums[...], axis=0)
    fan_wait(sum_copy, False)

    for s in range(slabs):
        fan_wait(out_copy(s), False)
        fan_wait(back_copy(s), False)
        side_rim(s).wait_send()
        side_halo(s).wait_send()
    for copy in edge_rims() + edge_halos():
        copy.wait_send()


def whole_program(offsets, zcell, fracs, live_q, slots, grp, pen, sizes):
    count = grp * pen
    groups, width = zcell.shape
    block_x, block_y = KX // grp, KY // pen
    fan = 128 // block_y
    slabs = len(sizes)
    cas = cas_table(KZ)
    cells = np.arange(KX).reshape(grp, block_x // fan, fan)
    order = np.concatenate(
        [
            cells[:, sum(sizes[:s]) : sum(sizes[: s + 1])].transpose(0, 2, 1).reshape(-1)
            for s in range(slabs)
        ]
    )
    factor, square = spline_factor(KX)
    tables = [*halves(cas), *halves(cas[:, order]), *halves(cas[order, :])]
    tables += [factor[None, :], factor[:, None], square[None, :], square[:, None]]
    tables = [jnp.asarray(table) for table in tables]
    vmem = pl.BlockSpec(memory_space=pltpu.VMEM)

    def held(*shape):
        return pltpu.VMEM(shape, jnp.float32)

    traffic = held(count, block_x // fan, 8, 128)
    dma = pltpu.SemaphoreType.DMA
    forces, energy = pl.pallas_call(
        functools.partial(whole_kernel, grp, pen, slots, sizes),
        out_shape=[
            jax.ShapeDtypeStruct((3, groups * width), jnp.float32),
            jax.ShapeDtypeStruct((1, 128), jnp.float32),
        ],
        in_specs=[vmem] * (4 + len(tables)),
        out_specs=[vmem] * 2,
        scratch_shapes=[
            held(block_x + 8, block_y + 8, KZ),
            held(block_x + 8, block_y + 8, KZ),
            *weight_scratch(groups, width),
            *weight_scratch(groups, width),
            traffic, traffic, traffic, traffic,
            held(16 * KX, 128),
            held(count, 1, 128),
            held(1, 128),
            held(block_x, 8, KZ), held(5, block_y, KZ), held(5, 8, KZ),
            held(block_x, 8, KZ), held(5, block_y, KZ), held(5, 8, KZ),
            dma((slabs, count)), dma((slabs, count)),
            dma((slabs, count)), dma((slabs, count)),
            dma((count,)), dma((count,)),
            dma((slabs,)), dma((slabs,)), dma((slabs,)), dma((slabs,)),
            dma((4,)), dma((4,)),
        ],
        compiler_params=pltpu.CompilerParams(
            collective_id=1, has_side_effects=True, vmem_limit_bytes=60 * 1024 * 1024
        ),
        name="whole",
    )(offsets, zcell, fracs, live_q, *tables)
    return (forces, energy[0, 0])


def slab_fits(grp, pen, sizes, block_x, block_y, per_row):
    fan = 128 // block_y
    return (
        grp * pen * 8 == KZ and KX == KY and KY == KZ and KZ == 256 and pen % fan == 0
        and block_x == fan * sum(sizes) and per_row * 8 == block_y and 8 % per_row == 0
    )


def local(cell_offsets, cell_z, frac, charges, tile_counts):
    block_x = KX // lax.axis_size("grp")
    block_y = KY // lax.axis_size("pen")
    tiles = tile_counts.shape[0]
    slots = charges.shape[0] // tiles
    width = 4 * slots
    groups = tiles // 4
    per_row = block_y // 8
    live = jnp.arange(slots, dtype=jnp.int32)[None, :] < tile_counts[:, None]
    live_q = (charges.reshape(tiles, slots) * live.astype(jnp.float32)).reshape(groups, width)
    offsets = cell_offsets.reshape(2, groups, width)
    zcell = cell_z.reshape(groups, width)
    fracs = frac.reshape(3, groups, width)
    grp, pen = lax.axis_size("grp"), lax.axis_size("pen")
    sizes = (4, 6, 4, 2)
    if slab_fits(grp, pen, sizes, block_x, block_y, per_row):
        forces, total = whole_program(offsets, zcell, fracs, live_q, slots, grp, pen, sizes)
        return (forces, total / ATOMS)
    vmem = pl.BlockSpec(memory_space=pltpu.VMEM)
    params = pltpu.CompilerParams(vmem_limit_bytes=60 * 1024 * 1024)
    padded = pl.pallas_call(
        functools.partial(spread_kernel, per_row, slots),
        out_shape=jax.ShapeDtypeStruct((block_x + 8, block_y + 8, KZ), jnp.float32),
        in_specs=[vmem] * 4,
        out_specs=vmem,
        scratch_shapes=weight_scratch(groups, width),
        compiler_params=params,
        name="spread",
    )(offsets, zcell, fracs, live_q)
    rim_y = shifted(padded[: block_x + 5, block_y : block_y + 5], "pen", 1)
    merged = padded[: block_x + 5, :block_y].at[:, :5].add(rim_y)
    rim_x = shifted(merged[block_x : block_x + 5], "grp", 1)
    grid = merged[:block_x] + jnp.pad(rim_x, ((0, block_x - 5), (0, 0), (0, 0)))
    potential, total = spectrum_of(grid, block_x, block_y)
    upper = shifted(potential[:5], "grp", -1)
    ext_x = jnp.concatenate([potential[:, :5], upper[:, :5]], axis=0)
    beside = shifted(ext_x, "pen", -1)
    beside = jnp.pad(beside, ((0, 0), (0, 3), (0, 0)))
    forces = pl.pallas_call(
        functools.partial(interp_kernel, per_row, slots),
        out_shape=jax.ShapeDtypeStruct((3, groups * width), jnp.float32),
        in_specs=[vmem] * 7,
        out_specs=vmem,
        scratch_shapes=[pltpu.VMEM((block_x + 8, block_y + 8, KZ), jnp.float32)]
        + 2 * weight_scratch(groups, width),
        compiler_params=params,
        name="interp",
    )(offsets, zcell, fracs, live_q, potential, upper, beside)
    return (forces, total / ATOMS)


def solution(mesh):
    in_specs = (
        P(None, ("grp", "pen")),
        P(("grp", "pen")),
        P(None, ("grp", "pen")),
        P(("grp", "pen")),
        P(("grp", "pen")),
    )
    out_specs = (P(None, ("grp", "pen")), P())
    return jax.shard_map(local, mesh=mesh, in_specs=in_specs, out_specs=out_specs, check_vma=False)
```

```python
import functools
import math

import jax
import jax.numpy as jnp
import numpy as np
from jax import lax
from jax.experimental import pallas as pl
from jax.experimental.pallas import tpu as pltpu
from jax.sharding import PartitionSpec as P

KX = 256
KY = 256
KZ = 256
ATOMS = 1048576


ewald_split = 0.6
highest = lax.Precision.HIGH


def shifted(block, axis, distance):
    devices = range(lax.axis_size(axis))
    route = [((i - distance) % len(devices), i) for i in devices]
    return lax.ppermute(block, axis, route)


def spline_rows(fracs):
    values = [jnp.ones_like(fracs)]
    fifth = values
    for order in range(2, 7):
        nxt = []
        for j in range(order):
            term = jnp.zeros_like(fracs)
            if j >= 1:
                term = values[j - 1] * (fracs + order - 1 - j)
            if j <= order - 2:
                term = term + values[j] * (1.0 - fracs + j)
            nxt.append(term / (order - 1))
        if order == 5:
            fifth = nxt
        values = nxt
    slopes = []
    for j in range(6):
        term = jnp.zeros_like(fracs)
        if j >= 1:
            term = fifth[j - 1]
        if j <= 4:
            term = term - fifth[j]
        slopes.append(term)
    return (values, slopes)


def split(values):
    high = values.astype(jnp.bfloat16)
    low = (values - high.astype(jnp.float32)).astype(jnp.bfloat16)
    return (high, low)


def shift_rows(values, offset):
    none = jnp.zeros_like(values[0])
    return [
        jnp.where(offset == 0, first, second)
        for first, second in zip(values + [none], [none] + values)
    ]


def store_weights(outer, slots, off_ref, frac_ref, x_ref, y_ref, z_ref, which):
    groups, width = off_ref.shape[1], off_ref.shape[2]
    rows = pl.ds(pl.multiple_of(outer * 8, 8), 8)
    lane_tile = lax.broadcasted_iota(jnp.int32, (8, width), 1) // slots
    along_x = spline_rows(frac_ref[0, rows, :])[which]
    along_y = spline_rows(frac_ref[1, rows, :])[which]
    along_z = spline_rows(frac_ref[2, rows, :])[which]
    for k, value in enumerate(shift_rows(along_x, off_ref[0, rows, :])):
        x_ref[k, rows, :] = value
    for k, value in enumerate(along_z):
        z_ref[k, rows, :] = value
    near = shift_rows(along_y, off_ref[1, rows, :])
    none = jnp.zeros_like(near[0])
    for r in range(16):
        value = none
        for tile in range(4):
            if 0 <= r - 2 * tile < 7:
                value = jnp.where(lane_tile == tile, near[r - 2 * tile], value)
        for h in range(width // 128):
            start = (h * groups + outer * 8) * 16 + r
            y_ref[pl.ds(start, 8, stride=16), :] = value[:, 128 * h : 128 * h + 128]


def rows_of_y(y_ref, group, groups, width):
    parts = []
    for h in range(width // 128):
        start = pl.multiple_of((h * groups + group) * 16, 16)
        parts.append(y_ref[pl.ds(start, 16), :])
    return jnp.concatenate(parts, axis=1)


def z_window(base, values):
    fine = lax.broadcasted_iota(jnp.int32, (32, base.shape[1]), 0) - (base & 15)
    total = jnp.zeros(fine.shape, jnp.float32)
    for j in range(6):
        total = jnp.where(fine == j, values[j], total)
    return split(total)


def z_masks(base):
    coarse = jnp.broadcast_to(base // 16, (16, base.shape[1])).astype(jnp.int16)
    return [coarse == jnp.int16(k) for k in range(16)]


def z_weights(masks, window):
    halves_of = []
    for part in window:
        lower, upper = part[:16], part[16:]
        none = jnp.zeros_like(lower)
        blocks = []
        for k in range(16):
            block = jnp.where(masks[k - 1], upper, none)
            blocks.append(jnp.where(masks[k], lower, block))
        halves_of.append(jnp.concatenate(blocks, axis=0))
    return halves_of


def dot3(left, right, left_dim, right_dim):
    dims = (((left_dim,), (right_dim,)), ((), ()))
    one = functools.partial(
        lax.dot_general, dimension_numbers=dims, preferred_element_type=jnp.float32
    )
    return one(left[0], right[0]) + one(left[0], right[1]) + one(left[1], right[0])


def stacked_dot(left, right, left_dim, right_dim):
    dims = (((left_dim,), (right_dim,)), ((), ()))
    one = functools.partial(
        lax.dot_general, dimension_numbers=dims, preferred_element_type=jnp.float32
    )
    rows = left[0].shape[0]
    both = one(jnp.concatenate(left, axis=0), right[0])
    return both[:rows] + both[rows:] + one(left[0], right[1])


def spread_row(a, per_row, cell_ref, q_ref, x_ref, y_ref, z_ref, grid_ref):
    groups, width = cell_ref.shape
    outs = []
    for b in range(per_row):
        group = a * per_row + b
        base = cell_ref[pl.ds(group, 1), :]
        values = [z_ref[j, pl.ds(group, 1), :] for j in range(6)]
        weights = z_weights(z_masks(base), z_window(base, values))
        along_y = rows_of_y(y_ref, group, groups, width) * q_ref[pl.ds(group, 1), :]
        pair = [x_ref[k, pl.ds(group, 1), :] * along_y for k in range(7)]
        outs.append(stacked_dot(split(jnp.concatenate(pair, axis=0)), weights, 1, 1))
    for k in range(7):
        for t in range(per_row + 1):
            value = 0.0
            if t < per_row:
                value = outs[t][16 * k : 16 * k + 8]
            if t >= 1:
                value = value + outs[t - 1][16 * k + 8 : 16 * k + 16]
            grid_ref[2 * a + k, 8 * t : 8 * t + 8, :] += value


def interp_row(a, per_row, cell_ref, q_ref, plain, slope, ext_ref, out_ref):
    groups, width = cell_ref.shape
    for b in range(per_row):
        group = a * per_row + b
        row = pl.ds(group, 1)
        base = cell_ref[row, :]
        masks = z_masks(base)
        footing = jnp.concatenate(
            [ext_ref[2 * a + k, 8 * b : 8 * b + 16, :] for k in range(7)], axis=0
        )
        footing = split(footing)
        both = []
        for refs in (plain, slope):
            window = z_window(base, [refs[2][j, row, :] for j in range(6)])
            both.append(dot3(footing, z_weights(masks, window), 1, 0))
        main, tilt = both
        along_x = 0.0
        along_y = 0.0
        along_z = 0.0
        for k in range(7):
            weight, grade = plain[0][k, row, :], slope[0][k, row, :]
            piece = main[16 * k : 16 * k + 16]
            along_x = along_x + grade * piece
            along_y = along_y + weight * piece
            along_z = along_z + weight * tilt[16 * k : 16 * k + 16]
        weight_y = rows_of_y(plain[1], group, groups, width)
        grade_y = rows_of_y(slope[1], group, groups, width)
        minus_q = -q_ref[row, :]
        pieces = (along_x * weight_y, along_y * grade_y, along_z * weight_y)
        sums = [jnp.sum(piece, axis=0, keepdims=True) for piece in pieces]
        lanes = pl.ds(pl.multiple_of(group * width, width), width)
        out_ref[:, lanes] = minus_q * jnp.concatenate(sums, axis=0)


def weight_scratch(groups, width):
    return [
        pltpu.VMEM((7, groups, width), jnp.float32),
        pltpu.VMEM((groups * 16 * (width // 128), 128), jnp.float32),
        pltpu.VMEM((6, groups, width), jnp.float32),
    ]


def spread_kernel(per_row, slots, off_ref, z_ref, frac_ref, q_ref, grid_ref, *weights):
    grid_ref[...] = jnp.zeros_like(grid_ref)
    groups = z_ref.shape[0]

    def prepare(outer, carry):
        store_weights(outer, slots, off_ref, frac_ref, *weights, 0)
        return carry

    def step(a, carry):
        spread_row(a, per_row, z_ref, q_ref, *weights, grid_ref)
        return carry

    lax.fori_loop(0, groups // 8, prepare, 0)
    lax.fori_loop(0, groups // per_row, step, 0)


def interp_kernel(
    per_row, slots, off_ref, z_ref, frac_ref, q_ref, pot_ref, up_ref, side_ref, out_ref,
    ext_ref, *weights
):
    groups = z_ref.shape[0]
    size_z = pot_ref.shape[2]
    block_x, block_y = pot_ref.shape[0], pot_ref.shape[1]
    ext_ref[:block_x, :block_y] = pot_ref[...]
    ext_ref[block_x : block_x + 5, :block_y] = up_ref[...]
    ext_ref[block_x + 5 :, :block_y] = jnp.zeros((3, block_y, size_z), jnp.float32)
    ext_ref[: block_x + 5, block_y:] = side_ref[...]
    ext_ref[block_x + 5 :, block_y:] = jnp.zeros((3, 8, size_z), jnp.float32)

    def prepare(outer, carry):
        store_weights(outer, slots, off_ref, frac_ref, *weights[:3], 0)
        store_weights(outer, slots, off_ref, frac_ref, *weights[3:], 1)
        return carry

    def step(a, carry):
        interp_row(a, per_row, z_ref, q_ref, weights[:3], weights[3:], ext_ref, out_ref)
        return carry

    lax.fori_loop(0, groups // 8, prepare, 0)
    lax.fori_loop(0, groups // per_row, step, 0)


def modulus(index, length):
    coeffs = (1.0 / 120.0, 26.0 / 120.0, 66.0 / 120.0, 26.0 / 120.0, 1.0 / 120.0)
    real_part = 0.0
    imag_part = 0.0
    for j in range(5):
        angle = (index * j % length).astype(jnp.float32) * (2.0 * math.pi / length)
        real_part = real_part + coeffs[j] * jnp.cos(angle)
        imag_part = imag_part + coeffs[j] * jnp.sin(angle)
    return real_part * real_part + imag_part * imag_part


def influence(index_x, index_y, index_z):
    freq_x = jnp.where(2 * index_x < KX, index_x, index_x - KX).astype(jnp.float32) / KX
    freq_y = jnp.where(2 * index_y < KY, index_y, index_y - KY).astype(jnp.float32) / KY
    freq_z = jnp.where(2 * index_z < KZ, index_z, index_z - KZ).astype(jnp.float32) / KZ
    square = freq_x * freq_x + freq_y * freq_y + freq_z * freq_z
    safe = jnp.where(square > 0, square, 1.0)
    volume = float(KX * KY * KZ)
    value = jnp.exp(-math.pi**2 * safe / ewald_split**2) / (math.pi * volume * safe)
    value = value / (modulus(index_x, KX) * modulus(index_y, KY) * modulus(index_z, KZ))
    return jnp.where(square > 0, value, 0.0)


def waves(index, length):
    angle = (index % length) * (2.0 * math.pi / length)
    return (np.cos(angle), np.sin(angle))


def z_table(groups):
    planes = KZ // (2 * groups)
    frequency = np.arange(KZ // 2).reshape(groups, planes)
    cos, sin = waves(frequency[..., None] * np.arange(KZ), KZ)
    table = np.stack([cos, -sin], axis=1)
    table[0, 1, 0] = waves(np.arange(KZ) * (KZ // 2), KZ)[0]
    weight = np.full((groups, 2, planes), 2.0)
    weight[0, :, 0] = 1.0
    table = table.reshape(KZ, KZ)
    return (table.astype(np.float32), (table * weight.reshape(KZ, 1)).astype(np.float32))


def block_table(frequency, length, groups):
    position = np.arange(length)
    cos, sin = waves(frequency[..., None] * position, length)
    shape = (frequency.shape[0], frequency.shape[1], groups, length // groups)
    cos, sin = cos.reshape(shape), sin.reshape(shape)
    real_row = np.stack([cos, sin], axis=3)
    imag_row = np.stack([-sin, cos], axis=3)
    table = np.stack([real_row, imag_row], axis=1)
    return table.reshape(2 * length, 2 * length).astype(np.float32)


def y_frequency(groups):
    first = np.arange(KY // 2).reshape(groups, -1)
    second = np.where(first == 0, KY // 2, (KY - first) % KY)
    return np.concatenate([first, second], axis=1)


def partner_of(me, d, count):
    if count & (count - 1):
        return lax.rem(me + d, count)
    peer = me
    bit = 1
    while bit < count:
        if d & bit:
            peer = peer + bit - 2 * bit * lax.rem(lax.div(me, bit), 2)
        bit = 2 * bit
    return peer


def exchange_kernel(axis, count, *refs):
    arrays = (len(refs) - 3) // 2
    sources, targets = refs[:arrays], refs[arrays : 2 * arrays]
    send_sem, recv_sem, own_sem = refs[2 * arrays :]
    me = lax.axis_index(axis)
    barrier = pltpu.get_barrier_semaphore()
    for d in range(1, count):
        pl.semaphore_signal(
            barrier,
            inc=1,
            device_id={axis: partner_of(me, d, count)},
            device_id_type=pl.DeviceIdType.MESH,
        )
    pl.semaphore_wait(barrier, count - 1)
    copies = []
    for k in range(arrays):
        for d in range(1, count):
            peer = partner_of(me, d, count)
            copies.append(
                pltpu.make_async_remote_copy(
                    src_ref=sources[k].at[peer],
                    dst_ref=targets[k].at[me],
                    send_sem=send_sem.at[k, d],
                    recv_sem=recv_sem.at[k, d],
                    device_id={axis: peer},
                    device_id_type=pl.DeviceIdType.MESH,
                )
            )
        copies.append(
            pltpu.make_async_copy(sources[k].at[me], targets[k].at[me], own_sem.at[k])
        )
    for copy in copies:
        copy.start()
    for copy in copies:
        copy.wait()


def exchange(arrays, axis, number):
    count = lax.axis_size(axis)
    vmem = pl.BlockSpec(memory_space=pltpu.VMEM)
    return pl.pallas_call(
        functools.partial(exchange_kernel, axis, count),
        out_shape=[jax.ShapeDtypeStruct(array.shape, array.dtype) for array in arrays],
        in_specs=[vmem] * len(arrays),
        out_specs=[vmem] * len(arrays),
        scratch_shapes=[
            pltpu.SemaphoreType.DMA((len(arrays), count)),
            pltpu.SemaphoreType.DMA((len(arrays), count)),
            pltpu.SemaphoreType.DMA((len(arrays),)),
        ],
        compiler_params=pltpu.CompilerParams(collective_id=number, has_side_effects=True),
        name="exchange" + str(number),
    )(*arrays)


def dot(left, right, left_dim, right_dim):
    dims = (((left_dim,), (right_dim,)), ((), ()))
    return lax.dot_general(
        left, right, dims, precision=highest, preferred_element_type=jnp.float32
    )


def spectrum_of(grid, block_x, block_y):
    grp, pen = lax.axis_size("grp"), lax.axis_size("pen")
    planes = KZ // (2 * pen)
    lines = KY // grp
    half = lines // 2
    forward_z, backward_z = z_table(pen)
    order_y = y_frequency(grp)
    table_y = block_table(order_y, KY, pen)
    table_x = block_table(np.arange(KX)[None], KX, grp)
    lines_z = dot(forward_z, grid.reshape(block_x * block_y, KZ), 1, 1)
    lines_z = lines_z.reshape(pen, 2, planes, block_x, block_y).transpose(0, 1, 4, 2, 3)
    (columns,) = exchange(
        [lines_z.reshape(pen, 2 * block_y, planes * block_x)], "pen", 1
    )
    lines_y = dot(table_y, columns.reshape(2 * KY, planes * block_x), 1, 0)
    lines_y = lines_y.reshape(grp, 2, lines, planes, block_x).transpose(0, 1, 4, 3, 2)
    (rows,) = exchange([lines_y.reshape(grp, 2 * block_x, planes * lines)], "grp", 2)
    rows = rows.reshape(grp, 2, block_x, planes * lines)
    at_grp, at_pen = lax.axis_index("grp"), lax.axis_index("pen")
    packed = rows[..., :lines]
    alone = (at_grp == 0) & (jnp.arange(lines) % half == 0)
    partner = jnp.where(
        alone, packed, jnp.concatenate([packed[..., half:], packed[..., :half]], axis=-1)
    )
    a, b = packed[:, :1], packed[:, 1:]
    c, d = partner[:, :1], partner[:, 1:]
    whole = jnp.concatenate([a + c, b - d], axis=1) * 0.5
    midway = jnp.concatenate([b + d, c - a], axis=1) * 0.5
    origin = at_pen == 0
    whole = jnp.where(origin, whole, packed)
    midway = jnp.where(origin, midway, 0.0)
    total_lanes = (planes + 1) * lines
    full = jnp.concatenate([whole, rows[..., lines:], midway], axis=-1)
    spectrum = dot(table_x, full.reshape(2 * KX, total_lanes), 1, 0)
    spectrum = spectrum.reshape(2, KX, total_lanes)
    index_x = jnp.arange(KX, dtype=jnp.int32)[:, None]
    slot = jnp.arange(planes + 1, dtype=jnp.int32)
    index_z = jnp.where(slot < planes, at_pen * planes + slot, KZ // 2)
    plane_weight = jnp.where(
        slot < planes,
        jnp.where(origin & (slot == 0), 1.0, 2.0),
        jnp.where(origin, 1.0, 0.0),
    )
    index_z = jnp.repeat(index_z, lines)[None, :]
    plane_weight = jnp.repeat(plane_weight, lines)[None, :]
    index_y = lax.dynamic_index_in_dim(jnp.asarray(order_y, jnp.int32), at_grp, 0, False)
    index_y = jnp.tile(index_y, planes + 1)[None, :]
    kernel = influence(index_x, index_y, index_z)
    power = spectrum[0] * spectrum[0] + spectrum[1] * spectrum[1]
    spectral = 0.5 * jnp.sum(plane_weight * kernel * power)
    scaled = (spectrum * kernel).reshape(2 * KX, total_lanes)
    returning = dot(table_x, scaled, 0, 0).reshape(grp, 2, block_x, total_lanes)
    midway = returning[..., planes * lines :]
    turned = jnp.concatenate([-midway[:, 1:], midway[:, :1]], axis=1)
    returning = jnp.concatenate(
        [returning[..., :lines] + turned, returning[..., lines : planes * lines]], axis=-1
    )
    rows, sums = exchange(
        [
            returning.reshape(grp, 2 * block_x, planes * lines),
            jnp.broadcast_to(spectral, (grp, 8, 128)),
        ],
        "grp",
        3,
    )
    spectral = jnp.sum(sums[:, 0, 0])
    rows = rows.reshape(grp, 2, block_x, planes, lines).transpose(0, 1, 4, 3, 2)
    columns = dot(table_y, rows.reshape(2 * KY, planes * block_x), 0, 0)
    columns, sums = exchange(
        [
            columns.reshape(pen, 2 * block_y, planes * block_x),
            jnp.broadcast_to(spectral, (pen, 8, 128)),
        ],
        "pen",
        4,
    )
    spectral = jnp.sum(sums[:, 0, 0])
    home = columns.reshape(pen, 2, block_y, planes, block_x).transpose(0, 1, 3, 4, 2)
    potential = dot(home.reshape(KZ, block_x * block_y), backward_z, 0, 0)
    return (potential.reshape(block_x, block_y, KZ), spectral)


def cas_table(length):
    position = np.arange(length)
    cos, sin = waves(position[:, None] * position, length)
    return cos + sin


def halves(table):
    high = table.astype(jnp.bfloat16)
    low = (table - high.astype(np.float64)).astype(jnp.bfloat16)
    return (high, low)


def spline_factor(length):
    index = np.arange(length)
    freq = np.where(2 * index < length, index, index - length) / length
    coeffs = np.array([1.0, 26.0, 66.0, 26.0, 1.0]) / 120.0
    phase = np.exp(2j * np.pi * index[:, None] * np.arange(5) / length)
    modulus_square = np.abs(phase @ coeffs) ** 2
    square = freq**2
    factor = np.exp(-(math.pi**2) * square / ewald_split**2) / modulus_square
    return (factor.astype(np.float32), square.astype(np.float32))


def regroup(tiles, width):
    lane = lax.broadcasted_iota(jnp.int32, tiles[0].shape, 1) // width
    bit = 1
    while bit < len(tiles):
        keep = (lane // bit) % 2 == 0
        mixed = list(tiles)
        for i in range(len(tiles)):
            if not i & bit:
                first, second = tiles[i], tiles[i + bit]
                mixed[i] = jnp.where(keep, first, pltpu.roll(second, bit * width, 1))
                mixed[i + bit] = jnp.where(
                    keep, pltpu.roll(first, 128 - bit * width, 1), second
                )
        tiles = mixed
        bit = 2 * bit
    return tiles


def whole_kernel(
    grp, pen, slots, sizes, off_ref, cell_ref, frac_ref, q_ref, cas_hi, cas_lo, into_hi, into_lo,
    back_hi, back_lo, factor_row, factor_col, square_row, square_col, out_ref, energy_ref,
    pad, ext, plain_x, plain_y, plain_z, slope_x, slope_y, slope_z,
    send, recv, send_back, recv_back, work, sums, part,
    rim_side, rim_up, rim_corner, halo_side, halo_up, halo_corner,
    out_send, out_recv, back_send, back_recv, sum_send, sum_recv,
    side_send, side_recv, halo_send, halo_recv, edge_send, edge_recv,
):
    count = grp * pen
    slabs = len(sizes)
    starts = [sum(sizes[:s]) for s in range(slabs)]
    groups = cell_ref.shape[0]
    block_x, block_y = KX // grp, KY // pen
    tile_rows = block_x // 2
    per_row = groups // tile_rows
    fan = 128 // block_y
    half = pen // fan
    at_grp, at_pen = lax.axis_index("grp"), lax.axis_index("pen")
    me = at_grp * pen + at_pen
    plain = (plain_x, plain_y, plain_z)
    slope = (slope_x, slope_y, slope_z)
    cas = (cas_hi[...], cas_lo[...])

    def device(d_grp, d_pen):
        return {
            "grp": lax.rem(at_grp + d_grp + grp, grp),
            "pen": lax.rem(at_pen + d_pen + pen, pen),
        }

    def remote(source, target, sems, where):
        return pltpu.make_async_remote_copy(
            src_ref=source, dst_ref=target, send_sem=sems[0], recv_sem=sems[1],
            device_id=where, device_id_type=pl.DeviceIdType.MESH,
        )

    def peer_of(d):
        peer = lax.rem(me + d, count)
        return (peer, {"grp": lax.div(peer, pen), "pen": lax.rem(peer, pen)})

    first_hop = pen * (grp // 2 - lax.rem(at_grp, grp // 2))

    def fan_out(make):
        def one(e, carry):
            make(1 + lax.rem(e + first_hop - 1, count - 1)).start()
            return carry

        lax.fori_loop(0, count - 1, one, 0)

    others = pl.ds(0, count - 1)

    def slab_copy(s, source, target, sems):
        part_of = pl.ds(starts[s], sizes[s])
        pair = (sems[0].at[s], sems[1].at[s])

        def make(d):
            peer, where = peer_of(d)
            return remote(source.at[peer, part_of], target.at[me, part_of], pair, where)

        total = remote(
            source.at[others, part_of], target.at[others, part_of], pair, peer_of(1)[1]
        )
        return (make, total)

    def out_copy(s):
        return slab_copy(s, send, recv, (out_send, out_recv))

    def back_copy(s):
        return slab_copy(s, send_back, recv_back, (back_send, back_recv))

    def sum_copy():
        pair = (sum_send.at[0], sum_recv.at[0])
        total = remote(sums.at[others], sums.at[others], pair, peer_of(1)[1])
        return (lambda d: remote(part, sums.at[me], pair, peer_of(d)[1]), total)

    def slab_rows(s):
        return pl.ds(starts[s] * fan, sizes[s] * fan)

    def side_rim(s):
        source = pad.at[slab_rows(s), pl.ds(block_y, 8), :]
        return remote(source, rim_side.at[slab_rows(s)], (side_send.at[s], side_recv.at[s]), device(0, 1))

    def edge_rims():
        source = pad.at[pl.ds(block_x, 5)]
        return [
            remote(
                source.at[:, pl.ds(0, block_y), :], rim_up,
                (edge_send.at[0], edge_recv.at[0]), device(1, 0),
            ),
            remote(
                source.at[:, pl.ds(block_y, 8), :], rim_corner,
                (edge_send.at[1], edge_recv.at[1]), device(1, 1),
            ),
        ]

    def side_halo(s):
        source = ext.at[slab_rows(s), pl.ds(0, 8), :]
        return remote(source, halo_side.at[slab_rows(s)], (halo_send.at[s], halo_recv.at[s]), device(0, -1))

    def edge_halos():
        source = ext.at[pl.ds(0, 5)]
        return [
            remote(
                source.at[:, pl.ds(0, block_y), :], halo_up,
                (edge_send.at[2], edge_recv.at[2]), device(-1, 0),
            ),
            remote(
                source.at[:, pl.ds(0, 8), :], halo_corner,
                (edge_send.at[3], edge_recv.at[3]), device(-1, -1),
            ),
        ]

    barrier = pltpu.get_barrier_semaphore()

    def greet(d, carry):
        pl.semaphore_signal(
            barrier, inc=1, device_id=peer_of(d)[1], device_id_type=pl.DeviceIdType.MESH
        )
        return carry

    lax.fori_loop(1, count, greet, 0)
    pad[...] = jnp.zeros_like(pad)

    def ship(s):
        side_rim(s).wait_recv()
        pad[slab_rows(s), pl.ds(0, 8), :] += rim_side[slab_rows(s)]

    def transform_out(s):
        def along_z(i, carry):
            tile = starts[s] + 2 * i
            rows = pad[pl.ds(tile * fan, 2 * fan), pl.ds(0, block_y), :]
            out = dot3(cas, split(rows.reshape(256, KZ)), 1, 1)
            for t in range(2):
                block = out[:, 128 * t : 128 * t + 128].reshape(count, 8, 128)
                send[:, tile + t] = block
            return carry

        lax.fori_loop(0, sizes[s] // 2, along_z, 0)
        fan_out(out_copy(s)[0])
        own = pl.ds(starts[s], sizes[s])
        recv[me, own] = send[me, own]

    ready = [max((start * fan - 5) // 2, 0) for start in starts]
    rows_per_outer = 8 // per_row

    def spread_plain(i, carry):
        a = tile_rows - 1 - i

        @pl.when(lax.rem(i, rows_per_outer) == 0)
        def _():
            outer = lax.div(a, rows_per_outer)
            store_weights(outer, slots, off_ref, frac_ref, *plain, 0)

        spread_row(a, per_row, cell_ref, q_ref, *plain, pad)
        return carry

    def spread_step(i, carry):
        a = tile_rows - 1 - i
        spread_plain(i, carry)

        @pl.when(a == ready[-1])
        def _():
            for copy in edge_rims():
                copy.start()

        for s in range(slabs):

            @pl.when(a == ready[s])
            def _(s=s):
                side_rim(s).start()

            if s:

                @pl.when(a == max(ready[s] - 5, 0))
                def _(s=s):
                    ship(s)
                    transform_out(s)

        return carry

    alone = tile_rows - 1 - ready[-1]
    lax.fori_loop(0, alone, spread_plain, 0)
    pl.semaphore_wait(barrier, count - 1)
    lax.fori_loop(alone, tile_rows, spread_step, 0)
    for copy in edge_rims():
        copy.wait_recv()
    ship(0)
    pad[:5, :block_y, :] += rim_up[...]
    pad[:5, :8, :] += rim_corner[...]
    transform_out(0)

    def prepare_slopes(outer, carry):
        store_weights(outer, slots, off_ref, frac_ref, *slope, 1)
        return carry

    lax.fori_loop(0, groups // 8, prepare_slopes, 0)

    def slab_lines(s, h):
        span = sizes[s] * 8 * KX // (block_x // fan)
        return pl.ds(starts[s] * 8 * KX // (block_x // fan) + h * 8 * KX, span)

    for s in reversed(range(slabs)):
        out_copy(s)[1].wait_recv()
        rows = []
        own = pl.ds(starts[s], sizes[s])
        for g in range(grp):
            parts = [[] for _ in range(fan)]
            for h in range(half):
                loaded = [
                    recv[g * pen + h * fan + k, own].reshape(8 * sizes[s], 128)
                    for k in range(fan)
                ]
                for k, tile in enumerate(regroup(loaded, block_y)):
                    parts[k].append(tile)
            rows += [jnp.concatenate(pieces, axis=1) for pieces in parts]
        out = dot3(split(jnp.concatenate(rows, axis=0)), cas, 1, 0)
        for h in range(2):
            work[slab_lines(s, h), :] = out[:, 128 * h : 128 * h + 128]

    scale = 1.0 / (math.pi * KX * KY * KZ)
    first = pl.multiple_of(8 * me, 8)
    factor_z = factor_col[pl.ds(first, 8), :]
    square_z = square_col[pl.ds(first, 8), :]
    pick = lax.broadcasted_iota(jnp.int32, (8, 1), 0)

    def along_x(i, total):
        for f in (2 * i, 2 * i + 1):
            chosen = pick == f
            fz = jnp.sum(jnp.where(chosen, factor_z, 0.0), axis=0, keepdims=True) * scale
            sz = jnp.sum(jnp.where(chosen, square_z, 0.0), axis=0, keepdims=True)
            rows = jnp.concatenate(
                [work[pl.ds(f + h * 8 * KX, KX, stride=8), :] for h in range(2)], axis=1
            )
            spectrum = dot3((into_hi[...], into_lo[...]), split(rows), 1, 0)
            square = square_col[...] + (square_row[...] + sz)
            safe = jnp.where(square > 0, square, 1.0)
            kernel = factor_col[...] * (factor_row[...] * fz) / safe
            kernel = jnp.where(square > 0, kernel, 0.0)
            scaled = kernel * spectrum
            total = total + jnp.sum(scaled * spectrum, axis=0, keepdims=True)
            out = dot3((back_hi[...], back_lo[...]), split(scaled), 1, 0)
            for h in range(2):
                rows = pl.ds(f + h * 8 * KX, KX, stride=8)
                work[rows, :] = out[:, 128 * h : 128 * h + 128]
        return total

    total = lax.fori_loop(0, 4, along_x, jnp.zeros((1, KY), jnp.float32))
    part[...] = jnp.broadcast_to(0.5 * jnp.sum(total, axis=1, keepdims=True), (1, 128))
    sums[me] = part[...]

    for s in range(slabs):
        rows = jnp.concatenate([work[slab_lines(s, h), :] for h in range(2)], axis=1)
        out = dot3(split(rows), cas, 1, 0)
        lines = 8 * sizes[s]
        own = pl.ds(starts[s], sizes[s])
        for g in range(grp):
            for h in range(half):
                parts = []
                for k in range(fan):
                    start = (g * fan + k) * lines
                    parts.append(out[start : start + lines, 128 * h : 128 * h + 128])
                for k, tile in enumerate(regroup(parts, block_y)):
                    send_back[g * pen + h * fan + k, own] = tile.reshape(sizes[s], 8, 128)
        recv_back[me, own] = send_back[me, own]
        if s == 0:
            fan_out(back_copy(s)[0])
    fan_out(sum_copy()[0])

    def home(s):
        back_copy(s)[1].wait_recv()
        if s + 1 < slabs:
            fan_out(back_copy(s + 1)[0])

        def home_z(i, inner):
            tile = starts[s] + 2 * i
            rows = jnp.concatenate(
                [recv_back[:, tile + t].reshape(KZ, 128) for t in range(2)], axis=1
            )
            out = dot3(split(jnp.transpose(rows)), cas, 1, 0)
            where = pl.ds(tile * fan, 2 * fan)
            ext[where, pl.ds(0, block_y), :] = out.reshape(2 * fan, block_y, KZ)
            return inner

        lax.fori_loop(0, sizes[s] // 2, home_z, 0)
        side_halo(s).start()

    def join_halo(s):
        side_halo(s).wait_recv()
        ext[slab_rows(s), pl.ds(block_y, 8), :] = halo_side[slab_rows(s)]

    home(0)
    for copy in edge_halos():
        copy.start()
    needed = [max((start * fan - 5) // 2, 0) for start in starts]
    early = [0] + [min(needed[s], 3) for s in range(1, slabs)]
    early[-1] = min(needed[-1], 5)

    def interp_step(a, carry):
        for s in range(1, slabs):

            @pl.when(a == needed[s] - early[s])
            def _(s=s):
                home(s)

        for s in range(slabs):

            @pl.when(a == needed[s])
            def _(s=s):
                join_halo(s)

        @pl.when(a == tile_rows - 3)
        def _():
            for copy in edge_halos():
                copy.wait_recv()
            ext[pl.ds(block_x, 5), pl.ds(0, block_y), :] = halo_up[...]
            ext[pl.ds(block_x, 5), pl.ds(block_y, 8), :] = halo_corner[...]

        interp_row(a, per_row, cell_ref, q_ref, plain, slope, ext, out_ref)
        return carry

    lax.fori_loop(0, tile_rows, interp_step, 0)
    sum_copy()[1].wait_recv()
    energy_ref[...] = jnp.sum(sums[...], axis=0)
    sum_copy()[1].wait_send()

    for s in range(slabs):
        out_copy(s)[1].wait_send()
        back_copy(s)[1].wait_send()
        side_rim(s).wait_send()
        side_halo(s).wait_send()
    for copy in edge_rims() + edge_halos():
        copy.wait_send()


def whole_program(offsets, zcell, fracs, live_q, slots, grp, pen, sizes):
    count = grp * pen
    groups, width = zcell.shape
    block_x, block_y = KX // grp, KY // pen
    fan = 128 // block_y
    slabs = len(sizes)
    cas = cas_table(KZ)
    cells = np.arange(KX).reshape(grp, block_x // fan, fan)
    order = np.concatenate(
        [
            cells[:, sum(sizes[:s]) : sum(sizes[: s + 1])].transpose(0, 2, 1).reshape(-1)
            for s in range(slabs)
        ]
    )
    factor, square = spline_factor(KX)
    tables = [*halves(cas), *halves(cas[:, order]), *halves(cas[order, :])]
    tables += [factor[None, :], factor[:, None], square[None, :], square[:, None]]
    tables = [jnp.asarray(table) for table in tables]
    vmem = pl.BlockSpec(memory_space=pltpu.VMEM)

    def held(*shape):
        return pltpu.VMEM(shape, jnp.float32)

    traffic = held(count, block_x // fan, 8, 128)
    dma = pltpu.SemaphoreType.DMA
    forces, energy = pl.pallas_call(
        functools.partial(whole_kernel, grp, pen, slots, sizes),
        out_shape=[
            jax.ShapeDtypeStruct((3, groups * width), jnp.float32),
            jax.ShapeDtypeStruct((1, 128), jnp.float32),
        ],
        in_specs=[vmem] * (4 + len(tables)),
        out_specs=[vmem] * 2,
        scratch_shapes=[
            held(block_x + 8, block_y + 8, KZ),
            held(block_x + 8, block_y + 8, KZ),
            *weight_scratch(groups, width),
            *weight_scratch(groups, width),
            traffic, traffic, traffic, traffic,
            held(16 * KX, 128),
            held(count, 1, 128),
            held(1, 128),
            held(block_x, 8, KZ), held(5, block_y, KZ), held(5, 8, KZ),
            held(block_x, 8, KZ), held(5, block_y, KZ), held(5, 8, KZ),
            dma((slabs,)), dma((slabs,)), dma((slabs,)), dma((slabs,)),
            dma((1,)), dma((1,)),
            dma((slabs,)), dma((slabs,)), dma((slabs,)), dma((slabs,)),
            dma((4,)), dma((4,)),
        ],
        compiler_params=pltpu.CompilerParams(
            collective_id=1, has_side_effects=True, vmem_limit_bytes=60 * 1024 * 1024
        ),
        name="whole",
    )(offsets, zcell, fracs, live_q, *tables)
    return (forces, energy[0, 0])


def slab_fits(grp, pen, sizes, block_x, block_y, per_row):
    fan = 128 // block_y
    return (
        grp * pen * 8 == KZ and KX == KY and KY == KZ and KZ == 256 and pen % fan == 0
        and block_x == fan * sum(sizes) and per_row * 8 == block_y and 8 % per_row == 0
    )


def local(cell_offsets, cell_z, frac, charges, tile_counts):
    block_x = KX // lax.axis_size("grp")
    block_y = KY // lax.axis_size("pen")
    tiles = tile_counts.shape[0]
    slots = charges.shape[0] // tiles
    width = 4 * slots
    groups = tiles // 4
    per_row = block_y // 8
    live = jnp.arange(slots, dtype=jnp.int32)[None, :] < tile_counts[:, None]
    live_q = (charges.reshape(tiles, slots) * live.astype(jnp.float32)).reshape(groups, width)
    offsets = cell_offsets.reshape(2, groups, width)
    zcell = cell_z.reshape(groups, width)
    fracs = frac.reshape(3, groups, width)
    grp, pen = lax.axis_size("grp"), lax.axis_size("pen")
    sizes = (6, 4, 4, 2)
    if slab_fits(grp, pen, sizes, block_x, block_y, per_row):
        forces, total = whole_program(offsets, zcell, fracs, live_q, slots, grp, pen, sizes)
        return (forces, total / ATOMS)
    vmem = pl.BlockSpec(memory_space=pltpu.VMEM)
    params = pltpu.CompilerParams(vmem_limit_bytes=60 * 1024 * 1024)
    padded = pl.pallas_call(
        functools.partial(spread_kernel, per_row, slots),
        out_shape=jax.ShapeDtypeStruct((block_x + 8, block_y + 8, KZ), jnp.float32),
        in_specs=[vmem] * 4,
        out_specs=vmem,
        scratch_shapes=weight_scratch(groups, width),
        compiler_params=params,
        name="spread",
    )(offsets, zcell, fracs, live_q)
    rim_y = shifted(padded[: block_x + 5, block_y : block_y + 5], "pen", 1)
    merged = padded[: block_x + 5, :block_y].at[:, :5].add(rim_y)
    rim_x = shifted(merged[block_x : block_x + 5], "grp", 1)
    grid = merged[:block_x] + jnp.pad(rim_x, ((0, block_x - 5), (0, 0), (0, 0)))
    potential, total = spectrum_of(grid, block_x, block_y)
    upper = shifted(potential[:5], "grp", -1)
    ext_x = jnp.concatenate([potential[:, :5], upper[:, :5]], axis=0)
    beside = shifted(ext_x, "pen", -1)
    beside = jnp.pad(beside, ((0, 0), (0, 3), (0, 0)))
    forces = pl.pallas_call(
        functools.partial(interp_kernel, per_row, slots),
        out_shape=jax.ShapeDtypeStruct((3, groups * width), jnp.float32),
        in_specs=[vmem] * 7,
        out_specs=vmem,
        scratch_shapes=[pltpu.VMEM((block_x + 8, block_y + 8, KZ), jnp.float32)]
        + 2 * weight_scratch(groups, width),
        compiler_params=params,
        name="interp",
    )(offsets, zcell, fracs, live_q, potential, upper, beside)
    return (forces, total / ATOMS)


def solution(mesh):
    in_specs = (
        P(None, ("grp", "pen")),
        P(("grp", "pen")),
        P(None, ("grp", "pen")),
        P(("grp", "pen")),
        P(("grp", "pen")),
    )
    out_specs = (P(None, ("grp", "pen")), P())
    return jax.shard_map(local, mesh=mesh, in_specs=in_specs, out_specs=out_specs, check_vma=False)
```

```python
import functools
import math

import jax
import jax.numpy as jnp
import numpy as np
from jax import lax
from jax.experimental import pallas as pl
from jax.experimental.pallas import tpu as pltpu
from jax.sharding import PartitionSpec as P

KX = 256
KY = 256
KZ = 256
ATOMS = 1048576


ewald_split = 0.6
highest = lax.Precision.HIGH


def shifted(block, axis, distance):
    devices = range(lax.axis_size(axis))
    route = [((i - distance) % len(devices), i) for i in devices]
    return lax.ppermute(block, axis, route)


def spline_rows(fracs):
    values = [jnp.ones_like(fracs)]
    fifth = values
    for order in range(2, 7):
        nxt = []
        for j in range(order):
            term = jnp.zeros_like(fracs)
            if j >= 1:
                term = values[j - 1] * (fracs + order - 1 - j)
            if j <= order - 2:
                term = term + values[j] * (1.0 - fracs + j)
            nxt.append(term / (order - 1))
        if order == 5:
            fifth = nxt
        values = nxt
    slopes = []
    for j in range(6):
        term = jnp.zeros_like(fracs)
        if j >= 1:
            term = fifth[j - 1]
        if j <= 4:
            term = term - fifth[j]
        slopes.append(term)
    return (values, slopes)


def split(values):
    high = values.astype(jnp.bfloat16)
    low = (values - high.astype(jnp.float32)).astype(jnp.bfloat16)
    return (high, low)


def shift_rows(values, offset):
    none = jnp.zeros_like(values[0])
    return [
        jnp.where(offset == 0, first, second)
        for first, second in zip(values + [none], [none] + values)
    ]


def store_weights(outer, slots, off_ref, frac_ref, x_ref, y_ref, z_ref, which):
    groups, width = off_ref.shape[1], off_ref.shape[2]
    rows = pl.ds(pl.multiple_of(outer * 8, 8), 8)
    lane_tile = lax.broadcasted_iota(jnp.int32, (8, width), 1) // slots
    along_x = spline_rows(frac_ref[0, rows, :])[which]
    along_y = spline_rows(frac_ref[1, rows, :])[which]
    along_z = spline_rows(frac_ref[2, rows, :])[which]
    for k, value in enumerate(shift_rows(along_x, off_ref[0, rows, :])):
        x_ref[k, rows, :] = value
    for k, value in enumerate(along_z):
        z_ref[k, rows, :] = value
    near = shift_rows(along_y, off_ref[1, rows, :])
    none = jnp.zeros_like(near[0])
    for r in range(16):
        value = none
        for tile in range(4):
            if 0 <= r - 2 * tile < 7:
                value = jnp.where(lane_tile == tile, near[r - 2 * tile], value)
        for h in range(width // 128):
            start = (h * groups + outer * 8) * 16 + r
            y_ref[pl.ds(start, 8, stride=16), :] = value[:, 128 * h : 128 * h + 128]


def rows_of_y(y_ref, group, groups, width):
    parts = []
    for h in range(width // 128):
        start = pl.multiple_of((h * groups + group) * 16, 16)
        parts.append(y_ref[pl.ds(start, 16), :])
    return jnp.concatenate(parts, axis=1)


def z_window(base, values):
    fine = lax.broadcasted_iota(jnp.int32, (32, base.shape[1]), 0) - (base & 15)
    total = jnp.zeros(fine.shape, jnp.float32)
    for j in range(6):
        total = jnp.where(fine == j, values[j], total)
    return split(total)


def z_masks(base):
    coarse = jnp.broadcast_to(base // 16, (16, base.shape[1])).astype(jnp.int16)
    return [coarse == jnp.int16(k) for k in range(16)]


def z_weights(masks, window):
    halves_of = []
    for part in window:
        lower, upper = part[:16], part[16:]
        none = jnp.zeros_like(lower)
        blocks = []
        for k in range(16):
            block = jnp.where(masks[k - 1], upper, none)
            blocks.append(jnp.where(masks[k], lower, block))
        halves_of.append(jnp.concatenate(blocks, axis=0))
    return halves_of


def dot3(left, right, left_dim, right_dim):
    dims = (((left_dim,), (right_dim,)), ((), ()))
    one = functools.partial(
        lax.dot_general, dimension_numbers=dims, preferred_element_type=jnp.float32
    )
    return one(left[0], right[0]) + one(left[0], right[1]) + one(left[1], right[0])


def stacked_dot(left, right, left_dim, right_dim):
    dims = (((left_dim,), (right_dim,)), ((), ()))
    one = functools.partial(
        lax.dot_general, dimension_numbers=dims, preferred_element_type=jnp.float32
    )
    rows = left[0].shape[0]
    both = one(jnp.concatenate(left, axis=0), right[0])
    return both[:rows] + both[rows:] + one(left[0], right[1])


def spread_row(a, per_row, cell_ref, q_ref, x_ref, y_ref, z_ref, grid_ref):
    groups, width = cell_ref.shape
    outs = []
    for b in range(per_row):
        group = a * per_row + b
        base = cell_ref[pl.ds(group, 1), :]
        values = [z_ref[j, pl.ds(group, 1), :] for j in range(6)]
        weights = z_weights(z_masks(base), z_window(base, values))
        along_y = rows_of_y(y_ref, group, groups, width) * q_ref[pl.ds(group, 1), :]
        pair = [x_ref[k, pl.ds(group, 1), :] * along_y for k in range(7)]
        outs.append(stacked_dot(split(jnp.concatenate(pair, axis=0)), weights, 1, 1))
    for k in range(7):
        for t in range(per_row + 1):
            value = 0.0
            if t < per_row:
                value = outs[t][16 * k : 16 * k + 8]
            if t >= 1:
                value = value + outs[t - 1][16 * k + 8 : 16 * k + 16]
            grid_ref[2 * a + k, 8 * t : 8 * t + 8, :] += value


def interp_row(a, per_row, cell_ref, q_ref, plain, slope, ext_ref, out_ref):
    groups, width = cell_ref.shape
    for b in range(per_row):
        group = a * per_row + b
        row = pl.ds(group, 1)
        base = cell_ref[row, :]
        masks = z_masks(base)
        footing = jnp.concatenate(
            [ext_ref[2 * a + k, 8 * b : 8 * b + 16, :] for k in range(7)], axis=0
        )
        footing = split(footing)
        both = []
        for refs in (plain, slope):
            window = z_window(base, [refs[2][j, row, :] for j in range(6)])
            both.append(dot3(footing, z_weights(masks, window), 1, 0))
        main, tilt = both
        along_x = 0.0
        along_y = 0.0
        along_z = 0.0
        for k in range(7):
            weight, grade = plain[0][k, row, :], slope[0][k, row, :]
            piece = main[16 * k : 16 * k + 16]
            along_x = along_x + grade * piece
            along_y = along_y + weight * piece
            along_z = along_z + weight * tilt[16 * k : 16 * k + 16]
        weight_y = rows_of_y(plain[1], group, groups, width)
        grade_y = rows_of_y(slope[1], group, groups, width)
        minus_q = -q_ref[row, :]
        pieces = (along_x * weight_y, along_y * grade_y, along_z * weight_y)
        sums = [jnp.sum(piece, axis=0, keepdims=True) for piece in pieces]
        lanes = pl.ds(pl.multiple_of(group * width, width), width)
        out_ref[:, lanes] = minus_q * jnp.concatenate(sums, axis=0)


def weight_scratch(groups, width):
    return [
        pltpu.VMEM((7, groups, width), jnp.float32),
        pltpu.VMEM((groups * 16 * (width // 128), 128), jnp.float32),
        pltpu.VMEM((6, groups, width), jnp.float32),
    ]


def spread_kernel(per_row, slots, off_ref, z_ref, frac_ref, q_ref, grid_ref, *weights):
    grid_ref[...] = jnp.zeros_like(grid_ref)
    groups = z_ref.shape[0]

    def prepare(outer, carry):
        store_weights(outer, slots, off_ref, frac_ref, *weights, 0)
        return carry

    def step(a, carry):
        spread_row(a, per_row, z_ref, q_ref, *weights, grid_ref)
        return carry

    lax.fori_loop(0, groups // 8, prepare, 0)
    lax.fori_loop(0, groups // per_row, step, 0)


def interp_kernel(
    per_row, slots, off_ref, z_ref, frac_ref, q_ref, pot_ref, up_ref, side_ref, out_ref,
    ext_ref, *weights
):
    groups = z_ref.shape[0]
    size_z = pot_ref.shape[2]
    block_x, block_y = pot_ref.shape[0], pot_ref.shape[1]
    ext_ref[:block_x, :block_y] = pot_ref[...]
    ext_ref[block_x : block_x + 5, :block_y] = up_ref[...]
    ext_ref[block_x + 5 :, :block_y] = jnp.zeros((3, block_y, size_z), jnp.float32)
    ext_ref[: block_x + 5, block_y:] = side_ref[...]
    ext_ref[block_x + 5 :, block_y:] = jnp.zeros((3, 8, size_z), jnp.float32)

    def prepare(outer, carry):
        store_weights(outer, slots, off_ref, frac_ref, *weights[:3], 0)
        store_weights(outer, slots, off_ref, frac_ref, *weights[3:], 1)
        return carry

    def step(a, carry):
        interp_row(a, per_row, z_ref, q_ref, weights[:3], weights[3:], ext_ref, out_ref)
        return carry

    lax.fori_loop(0, groups // 8, prepare, 0)
    lax.fori_loop(0, groups // per_row, step, 0)


def modulus(index, length):
    coeffs = (1.0 / 120.0, 26.0 / 120.0, 66.0 / 120.0, 26.0 / 120.0, 1.0 / 120.0)
    real_part = 0.0
    imag_part = 0.0
    for j in range(5):
        angle = (index * j % length).astype(jnp.float32) * (2.0 * math.pi / length)
        real_part = real_part + coeffs[j] * jnp.cos(angle)
        imag_part = imag_part + coeffs[j] * jnp.sin(angle)
    return real_part * real_part + imag_part * imag_part


def influence(index_x, index_y, index_z):
    freq_x = jnp.where(2 * index_x < KX, index_x, index_x - KX).astype(jnp.float32) / KX
    freq_y = jnp.where(2 * index_y < KY, index_y, index_y - KY).astype(jnp.float32) / KY
    freq_z = jnp.where(2 * index_z < KZ, index_z, index_z - KZ).astype(jnp.float32) / KZ
    square = freq_x * freq_x + freq_y * freq_y + freq_z * freq_z
    safe = jnp.where(square > 0, square, 1.0)
    volume = float(KX * KY * KZ)
    value = jnp.exp(-math.pi**2 * safe / ewald_split**2) / (math.pi * volume * safe)
    value = value / (modulus(index_x, KX) * modulus(index_y, KY) * modulus(index_z, KZ))
    return jnp.where(square > 0, value, 0.0)


def waves(index, length):
    angle = (index % length) * (2.0 * math.pi / length)
    return (np.cos(angle), np.sin(angle))


def z_table(groups):
    planes = KZ // (2 * groups)
    frequency = np.arange(KZ // 2).reshape(groups, planes)
    cos, sin = waves(frequency[..., None] * np.arange(KZ), KZ)
    table = np.stack([cos, -sin], axis=1)
    table[0, 1, 0] = waves(np.arange(KZ) * (KZ // 2), KZ)[0]
    weight = np.full((groups, 2, planes), 2.0)
    weight[0, :, 0] = 1.0
    table = table.reshape(KZ, KZ)
    return (table.astype(np.float32), (table * weight.reshape(KZ, 1)).astype(np.float32))


def block_table(frequency, length, groups):
    position = np.arange(length)
    cos, sin = waves(frequency[..., None] * position, length)
    shape = (frequency.shape[0], frequency.shape[1], groups, length // groups)
    cos, sin = cos.reshape(shape), sin.reshape(shape)
    real_row = np.stack([cos, sin], axis=3)
    imag_row = np.stack([-sin, cos], axis=3)
    table = np.stack([real_row, imag_row], axis=1)
    return table.reshape(2 * length, 2 * length).astype(np.float32)


def y_frequency(groups):
    first = np.arange(KY // 2).reshape(groups, -1)
    second = np.where(first == 0, KY // 2, (KY - first) % KY)
    return np.concatenate([first, second], axis=1)


def partner_of(me, d, count):
    if count & (count - 1):
        return lax.rem(me + d, count)
    peer = me
    bit = 1
    while bit < count:
        if d & bit:
            peer = peer + bit - 2 * bit * lax.rem(lax.div(me, bit), 2)
        bit = 2 * bit
    return peer


def exchange_kernel(axis, count, *refs):
    arrays = (len(refs) - 3) // 2
    sources, targets = refs[:arrays], refs[arrays : 2 * arrays]
    send_sem, recv_sem, own_sem = refs[2 * arrays :]
    me = lax.axis_index(axis)
    barrier = pltpu.get_barrier_semaphore()
    for d in range(1, count):
        pl.semaphore_signal(
            barrier,
            inc=1,
            device_id={axis: partner_of(me, d, count)},
            device_id_type=pl.DeviceIdType.MESH,
        )
    pl.semaphore_wait(barrier, count - 1)
    copies = []
    for k in range(arrays):
        for d in range(1, count):
            peer = partner_of(me, d, count)
            copies.append(
                pltpu.make_async_remote_copy(
                    src_ref=sources[k].at[peer],
                    dst_ref=targets[k].at[me],
                    send_sem=send_sem.at[k, d],
                    recv_sem=recv_sem.at[k, d],
                    device_id={axis: peer},
                    device_id_type=pl.DeviceIdType.MESH,
                )
            )
        copies.append(
            pltpu.make_async_copy(sources[k].at[me], targets[k].at[me], own_sem.at[k])
        )
    for copy in copies:
        copy.start()
    for copy in copies:
        copy.wait()


def exchange(arrays, axis, number):
    count = lax.axis_size(axis)
    vmem = pl.BlockSpec(memory_space=pltpu.VMEM)
    return pl.pallas_call(
        functools.partial(exchange_kernel, axis, count),
        out_shape=[jax.ShapeDtypeStruct(array.shape, array.dtype) for array in arrays],
        in_specs=[vmem] * len(arrays),
        out_specs=[vmem] * len(arrays),
        scratch_shapes=[
            pltpu.SemaphoreType.DMA((len(arrays), count)),
            pltpu.SemaphoreType.DMA((len(arrays), count)),
            pltpu.SemaphoreType.DMA((len(arrays),)),
        ],
        compiler_params=pltpu.CompilerParams(collective_id=number, has_side_effects=True),
        name="exchange" + str(number),
    )(*arrays)


def dot(left, right, left_dim, right_dim):
    dims = (((left_dim,), (right_dim,)), ((), ()))
    return lax.dot_general(
        left, right, dims, precision=highest, preferred_element_type=jnp.float32
    )


def spectrum_of(grid, block_x, block_y):
    grp, pen = lax.axis_size("grp"), lax.axis_size("pen")
    planes = KZ // (2 * pen)
    lines = KY // grp
    half = lines // 2
    forward_z, backward_z = z_table(pen)
    order_y = y_frequency(grp)
    table_y = block_table(order_y, KY, pen)
    table_x = block_table(np.arange(KX)[None], KX, grp)
    lines_z = dot(forward_z, grid.reshape(block_x * block_y, KZ), 1, 1)
    lines_z = lines_z.reshape(pen, 2, planes, block_x, block_y).transpose(0, 1, 4, 2, 3)
    (columns,) = exchange(
        [lines_z.reshape(pen, 2 * block_y, planes * block_x)], "pen", 1
    )
    lines_y = dot(table_y, columns.reshape(2 * KY, planes * block_x), 1, 0)
    lines_y = lines_y.reshape(grp, 2, lines, planes, block_x).transpose(0, 1, 4, 3, 2)
    (rows,) = exchange([lines_y.reshape(grp, 2 * block_x, planes * lines)], "grp", 2)
    rows = rows.reshape(grp, 2, block_x, planes * lines)
    at_grp, at_pen = lax.axis_index("grp"), lax.axis_index("pen")
    packed = rows[..., :lines]
    alone = (at_grp == 0) & (jnp.arange(lines) % half == 0)
    partner = jnp.where(
        alone, packed, jnp.concatenate([packed[..., half:], packed[..., :half]], axis=-1)
    )
    a, b = packed[:, :1], packed[:, 1:]
    c, d = partner[:, :1], partner[:, 1:]
    whole = jnp.concatenate([a + c, b - d], axis=1) * 0.5
    midway = jnp.concatenate([b + d, c - a], axis=1) * 0.5
    origin = at_pen == 0
    whole = jnp.where(origin, whole, packed)
    midway = jnp.where(origin, midway, 0.0)
    total_lanes = (planes + 1) * lines
    full = jnp.concatenate([whole, rows[..., lines:], midway], axis=-1)
    spectrum = dot(table_x, full.reshape(2 * KX, total_lanes), 1, 0)
    spectrum = spectrum.reshape(2, KX, total_lanes)
    index_x = jnp.arange(KX, dtype=jnp.int32)[:, None]
    slot = jnp.arange(planes + 1, dtype=jnp.int32)
    index_z = jnp.where(slot < planes, at_pen * planes + slot, KZ // 2)
    plane_weight = jnp.where(
        slot < planes,
        jnp.where(origin & (slot == 0), 1.0, 2.0),
        jnp.where(origin, 1.0, 0.0),
    )
    index_z = jnp.repeat(index_z, lines)[None, :]
    plane_weight = jnp.repeat(plane_weight, lines)[None, :]
    index_y = lax.dynamic_index_in_dim(jnp.asarray(order_y, jnp.int32), at_grp, 0, False)
    index_y = jnp.tile(index_y, planes + 1)[None, :]
    kernel = influence(index_x, index_y, index_z)
    power = spectrum[0] * spectrum[0] + spectrum[1] * spectrum[1]
    spectral = 0.5 * jnp.sum(plane_weight * kernel * power)
    scaled = (spectrum * kernel).reshape(2 * KX, total_lanes)
    returning = dot(table_x, scaled, 0, 0).reshape(grp, 2, block_x, total_lanes)
    midway = returning[..., planes * lines :]
    turned = jnp.concatenate([-midway[:, 1:], midway[:, :1]], axis=1)
    returning = jnp.concatenate(
        [returning[..., :lines] + turned, returning[..., lines : planes * lines]], axis=-1
    )
    rows, sums = exchange(
        [
            returning.reshape(grp, 2 * block_x, planes * lines),
            jnp.broadcast_to(spectral, (grp, 8, 128)),
        ],
        "grp",
        3,
    )
    spectral = jnp.sum(sums[:, 0, 0])
    rows = rows.reshape(grp, 2, block_x, planes, lines).transpose(0, 1, 4, 3, 2)
    columns = dot(table_y, rows.reshape(2 * KY, planes * block_x), 0, 0)
    columns, sums = exchange(
        [
            columns.reshape(pen, 2 * block_y, planes * block_x),
            jnp.broadcast_to(spectral, (pen, 8, 128)),
        ],
        "pen",
        4,
    )
    spectral = jnp.sum(sums[:, 0, 0])
    home = columns.reshape(pen, 2, block_y, planes, block_x).transpose(0, 1, 3, 4, 2)
    potential = dot(home.reshape(KZ, block_x * block_y), backward_z, 0, 0)
    return (potential.reshape(block_x, block_y, KZ), spectral)


def cas_table(length):
    position = np.arange(length)
    cos, sin = waves(position[:, None] * position, length)
    return cos + sin


def halves(table):
    high = table.astype(jnp.bfloat16)
    low = (table - high.astype(np.float64)).astype(jnp.bfloat16)
    return (high, low)


def spline_factor(length):
    index = np.arange(length)
    freq = np.where(2 * index < length, index, index - length) / length
    coeffs = np.array([1.0, 26.0, 66.0, 26.0, 1.0]) / 120.0
    phase = np.exp(2j * np.pi * index[:, None] * np.arange(5) / length)
    modulus_square = np.abs(phase @ coeffs) ** 2
    square = freq**2
    factor = np.exp(-(math.pi**2) * square / ewald_split**2) / modulus_square
    return (factor.astype(np.float32), square.astype(np.float32))


def regroup(tiles, width):
    lane = lax.broadcasted_iota(jnp.int32, tiles[0].shape, 1) // width
    bit = 1
    while bit < len(tiles):
        keep = (lane // bit) % 2 == 0
        mixed = list(tiles)
        for i in range(len(tiles)):
            if not i & bit:
                first, second = tiles[i], tiles[i + bit]
                mixed[i] = jnp.where(keep, first, pltpu.roll(second, bit * width, 1))
                mixed[i + bit] = jnp.where(
                    keep, pltpu.roll(first, 128 - bit * width, 1), second
                )
        tiles = mixed
        bit = 2 * bit
    return tiles


def whole_kernel(
    grp, pen, slots, sizes, off_ref, cell_ref, frac_ref, q_ref, cas_hi, cas_lo, into_hi, into_lo,
    back_hi, back_lo, factor_row, factor_col, square_row, square_col, out_ref, energy_ref,
    pad, ext, plain_x, plain_y, plain_z, slope_x, slope_y, slope_z,
    send, recv, send_back, recv_back, work, sums, part,
    rim_side, rim_up, rim_corner, halo_side, halo_up, halo_corner,
    out_send, out_recv, back_send, back_recv, sum_send, sum_recv,
    side_send, side_recv, halo_send, halo_recv, edge_send, edge_recv,
):
    count = grp * pen
    slabs = len(sizes)
    starts = [sum(sizes[:s]) for s in range(slabs)]
    groups = cell_ref.shape[0]
    block_x, block_y = KX // grp, KY // pen
    tile_rows = block_x // 2
    per_row = groups // tile_rows
    fan = 128 // block_y
    half = pen // fan
    at_grp, at_pen = lax.axis_index("grp"), lax.axis_index("pen")
    me = at_grp * pen + at_pen
    plain = (plain_x, plain_y, plain_z)
    slope = (slope_x, slope_y, slope_z)
    cas = (cas_hi[...], cas_lo[...])

    def device(d_grp, d_pen):
        return {
            "grp": lax.rem(at_grp + d_grp + grp, grp),
            "pen": lax.rem(at_pen + d_pen + pen, pen),
        }

    def remote(source, target, sems, where):
        return pltpu.make_async_remote_copy(
            src_ref=source, dst_ref=target, send_sem=sems[0], recv_sem=sems[1],
            device_id=where, device_id_type=pl.DeviceIdType.MESH,
        )

    def peer_of(d):
        peer = lax.rem(me + d, count)
        return (peer, {"grp": lax.div(peer, pen), "pen": lax.rem(peer, pen)})

    first_hop = pen * (grp // 2 - lax.rem(at_grp, grp // 2))

    def fan_out(make, before=None):
        def one(e, carry):
            d = 1 + lax.rem(e + first_hop - 1, count - 1)
            if before is not None:
                before(d).wait_send()
            if make is not None:
                make(d).start()
            return carry

        lax.fori_loop(0, count - 1, one, 0)

    others = pl.ds(0, count - 1)

    def slab_copy(s, source, target, sems):
        part_of = pl.ds(starts[s], sizes[s])
        pair = (sems[0].at[s], sems[1].at[s])

        def make(d):
            peer, where = peer_of(d)
            return remote(source.at[peer, part_of], target.at[me, part_of], pair, where)

        total = remote(
            source.at[others, part_of], target.at[others, part_of], pair, peer_of(1)[1]
        )
        return (make, total)

    def out_copy(s):
        return slab_copy(s, send, recv, (out_send, out_recv))

    def back_copy(s):
        part_of = pl.ds(starts[s], sizes[s])

        def make(d):
            peer, where = peer_of(d)
            pair = (back_send.at[d], back_recv.at[s])
            return remote(send_back.at[peer, part_of], recv_back.at[me, part_of], pair, where)

        pair = (back_send.at[0], back_recv.at[s])
        total = remote(
            send_back.at[others, part_of], recv_back.at[others, part_of], pair, peer_of(1)[1]
        )
        return (make, total)

    def sum_copy():
        pair = (sum_send.at[0], sum_recv.at[0])
        total = remote(sums.at[others], sums.at[others], pair, peer_of(1)[1])
        return (lambda d: remote(part, sums.at[me], pair, peer_of(d)[1]), total)

    def slab_rows(s):
        return pl.ds(starts[s] * fan, sizes[s] * fan)

    def side_rim(s):
        source = pad.at[slab_rows(s), pl.ds(block_y, 8), :]
        return remote(source, rim_side.at[slab_rows(s)], (side_send.at[s], side_recv.at[s]), device(0, 1))

    def edge_rims():
        source = pad.at[pl.ds(block_x, 5)]
        return [
            remote(
                source.at[:, pl.ds(0, block_y), :], rim_up,
                (edge_send.at[0], edge_recv.at[0]), device(1, 0),
            ),
            remote(
                source.at[:, pl.ds(block_y, 8), :], rim_corner,
                (edge_send.at[1], edge_recv.at[1]), device(1, 1),
            ),
        ]

    def side_halo(s):
        source = ext.at[slab_rows(s), pl.ds(0, 8), :]
        return remote(source, halo_side.at[slab_rows(s)], (halo_send.at[s], halo_recv.at[s]), device(0, -1))

    def edge_halos():
        source = ext.at[pl.ds(0, 5)]
        return [
            remote(
                source.at[:, pl.ds(0, block_y), :], halo_up,
                (edge_send.at[2], edge_recv.at[2]), device(-1, 0),
            ),
            remote(
                source.at[:, pl.ds(0, 8), :], halo_corner,
                (edge_send.at[3], edge_recv.at[3]), device(-1, -1),
            ),
        ]

    barrier = pltpu.get_barrier_semaphore()

    def greet(d, carry):
        pl.semaphore_signal(
            barrier, inc=1, device_id=peer_of(d)[1], device_id_type=pl.DeviceIdType.MESH
        )
        return carry

    lax.fori_loop(1, count, greet, 0)
    pad[...] = jnp.zeros_like(pad)

    def ship(s):
        side_rim(s).wait_recv()
        pad[slab_rows(s), pl.ds(0, 8), :] += rim_side[slab_rows(s)]

    def transform_out(s):
        def along_z(i, carry):
            tile = starts[s] + 2 * i
            rows = pad[pl.ds(tile * fan, 2 * fan), pl.ds(0, block_y), :]
            out = dot3(cas, split(rows.reshape(256, KZ)), 1, 1)
            for t in range(2):
                block = out[:, 128 * t : 128 * t + 128].reshape(count, 8, 128)
                send[:, tile + t] = block
            return carry

        lax.fori_loop(0, sizes[s] // 2, along_z, 0)
        fan_out(out_copy(s)[0])
        own = pl.ds(starts[s], sizes[s])
        recv[me, own] = send[me, own]

    ready = [max((start * fan - 5) // 2, 0) for start in starts]
    rows_per_outer = 8 // per_row

    def spread_plain(i, carry):
        a = tile_rows - 1 - i

        @pl.when(lax.rem(i, rows_per_outer) == 0)
        def _():
            outer = lax.div(a, rows_per_outer)
            store_weights(outer, slots, off_ref, frac_ref, *plain, 0)

        spread_row(a, per_row, cell_ref, q_ref, *plain, pad)
        return carry

    def spread_step(i, carry):
        a = tile_rows - 1 - i
        spread_plain(i, carry)

        @pl.when(a == ready[-1])
        def _():
            for copy in edge_rims():
                copy.start()

        for s in range(slabs):

            @pl.when(a == ready[s])
            def _(s=s):
                side_rim(s).start()

            if s:

                @pl.when(a == max(ready[s] - 5, 0))
                def _(s=s):
                    ship(s)
                    transform_out(s)

        return carry

    alone = tile_rows - 1 - ready[-1]
    lax.fori_loop(0, alone, spread_plain, 0)
    pl.semaphore_wait(barrier, count - 1)
    lax.fori_loop(alone, tile_rows, spread_step, 0)
    for copy in edge_rims():
        copy.wait_recv()
    ship(0)
    pad[:5, :block_y, :] += rim_up[...]
    pad[:5, :8, :] += rim_corner[...]
    transform_out(0)

    def prepare_slopes(outer, carry):
        store_weights(outer, slots, off_ref, frac_ref, *slope, 1)
        return carry

    lax.fori_loop(0, groups // 8, prepare_slopes, 0)

    def slab_lines(s, h):
        span = sizes[s] * 8 * KX // (block_x // fan)
        return pl.ds(starts[s] * 8 * KX // (block_x // fan) + h * 8 * KX, span)

    for s in reversed(range(slabs)):
        out_copy(s)[1].wait_recv()
        rows = []
        own = pl.ds(starts[s], sizes[s])
        for g in range(grp):
            parts = [[] for _ in range(fan)]
            for h in range(half):
                loaded = [
                    recv[g * pen + h * fan + k, own].reshape(8 * sizes[s], 128)
                    for k in range(fan)
                ]
                for k, tile in enumerate(regroup(loaded, block_y)):
                    parts[k].append(tile)
            rows += [jnp.concatenate(pieces, axis=1) for pieces in parts]
        out = dot3(split(jnp.concatenate(rows, axis=0)), cas, 1, 0)
        for h in range(2):
            work[slab_lines(s, h), :] = out[:, 128 * h : 128 * h + 128]

    scale = 1.0 / (math.pi * KX * KY * KZ)
    first = pl.multiple_of(8 * me, 8)
    factor_z = factor_col[pl.ds(first, 8), :]
    square_z = square_col[pl.ds(first, 8), :]
    pick = lax.broadcasted_iota(jnp.int32, (8, 1), 0)

    def along_x(i, total):
        for f in (2 * i, 2 * i + 1):
            chosen = pick == f
            fz = jnp.sum(jnp.where(chosen, factor_z, 0.0), axis=0, keepdims=True) * scale
            sz = jnp.sum(jnp.where(chosen, square_z, 0.0), axis=0, keepdims=True)
            rows = jnp.concatenate(
                [work[pl.ds(f + h * 8 * KX, KX, stride=8), :] for h in range(2)], axis=1
            )
            spectrum = dot3((into_hi[...], into_lo[...]), split(rows), 1, 0)
            square = square_col[...] + (square_row[...] + sz)
            safe = jnp.where(square > 0, square, 1.0)
            kernel = factor_col[...] * (factor_row[...] * fz) / safe
            kernel = jnp.where(square > 0, kernel, 0.0)
            scaled = kernel * spectrum
            total = total + jnp.sum(scaled * spectrum, axis=0, keepdims=True)
            out = dot3((back_hi[...], back_lo[...]), split(scaled), 1, 0)
            for h in range(2):
                rows = pl.ds(f + h * 8 * KX, KX, stride=8)
                work[rows, :] = out[:, 128 * h : 128 * h + 128]
        return total

    total = lax.fori_loop(0, 4, along_x, jnp.zeros((1, KY), jnp.float32))
    part[...] = jnp.broadcast_to(0.5 * jnp.sum(total, axis=1, keepdims=True), (1, 128))
    sums[me] = part[...]

    for s in range(slabs):
        rows = jnp.concatenate([work[slab_lines(s, h), :] for h in range(2)], axis=1)
        out = dot3(split(rows), cas, 1, 0)
        lines = 8 * sizes[s]
        own = pl.ds(starts[s], sizes[s])
        for g in range(grp):
            for h in range(half):
                parts = []
                for k in range(fan):
                    start = (g * fan + k) * lines
                    parts.append(out[start : start + lines, 128 * h : 128 * h + 128])
                for k, tile in enumerate(regroup(parts, block_y)):
                    send_back[g * pen + h * fan + k, own] = tile.reshape(sizes[s], 8, 128)
        recv_back[me, own] = send_back[me, own]
        if s == 0:
            fan_out(back_copy(s)[0])
    fan_out(sum_copy()[0])

    def home(s):
        if s + 1 < slabs:
            fan_out(back_copy(s + 1)[0], back_copy(s)[0])
        back_copy(s)[1].wait_recv()

        def home_z(i, inner):
            tile = starts[s] + 2 * i
            rows = jnp.concatenate(
                [recv_back[:, tile + t].reshape(KZ, 128) for t in range(2)], axis=1
            )
            out = dot3(split(jnp.transpose(rows)), cas, 1, 0)
            where = pl.ds(tile * fan, 2 * fan)
            ext[where, pl.ds(0, block_y), :] = out.reshape(2 * fan, block_y, KZ)
            return inner

        lax.fori_loop(0, sizes[s] // 2, home_z, 0)
        side_halo(s).start()

    def join_halo(s):
        side_halo(s).wait_recv()
        ext[slab_rows(s), pl.ds(block_y, 8), :] = halo_side[slab_rows(s)]

    home(0)
    for copy in edge_halos():
        copy.start()
    needed = [max((start * fan - 5) // 2, 0) for start in starts]
    early = [0] + [min(needed[s], 3) for s in range(1, slabs)]
    early[-1] = min(needed[-1], 5)

    def interp_step(a, carry):
        for s in range(1, slabs):

            @pl.when(a == needed[s] - early[s])
            def _(s=s):
                home(s)

        for s in range(slabs):

            @pl.when(a == needed[s])
            def _(s=s):
                join_halo(s)

        @pl.when(a == tile_rows - 3)
        def _():
            for copy in edge_halos():
                copy.wait_recv()
            ext[pl.ds(block_x, 5), pl.ds(0, block_y), :] = halo_up[...]
            ext[pl.ds(block_x, 5), pl.ds(block_y, 8), :] = halo_corner[...]

        interp_row(a, per_row, cell_ref, q_ref, plain, slope, ext, out_ref)
        return carry

    lax.fori_loop(0, tile_rows, interp_step, 0)
    sum_copy()[1].wait_recv()
    energy_ref[...] = jnp.sum(sums[...], axis=0)
    sum_copy()[1].wait_send()

    for s in range(slabs):
        out_copy(s)[1].wait_send()
        if s + 1 == slabs:
            fan_out(None, back_copy(s)[0])
        side_rim(s).wait_send()
        side_halo(s).wait_send()
    for copy in edge_rims() + edge_halos():
        copy.wait_send()


def whole_program(offsets, zcell, fracs, live_q, slots, grp, pen, sizes):
    count = grp * pen
    groups, width = zcell.shape
    block_x, block_y = KX // grp, KY // pen
    fan = 128 // block_y
    slabs = len(sizes)
    cas = cas_table(KZ)
    cells = np.arange(KX).reshape(grp, block_x // fan, fan)
    order = np.concatenate(
        [
            cells[:, sum(sizes[:s]) : sum(sizes[: s + 1])].transpose(0, 2, 1).reshape(-1)
            for s in range(slabs)
        ]
    )
    factor, square = spline_factor(KX)
    tables = [*halves(cas), *halves(cas[:, order]), *halves(cas[order, :])]
    tables += [factor[None, :], factor[:, None], square[None, :], square[:, None]]
    tables = [jnp.asarray(table) for table in tables]
    vmem = pl.BlockSpec(memory_space=pltpu.VMEM)

    def held(*shape):
        return pltpu.VMEM(shape, jnp.float32)

    traffic = held(count, block_x // fan, 8, 128)
    dma = pltpu.SemaphoreType.DMA
    forces, energy = pl.pallas_call(
        functools.partial(whole_kernel, grp, pen, slots, sizes),
        out_shape=[
            jax.ShapeDtypeStruct((3, groups * width), jnp.float32),
            jax.ShapeDtypeStruct((1, 128), jnp.float32),
        ],
        in_specs=[vmem] * (4 + len(tables)),
        out_specs=[vmem] * 2,
        scratch_shapes=[
            held(block_x + 8, block_y + 8, KZ),
            held(block_x + 8, block_y + 8, KZ),
            *weight_scratch(groups, width),
            *weight_scratch(groups, width),
            traffic, traffic, traffic, traffic,
            held(16 * KX, 128),
            held(count, 1, 128),
            held(1, 128),
            held(block_x, 8, KZ), held(5, block_y, KZ), held(5, 8, KZ),
            held(block_x, 8, KZ), held(5, block_y, KZ), held(5, 8, KZ),
            dma((slabs,)), dma((slabs,)), dma((count,)), dma((slabs,)),
            dma((1,)), dma((1,)),
            dma((slabs,)), dma((slabs,)), dma((slabs,)), dma((slabs,)),
            dma((4,)), dma((4,)),
        ],
        compiler_params=pltpu.CompilerParams(
            collective_id=1, has_side_effects=True, vmem_limit_bytes=60 * 1024 * 1024
        ),
        name="whole",
    )(offsets, zcell, fracs, live_q, *tables)
    return (forces, energy[0, 0])


def slab_fits(grp, pen, sizes, block_x, block_y, per_row):
    fan = 128 // block_y
    return (
        grp * pen * 8 == KZ and KX == KY and KY == KZ and KZ == 256 and pen % fan == 0
        and block_x == fan * sum(sizes) and per_row * 8 == block_y and 8 % per_row == 0
    )


def local(cell_offsets, cell_z, frac, charges, tile_counts):
    block_x = KX // lax.axis_size("grp")
    block_y = KY // lax.axis_size("pen")
    tiles = tile_counts.shape[0]
    slots = charges.shape[0] // tiles
    width = 4 * slots
    groups = tiles // 4
    per_row = block_y // 8
    live = jnp.arange(slots, dtype=jnp.int32)[None, :] < tile_counts[:, None]
    live_q = (charges.reshape(tiles, slots) * live.astype(jnp.float32)).reshape(groups, width)
    offsets = cell_offsets.reshape(2, groups, width)
    zcell = cell_z.reshape(groups, width)
    fracs = frac.reshape(3, groups, width)
    grp, pen = lax.axis_size("grp"), lax.axis_size("pen")
    sizes = (6, 4, 4, 2)
    if slab_fits(grp, pen, sizes, block_x, block_y, per_row):
        forces, total = whole_program(offsets, zcell, fracs, live_q, slots, grp, pen, sizes)
        return (forces, total / ATOMS)
    vmem = pl.BlockSpec(memory_space=pltpu.VMEM)
    params = pltpu.CompilerParams(vmem_limit_bytes=60 * 1024 * 1024)
    padded = pl.pallas_call(
        functools.partial(spread_kernel, per_row, slots),
        out_shape=jax.ShapeDtypeStruct((block_x + 8, block_y + 8, KZ), jnp.float32),
        in_specs=[vmem] * 4,
        out_specs=vmem,
        scratch_shapes=weight_scratch(groups, width),
        compiler_params=params,
        name="spread",
    )(offsets, zcell, fracs, live_q)
    rim_y = shifted(padded[: block_x + 5, block_y : block_y + 5], "pen", 1)
    merged = padded[: block_x + 5, :block_y].at[:, :5].add(rim_y)
    rim_x = shifted(merged[block_x : block_x + 5], "grp", 1)
    grid = merged[:block_x] + jnp.pad(rim_x, ((0, block_x - 5), (0, 0), (0, 0)))
    potential, total = spectrum_of(grid, block_x, block_y)
    upper = shifted(potential[:5], "grp", -1)
    ext_x = jnp.concatenate([potential[:, :5], upper[:, :5]], axis=0)
    beside = shifted(ext_x, "pen", -1)
    beside = jnp.pad(beside, ((0, 0), (0, 3), (0, 0)))
    forces = pl.pallas_call(
        functools.partial(interp_kernel, per_row, slots),
        out_shape=jax.ShapeDtypeStruct((3, groups * width), jnp.float32),
        in_specs=[vmem] * 7,
        out_specs=vmem,
        scratch_shapes=[pltpu.VMEM((block_x + 8, block_y + 8, KZ), jnp.float32)]
        + 2 * weight_scratch(groups, width),
        compiler_params=params,
        name="interp",
    )(offsets, zcell, fracs, live_q, potential, upper, beside)
    return (forces, total / ATOMS)


def solution(mesh):
    in_specs = (
        P(None, ("grp", "pen")),
        P(("grp", "pen")),
        P(None, ("grp", "pen")),
        P(("grp", "pen")),
        P(("grp", "pen")),
    )
    out_specs = (P(None, ("grp", "pen")), P())
    return jax.shard_map(local, mesh=mesh, in_specs=in_specs, out_specs=out_specs, check_vma=False)
```

```python
import functools
import math

import jax
import jax.numpy as jnp
import numpy as np
from jax import lax
from jax.experimental import pallas as pl
from jax.experimental.pallas import tpu as pltpu
from jax.sharding import PartitionSpec as P

KX = 256
KY = 256
KZ = 256
ATOMS = 1048576


ewald_split = 0.6
highest = lax.Precision.HIGH


def shifted(block, axis, distance):
    devices = range(lax.axis_size(axis))
    route = [((i - distance) % len(devices), i) for i in devices]
    return lax.ppermute(block, axis, route)


def spline_rows(fracs):
    values = [jnp.ones_like(fracs)]
    fifth = values
    for order in range(2, 7):
        nxt = []
        for j in range(order):
            term = jnp.zeros_like(fracs)
            if j >= 1:
                term = values[j - 1] * (fracs + order - 1 - j)
            if j <= order - 2:
                term = term + values[j] * (1.0 - fracs + j)
            nxt.append(term / (order - 1))
        if order == 5:
            fifth = nxt
        values = nxt
    slopes = []
    for j in range(6):
        term = jnp.zeros_like(fracs)
        if j >= 1:
            term = fifth[j - 1]
        if j <= 4:
            term = term - fifth[j]
        slopes.append(term)
    return (values, slopes)


def split(values):
    high = values.astype(jnp.bfloat16)
    low = (values - high.astype(jnp.float32)).astype(jnp.bfloat16)
    return (high, low)


def shift_rows(values, offset):
    none = jnp.zeros_like(values[0])
    return [
        jnp.where(offset == 0, first, second)
        for first, second in zip(values + [none], [none] + values)
    ]


def store_weights(outer, slots, off_ref, frac_ref, x_ref, y_ref, z_ref, which):
    groups, width = off_ref.shape[1], off_ref.shape[2]
    rows = pl.ds(pl.multiple_of(outer * 8, 8), 8)
    lane_tile = lax.broadcasted_iota(jnp.int32, (8, width), 1) // slots
    along_x = spline_rows(frac_ref[0, rows, :])[which]
    along_y = spline_rows(frac_ref[1, rows, :])[which]
    along_z = spline_rows(frac_ref[2, rows, :])[which]
    for k, value in enumerate(shift_rows(along_x, off_ref[0, rows, :])):
        x_ref[k, rows, :] = value
    for k, value in enumerate(along_z):
        z_ref[k, rows, :] = value
    near = shift_rows(along_y, off_ref[1, rows, :])
    none = jnp.zeros_like(near[0])
    for r in range(16):
        value = none
        for tile in range(4):
            if 0 <= r - 2 * tile < 7:
                value = jnp.where(lane_tile == tile, near[r - 2 * tile], value)
        for h in range(width // 128):
            start = (h * groups + outer * 8) * 16 + r
            y_ref[pl.ds(start, 8, stride=16), :] = value[:, 128 * h : 128 * h + 128]


def rows_of_y(y_ref, group, groups, width):
    parts = []
    for h in range(width // 128):
        start = pl.multiple_of((h * groups + group) * 16, 16)
        parts.append(y_ref[pl.ds(start, 16), :])
    return jnp.concatenate(parts, axis=1)


def z_window(base, values):
    fine = lax.broadcasted_iota(jnp.int32, (32, base.shape[1]), 0) - (base & 15)
    total = jnp.zeros(fine.shape, jnp.float32)
    for j in range(6):
        total = jnp.where(fine == j, values[j], total)
    return split(total)


def z_masks(base):
    coarse = jnp.broadcast_to(base // 16, (16, base.shape[1])).astype(jnp.int16)
    return [coarse == jnp.int16(k) for k in range(16)]


def z_weights(masks, window):
    halves_of = []
    for part in window:
        lower, upper = part[:16], part[16:]
        none = jnp.zeros_like(lower)
        blocks = []
        for k in range(16):
            block = jnp.where(masks[k - 1], upper, none)
            blocks.append(jnp.where(masks[k], lower, block))
        halves_of.append(jnp.concatenate(blocks, axis=0))
    return halves_of


def dot3(left, right, left_dim, right_dim):
    dims = (((left_dim,), (right_dim,)), ((), ()))
    one = functools.partial(
        lax.dot_general, dimension_numbers=dims, preferred_element_type=jnp.float32
    )
    return one(left[0], right[0]) + one(left[0], right[1]) + one(left[1], right[0])


def wide_row(ref, group, width):
    parts = width // ref.shape[1]
    rows = [ref[pl.ds(group * parts + i, 1), :] for i in range(parts)]
    return rows[0] if parts == 1 else jnp.concatenate(rows, axis=1)


def stacked_dot(left, right, left_dim, right_dim):
    dims = (((left_dim,), (right_dim,)), ((), ()))
    one = functools.partial(
        lax.dot_general, dimension_numbers=dims, preferred_element_type=jnp.float32
    )
    rows = left[0].shape[0]
    both = one(jnp.concatenate(left, axis=0), right[0])
    return both[:rows] + both[rows:] + one(left[0], right[1])


def spread_row(a, per_row, cell_ref, q_ref, x_ref, y_ref, z_ref, grid_ref):
    groups, width = x_ref.shape[1:]
    outs = []
    for b in range(per_row):
        group = a * per_row + b
        base = wide_row(cell_ref, group, width)
        values = [z_ref[j, pl.ds(group, 1), :] for j in range(6)]
        weights = z_weights(z_masks(base), z_window(base, values))
        along_y = rows_of_y(y_ref, group, groups, width)
        along_y = along_y * wide_row(q_ref, group, width)
        pair = [x_ref[k, pl.ds(group, 1), :] * along_y for k in range(7)]
        outs.append(stacked_dot(split(jnp.concatenate(pair, axis=0)), weights, 1, 1))
    for k in range(7):
        for t in range(per_row + 1):
            value = 0.0
            if t < per_row:
                value = outs[t][16 * k : 16 * k + 8]
            if t >= 1:
                value = value + outs[t - 1][16 * k + 8 : 16 * k + 16]
            grid_ref[2 * a + k, 8 * t : 8 * t + 8, :] += value


def interp_row(a, per_row, cell_ref, q_ref, plain, slope, ext_ref, out_ref):
    groups, width = plain[0].shape[1:]
    for b in range(per_row):
        group = a * per_row + b
        row = pl.ds(group, 1)
        base = wide_row(cell_ref, group, width)
        masks = z_masks(base)
        footing = jnp.concatenate(
            [ext_ref[2 * a + k, 8 * b : 8 * b + 16, :] for k in range(7)], axis=0
        )
        footing = split(footing)
        both = []
        for refs in (plain, slope):
            window = z_window(base, [refs[2][j, row, :] for j in range(6)])
            both.append(dot3(footing, z_weights(masks, window), 1, 0))
        main, tilt = both
        along_x = 0.0
        along_y = 0.0
        along_z = 0.0
        for k in range(7):
            weight, grade = plain[0][k, row, :], slope[0][k, row, :]
            piece = main[16 * k : 16 * k + 16]
            along_x = along_x + grade * piece
            along_y = along_y + weight * piece
            along_z = along_z + weight * tilt[16 * k : 16 * k + 16]
        weight_y = rows_of_y(plain[1], group, groups, width)
        grade_y = rows_of_y(slope[1], group, groups, width)
        minus_q = -wide_row(q_ref, group, width)
        pieces = (along_x * weight_y, along_y * grade_y, along_z * weight_y)
        sums = [jnp.sum(piece, axis=0, keepdims=True) for piece in pieces]
        lanes = pl.ds(pl.multiple_of(group * width, width), width)
        out_ref[:, lanes] = minus_q * jnp.concatenate(sums, axis=0)


def weight_scratch(groups, width):
    return [
        pltpu.VMEM((7, groups, width), jnp.float32),
        pltpu.VMEM((groups * 16 * (width // 128), 128), jnp.float32),
        pltpu.VMEM((6, groups, width), jnp.float32),
    ]


def spread_kernel(per_row, slots, off_ref, z_ref, frac_ref, q_ref, grid_ref, *weights):
    grid_ref[...] = jnp.zeros_like(grid_ref)
    groups = z_ref.shape[0]

    def prepare(outer, carry):
        store_weights(outer, slots, off_ref, frac_ref, *weights, 0)
        return carry

    def step(a, carry):
        spread_row(a, per_row, z_ref, q_ref, *weights, grid_ref)
        return carry

    lax.fori_loop(0, groups // 8, prepare, 0)
    lax.fori_loop(0, groups // per_row, step, 0)


def interp_kernel(
    per_row, slots, off_ref, z_ref, frac_ref, q_ref, pot_ref, up_ref, side_ref, out_ref,
    ext_ref, *weights
):
    groups = z_ref.shape[0]
    size_z = pot_ref.shape[2]
    block_x, block_y = pot_ref.shape[0], pot_ref.shape[1]
    ext_ref[:block_x, :block_y] = pot_ref[...]
    ext_ref[block_x : block_x + 5, :block_y] = up_ref[...]
    ext_ref[block_x + 5 :, :block_y] = jnp.zeros((3, block_y, size_z), jnp.float32)
    ext_ref[: block_x + 5, block_y:] = side_ref[...]
    ext_ref[block_x + 5 :, block_y:] = jnp.zeros((3, 8, size_z), jnp.float32)

    def prepare(outer, carry):
        store_weights(outer, slots, off_ref, frac_ref, *weights[:3], 0)
        store_weights(outer, slots, off_ref, frac_ref, *weights[3:], 1)
        return carry

    def step(a, carry):
        interp_row(a, per_row, z_ref, q_ref, weights[:3], weights[3:], ext_ref, out_ref)
        return carry

    lax.fori_loop(0, groups // 8, prepare, 0)
    lax.fori_loop(0, groups // per_row, step, 0)


def modulus(index, length):
    coeffs = (1.0 / 120.0, 26.0 / 120.0, 66.0 / 120.0, 26.0 / 120.0, 1.0 / 120.0)
    real_part = 0.0
    imag_part = 0.0
    for j in range(5):
        angle = (index * j % length).astype(jnp.float32) * (2.0 * math.pi / length)
        real_part = real_part + coeffs[j] * jnp.cos(angle)
        imag_part = imag_part + coeffs[j] * jnp.sin(angle)
    return real_part * real_part + imag_part * imag_part


def influence(index_x, index_y, index_z):
    freq_x = jnp.where(2 * index_x < KX, index_x, index_x - KX).astype(jnp.float32) / KX
    freq_y = jnp.where(2 * index_y < KY, index_y, index_y - KY).astype(jnp.float32) / KY
    freq_z = jnp.where(2 * index_z < KZ, index_z, index_z - KZ).astype(jnp.float32) / KZ
    square = freq_x * freq_x + freq_y * freq_y + freq_z * freq_z
    safe = jnp.where(square > 0, square, 1.0)
    volume = float(KX * KY * KZ)
    value = jnp.exp(-math.pi**2 * safe / ewald_split**2) / (math.pi * volume * safe)
    value = value / (modulus(index_x, KX) * modulus(index_y, KY) * modulus(index_z, KZ))
    return jnp.where(square > 0, value, 0.0)


def waves(index, length):
    angle = (index % length) * (2.0 * math.pi / length)
    return (np.cos(angle), np.sin(angle))


def z_table(groups):
    planes = KZ // (2 * groups)
    frequency = np.arange(KZ // 2).reshape(groups, planes)
    cos, sin = waves(frequency[..., None] * np.arange(KZ), KZ)
    table = np.stack([cos, -sin], axis=1)
    table[0, 1, 0] = waves(np.arange(KZ) * (KZ // 2), KZ)[0]
    weight = np.full((groups, 2, planes), 2.0)
    weight[0, :, 0] = 1.0
    table = table.reshape(KZ, KZ)
    return (table.astype(np.float32), (table * weight.reshape(KZ, 1)).astype(np.float32))


def block_table(frequency, length, groups):
    position = np.arange(length)
    cos, sin = waves(frequency[..., None] * position, length)
    shape = (frequency.shape[0], frequency.shape[1], groups, length // groups)
    cos, sin = cos.reshape(shape), sin.reshape(shape)
    real_row = np.stack([cos, sin], axis=3)
    imag_row = np.stack([-sin, cos], axis=3)
    table = np.stack([real_row, imag_row], axis=1)
    return table.reshape(2 * length, 2 * length).astype(np.float32)


def y_frequency(groups):
    first = np.arange(KY // 2).reshape(groups, -1)
    second = np.where(first == 0, KY // 2, (KY - first) % KY)
    return np.concatenate([first, second], axis=1)


def partner_of(me, d, count):
    if count & (count - 1):
        return lax.rem(me + d, count)
    peer = me
    bit = 1
    while bit < count:
        if d & bit:
            peer = peer + bit - 2 * bit * lax.rem(lax.div(me, bit), 2)
        bit = 2 * bit
    return peer


def exchange_kernel(axis, count, *refs):
    arrays = (len(refs) - 3) // 2
    sources, targets = refs[:arrays], refs[arrays : 2 * arrays]
    send_sem, recv_sem, own_sem = refs[2 * arrays :]
    me = lax.axis_index(axis)
    barrier = pltpu.get_barrier_semaphore()
    for d in range(1, count):
        pl.semaphore_signal(
            barrier,
            inc=1,
            device_id={axis: partner_of(me, d, count)},
            device_id_type=pl.DeviceIdType.MESH,
        )
    pl.semaphore_wait(barrier, count - 1)
    copies = []
    for k in range(arrays):
        for d in range(1, count):
            peer = partner_of(me, d, count)
            copies.append(
                pltpu.make_async_remote_copy(
                    src_ref=sources[k].at[peer],
                    dst_ref=targets[k].at[me],
                    send_sem=send_sem.at[k, d],
                    recv_sem=recv_sem.at[k, d],
                    device_id={axis: peer},
                    device_id_type=pl.DeviceIdType.MESH,
                )
            )
        copies.append(
            pltpu.make_async_copy(sources[k].at[me], targets[k].at[me], own_sem.at[k])
        )
    for copy in copies:
        copy.start()
    for copy in copies:
        copy.wait()


def exchange(arrays, axis, number):
    count = lax.axis_size(axis)
    vmem = pl.BlockSpec(memory_space=pltpu.VMEM)
    return pl.pallas_call(
        functools.partial(exchange_kernel, axis, count),
        out_shape=[jax.ShapeDtypeStruct(array.shape, array.dtype) for array in arrays],
        in_specs=[vmem] * len(arrays),
        out_specs=[vmem] * len(arrays),
        scratch_shapes=[
            pltpu.SemaphoreType.DMA((len(arrays), count)),
            pltpu.SemaphoreType.DMA((len(arrays), count)),
            pltpu.SemaphoreType.DMA((len(arrays),)),
        ],
        compiler_params=pltpu.CompilerParams(collective_id=number, has_side_effects=True),
        name="exchange" + str(number),
    )(*arrays)


def dot(left, right, left_dim, right_dim):
    dims = (((left_dim,), (right_dim,)), ((), ()))
    return lax.dot_general(
        left, right, dims, precision=highest, preferred_element_type=jnp.float32
    )


def spectrum_of(grid, block_x, block_y):
    grp, pen = lax.axis_size("grp"), lax.axis_size("pen")
    planes = KZ // (2 * pen)
    lines = KY // grp
    half = lines // 2
    forward_z, backward_z = z_table(pen)
    order_y = y_frequency(grp)
    table_y = block_table(order_y, KY, pen)
    table_x = block_table(np.arange(KX)[None], KX, grp)
    lines_z = dot(forward_z, grid.reshape(block_x * block_y, KZ), 1, 1)
    lines_z = lines_z.reshape(pen, 2, planes, block_x, block_y).transpose(0, 1, 4, 2, 3)
    (columns,) = exchange(
        [lines_z.reshape(pen, 2 * block_y, planes * block_x)], "pen", 1
    )
    lines_y = dot(table_y, columns.reshape(2 * KY, planes * block_x), 1, 0)
    lines_y = lines_y.reshape(grp, 2, lines, planes, block_x).transpose(0, 1, 4, 3, 2)
    (rows,) = exchange([lines_y.reshape(grp, 2 * block_x, planes * lines)], "grp", 2)
    rows = rows.reshape(grp, 2, block_x, planes * lines)
    at_grp, at_pen = lax.axis_index("grp"), lax.axis_index("pen")
    packed = rows[..., :lines]
    alone = (at_grp == 0) & (jnp.arange(lines) % half == 0)
    partner = jnp.where(
        alone, packed, jnp.concatenate([packed[..., half:], packed[..., :half]], axis=-1)
    )
    a, b = packed[:, :1], packed[:, 1:]
    c, d = partner[:, :1], partner[:, 1:]
    whole = jnp.concatenate([a + c, b - d], axis=1) * 0.5
    midway = jnp.concatenate([b + d, c - a], axis=1) * 0.5
    origin = at_pen == 0
    whole = jnp.where(origin, whole, packed)
    midway = jnp.where(origin, midway, 0.0)
    total_lanes = (planes + 1) * lines
    full = jnp.concatenate([whole, rows[..., lines:], midway], axis=-1)
    spectrum = dot(table_x, full.reshape(2 * KX, total_lanes), 1, 0)
    spectrum = spectrum.reshape(2, KX, total_lanes)
    index_x = jnp.arange(KX, dtype=jnp.int32)[:, None]
    slot = jnp.arange(planes + 1, dtype=jnp.int32)
    index_z = jnp.where(slot < planes, at_pen * planes + slot, KZ // 2)
    plane_weight = jnp.where(
        slot < planes,
        jnp.where(origin & (slot == 0), 1.0, 2.0),
        jnp.where(origin, 1.0, 0.0),
    )
    index_z = jnp.repeat(index_z, lines)[None, :]
    plane_weight = jnp.repeat(plane_weight, lines)[None, :]
    index_y = lax.dynamic_index_in_dim(jnp.asarray(order_y, jnp.int32), at_grp, 0, False)
    index_y = jnp.tile(index_y, planes + 1)[None, :]
    kernel = influence(index_x, index_y, index_z)
    power = spectrum[0] * spectrum[0] + spectrum[1] * spectrum[1]
    spectral = 0.5 * jnp.sum(plane_weight * kernel * power)
    scaled = (spectrum * kernel).reshape(2 * KX, total_lanes)
    returning = dot(table_x, scaled, 0, 0).reshape(grp, 2, block_x, total_lanes)
    midway = returning[..., planes * lines :]
    turned = jnp.concatenate([-midway[:, 1:], midway[:, :1]], axis=1)
    returning = jnp.concatenate(
        [returning[..., :lines] + turned, returning[..., lines : planes * lines]], axis=-1
    )
    rows, sums = exchange(
        [
            returning.reshape(grp, 2 * block_x, planes * lines),
            jnp.broadcast_to(spectral, (grp, 8, 128)),
        ],
        "grp",
        3,
    )
    spectral = jnp.sum(sums[:, 0, 0])
    rows = rows.reshape(grp, 2, block_x, planes, lines).transpose(0, 1, 4, 3, 2)
    columns = dot(table_y, rows.reshape(2 * KY, planes * block_x), 0, 0)
    columns, sums = exchange(
        [
            columns.reshape(pen, 2 * block_y, planes * block_x),
            jnp.broadcast_to(spectral, (pen, 8, 128)),
        ],
        "pen",
        4,
    )
    spectral = jnp.sum(sums[:, 0, 0])
    home = columns.reshape(pen, 2, block_y, planes, block_x).transpose(0, 1, 3, 4, 2)
    potential = dot(home.reshape(KZ, block_x * block_y), backward_z, 0, 0)
    return (potential.reshape(block_x, block_y, KZ), spectral)


def cas_table(length):
    position = np.arange(length)
    cos, sin = waves(position[:, None] * position, length)
    return cos + sin


def halves(table):
    high = table.astype(jnp.bfloat16)
    low = (table - high.astype(np.float64)).astype(jnp.bfloat16)
    return (high, low)


def spline_factor(length):
    index = np.arange(length)
    freq = np.where(2 * index < length, index, index - length) / length
    coeffs = np.array([1.0, 26.0, 66.0, 26.0, 1.0]) / 120.0
    phase = np.exp(2j * np.pi * index[:, None] * np.arange(5) / length)
    modulus_square = np.abs(phase @ coeffs) ** 2
    square = freq**2
    factor = np.exp(-(math.pi**2) * square / ewald_split**2) / modulus_square
    return (factor.astype(np.float32), square.astype(np.float32))


def regroup(tiles, width):
    lane = lax.broadcasted_iota(jnp.int32, tiles[0].shape, 1) // width
    bit = 1
    while bit < len(tiles):
        keep = (lane // bit) % 2 == 0
        mixed = list(tiles)
        for i in range(len(tiles)):
            if not i & bit:
                first, second = tiles[i], tiles[i + bit]
                mixed[i] = jnp.where(keep, first, pltpu.roll(second, bit * width, 1))
                mixed[i + bit] = jnp.where(
                    keep, pltpu.roll(first, 128 - bit * width, 1), second
                )
        tiles = mixed
        bit = 2 * bit
    return tiles


def whole_kernel(
    grp, pen, slots, sizes, off_ref, cell_ref, frac_ref, q_ref, cas_hi, cas_lo, into_hi, into_lo,
    back_hi, back_lo, factor_row, factor_col, square_row, square_col, out_ref, energy_ref,
    pad, ext, plain_x, plain_y, plain_z, slope_x, slope_y, slope_z,
    send, recv, send_back, recv_back, work, sums, part,
    rim_side, rim_up, rim_corner, halo_side, halo_up, halo_corner,
    out_send, out_recv, back_send, back_recv, sum_send, sum_recv,
    side_send, side_recv, halo_send, halo_recv, edge_send, edge_recv,
):
    count = grp * pen
    slabs = len(sizes)
    starts = [sum(sizes[:s]) for s in range(slabs)]
    groups = off_ref.shape[1]
    block_x, block_y = KX // grp, KY // pen
    tile_rows = block_x // 2
    per_row = groups // tile_rows
    fan = 128 // block_y
    half = pen // fan
    at_grp, at_pen = lax.axis_index("grp"), lax.axis_index("pen")
    me = at_grp * pen + at_pen
    plain = (plain_x, plain_y, plain_z)
    slope = (slope_x, slope_y, slope_z)
    cas = (cas_hi[...], cas_lo[...])

    def device(d_grp, d_pen):
        return {
            "grp": lax.rem(at_grp + d_grp + grp, grp),
            "pen": lax.rem(at_pen + d_pen + pen, pen),
        }

    def remote(source, target, sems, where):
        return pltpu.make_async_remote_copy(
            src_ref=source, dst_ref=target, send_sem=sems[0], recv_sem=sems[1],
            device_id=where, device_id_type=pl.DeviceIdType.MESH,
        )

    def peer_of(d):
        peer = lax.rem(me + d, count)
        return (peer, {"grp": lax.div(peer, pen), "pen": lax.rem(peer, pen)})

    def fan_out(make, before=None):
        def one(e, carry):
            plane = lax.rem(at_grp + grp + jnp.where(2 * at_grp < grp, 1 + lax.div(e, pen), -1 - lax.div(e, pen)), grp)
            other = plane * pen + lax.rem(at_pen + lax.rem(e, pen), pen)
            d = lax.rem(other - me + count, count)

            @pl.when(d != 0)
            def _():
                if before is not None:
                    before(d).wait_send()
                if make is not None:
                    make(d).start()

            return carry

        lax.fori_loop(0, count, one, 0)

    others = pl.ds(0, count - 1)

    def slab_copy(s, source, target, sems):
        part_of = pl.ds(starts[s], sizes[s])
        pair = (sems[0].at[s], sems[1].at[s])

        def make(d):
            peer, where = peer_of(d)
            return remote(source.at[peer, part_of], target.at[me, part_of], pair, where)

        total = remote(
            source.at[others, part_of], target.at[others, part_of], pair, peer_of(1)[1]
        )
        return (make, total)

    def out_copy(s):
        return slab_copy(s, send, recv, (out_send, out_recv))

    def back_copy(s):
        part_of = pl.ds(starts[s], sizes[s])

        def make(d):
            peer, where = peer_of(d)
            pair = (back_send.at[d], back_recv.at[s])
            return remote(send_back.at[peer, part_of], recv_back.at[me, part_of], pair, where)

        pair = (back_send.at[0], back_recv.at[s])
        total = remote(
            send_back.at[others, part_of], recv_back.at[others, part_of], pair, peer_of(1)[1]
        )
        return (make, total)

    def sum_copy():
        pair = (sum_send.at[0], sum_recv.at[0])
        total = remote(sums.at[others], sums.at[others], pair, peer_of(1)[1])
        return (lambda d: remote(part, sums.at[me], pair, peer_of(d)[1]), total)

    def slab_rows(s):
        return pl.ds(starts[s] * fan, sizes[s] * fan)

    def side_rim(s):
        source = pad.at[slab_rows(s), pl.ds(block_y, 8), :]
        return remote(source, rim_side.at[slab_rows(s)], (side_send.at[s], side_recv.at[s]), device(0, 1))

    def edge_rims():
        source = pad.at[pl.ds(block_x, 5)]
        return [
            remote(
                source.at[:, pl.ds(0, block_y), :], rim_up,
                (edge_send.at[0], edge_recv.at[0]), device(1, 0),
            ),
            remote(
                source.at[:, pl.ds(block_y, 8), :], rim_corner,
                (edge_send.at[1], edge_recv.at[1]), device(1, 1),
            ),
        ]

    def side_halo(s):
        source = ext.at[slab_rows(s), pl.ds(0, 8), :]
        return remote(source, halo_side.at[slab_rows(s)], (halo_send.at[s], halo_recv.at[s]), device(0, -1))

    def edge_halos():
        source = ext.at[pl.ds(0, 5)]
        return [
            remote(
                source.at[:, pl.ds(0, block_y), :], halo_up,
                (edge_send.at[2], edge_recv.at[2]), device(-1, 0),
            ),
            remote(
                source.at[:, pl.ds(0, 8), :], halo_corner,
                (edge_send.at[3], edge_recv.at[3]), device(-1, -1),
            ),
        ]

    barrier = pltpu.get_barrier_semaphore()

    def greet(d, carry):
        pl.semaphore_signal(
            barrier, inc=1, device_id=peer_of(d)[1], device_id_type=pl.DeviceIdType.MESH
        )
        return carry

    lax.fori_loop(1, count, greet, 0)
    pad[...] = jnp.zeros_like(pad)

    def ship(s):
        side_rim(s).wait_recv()
        pad[slab_rows(s), pl.ds(0, 8), :] += rim_side[slab_rows(s)]

    def transform_out(s):
        def along_z(i, carry):
            tile = starts[s] + 2 * i
            rows = pad[pl.ds(tile * fan, 2 * fan), pl.ds(0, block_y), :]
            out = dot3(cas, split(rows.reshape(256, KZ)), 1, 1)
            for t in range(2):
                block = out[:, 128 * t : 128 * t + 128].reshape(count, 8, 128)
                send[:, tile + t] = block
            return carry

        lax.fori_loop(0, sizes[s] // 2, along_z, 0)
        fan_out(out_copy(s)[0])
        own = pl.ds(starts[s], sizes[s])
        recv[me, own] = send[me, own]

    ready = [max((start * fan - 5) // 2, 0) for start in starts]
    rows_per_outer = 8 // per_row

    def spread_plain(i, carry):
        a = tile_rows - 1 - i

        @pl.when(lax.rem(i, rows_per_outer) == 0)
        def _():
            outer = lax.div(a, rows_per_outer)
            store_weights(outer, slots, off_ref, frac_ref, *plain, 0)

        spread_row(a, per_row, cell_ref, q_ref, *plain, pad)
        return carry

    def spread_step(i, carry):
        a = tile_rows - 1 - i
        spread_plain(i, carry)

        @pl.when(a == ready[-1])
        def _():
            for copy in edge_rims():
                copy.start()

        for s in range(slabs):

            @pl.when(a == ready[s])
            def _(s=s):
                side_rim(s).start()

            if s:

                @pl.when(a == max(ready[s] - 5, 0))
                def _(s=s):
                    ship(s)
                    transform_out(s)

        return carry

    alone = tile_rows - 1 - ready[-1]
    lax.fori_loop(0, alone, spread_plain, 0)
    pl.semaphore_wait(barrier, count - 1)
    lax.fori_loop(alone, tile_rows, spread_step, 0)
    for copy in edge_rims():
        copy.wait_recv()
    ship(0)
    pad[:5, :block_y, :] += rim_up[...]
    pad[:5, :8, :] += rim_corner[...]
    transform_out(0)

    def prepare_slopes(outer, carry):
        store_weights(outer, slots, off_ref, frac_ref, *slope, 1)
        return carry

    lax.fori_loop(0, groups // 8, prepare_slopes, 0)

    def slab_lines(s, h):
        span = sizes[s] * 8 * KX // (block_x // fan)
        return pl.ds(starts[s] * 8 * KX // (block_x // fan) + h * 8 * KX, span)

    for s in reversed(range(slabs)):
        out_copy(s)[1].wait_recv()
        rows = []
        own = pl.ds(starts[s], sizes[s])
        for g in range(grp):
            parts = [[] for _ in range(fan)]
            for h in range(half):
                loaded = [
                    recv[g * pen + h * fan + k, own].reshape(8 * sizes[s], 128)
                    for k in range(fan)
                ]
                for k, tile in enumerate(regroup(loaded, block_y)):
                    parts[k].append(tile)
            rows += [jnp.concatenate(pieces, axis=1) for pieces in parts]
        out = dot3(split(jnp.concatenate(rows, axis=0)), cas, 1, 0)
        for h in range(2):
            work[slab_lines(s, h), :] = out[:, 128 * h : 128 * h + 128]

    scale = 1.0 / (math.pi * KX * KY * KZ)
    first = pl.multiple_of(8 * me, 8)
    factor_z = factor_col[pl.ds(first, 8), :]
    square_z = square_col[pl.ds(first, 8), :]
    pick = lax.broadcasted_iota(jnp.int32, (8, 1), 0)

    def along_x(i, total):
        for f in (2 * i, 2 * i + 1):
            chosen = pick == f
            fz = jnp.sum(jnp.where(chosen, factor_z, 0.0), axis=0, keepdims=True) * scale
            sz = jnp.sum(jnp.where(chosen, square_z, 0.0), axis=0, keepdims=True)
            rows = jnp.concatenate(
                [work[pl.ds(f + h * 8 * KX, KX, stride=8), :] for h in range(2)], axis=1
            )
            spectrum = dot3((into_hi[...], into_lo[...]), split(rows), 1, 0)
            square = square_col[...] + (square_row[...] + sz)
            safe = jnp.where(square > 0, square, 1.0)
            kernel = factor_col[...] * (factor_row[...] * fz) / safe
            kernel = jnp.where(square > 0, kernel, 0.0)
            scaled = kernel * spectrum
            total = total + jnp.sum(scaled * spectrum, axis=0, keepdims=True)
            out = dot3((back_hi[...], back_lo[...]), split(scaled), 1, 0)
            for h in range(2):
                rows = pl.ds(f + h * 8 * KX, KX, stride=8)
                work[rows, :] = out[:, 128 * h : 128 * h + 128]
        return total

    total = lax.fori_loop(0, 4, along_x, jnp.zeros((1, KY), jnp.float32))
    part[...] = jnp.broadcast_to(0.5 * jnp.sum(total, axis=1, keepdims=True), (1, 128))
    sums[me] = part[...]

    for s in range(slabs):
        rows = jnp.concatenate([work[slab_lines(s, h), :] for h in range(2)], axis=1)
        out = dot3(split(rows), cas, 1, 0)
        lines = 8 * sizes[s]
        own = pl.ds(starts[s], sizes[s])
        for g in range(grp):
            for h in range(half):
                parts = []
                for k in range(fan):
                    start = (g * fan + k) * lines
                    parts.append(out[start : start + lines, 128 * h : 128 * h + 128])
                for k, tile in enumerate(regroup(parts, block_y)):
                    send_back[g * pen + h * fan + k, own] = tile.reshape(sizes[s], 8, 128)
        recv_back[me, own] = send_back[me, own]
        if s == 0:
            fan_out(back_copy(s)[0])
    fan_out(sum_copy()[0])

    def home(s):
        if s + 1 < slabs:
            fan_out(back_copy(s + 1)[0], back_copy(s)[0])
        back_copy(s)[1].wait_recv()

        def home_z(i, inner):
            tile = starts[s] + 2 * i
            rows = jnp.concatenate(
                [recv_back[:, tile + t].reshape(KZ, 128) for t in range(2)], axis=1
            )
            out = dot3(split(jnp.transpose(rows)), cas, 1, 0)
            where = pl.ds(tile * fan, 2 * fan)
            ext[where, pl.ds(0, block_y), :] = out.reshape(2 * fan, block_y, KZ)
            return inner

        lax.fori_loop(0, sizes[s] // 2, home_z, 0)
        side_halo(s).start()

    def join_halo(s):
        side_halo(s).wait_recv()
        ext[slab_rows(s), pl.ds(block_y, 8), :] = halo_side[slab_rows(s)]

    home(0)
    for copy in edge_halos():
        copy.start()
    needed = [max((start * fan - 5) // 2, 0) for start in starts]
    early = [0] + [min(needed[s], 3) for s in range(1, slabs)]
    early[-1] = min(needed[-1], 5)

    def interp_step(a, carry):
        for s in range(1, slabs):

            @pl.when(a == needed[s] - early[s])
            def _(s=s):
                home(s)

        for s in range(slabs):

            @pl.when(a == needed[s])
            def _(s=s):
                join_halo(s)

        @pl.when(a == tile_rows - 3)
        def _():
            for copy in edge_halos():
                copy.wait_recv()
            ext[pl.ds(block_x, 5), pl.ds(0, block_y), :] = halo_up[...]
            ext[pl.ds(block_x, 5), pl.ds(block_y, 8), :] = halo_corner[...]

        interp_row(a, per_row, cell_ref, q_ref, plain, slope, ext, out_ref)
        return carry

    lax.fori_loop(0, tile_rows, interp_step, 0)
    sum_copy()[1].wait_recv()
    energy_ref[...] = jnp.sum(sums[...], axis=0)
    sum_copy()[1].wait_send()

    for s in range(slabs):
        out_copy(s)[1].wait_send()
        if s + 1 == slabs:
            fan_out(None, back_copy(s)[0])
        side_rim(s).wait_send()
        side_halo(s).wait_send()
    for copy in edge_rims() + edge_halos():
        copy.wait_send()


def whole_program(offsets, zcell, fracs, live_q, slots, grp, pen, sizes):
    count = grp * pen
    groups, width = offsets.shape[1:]
    block_x, block_y = KX // grp, KY // pen
    fan = 128 // block_y
    slabs = len(sizes)
    cas = cas_table(KZ)
    cells = np.arange(KX).reshape(grp, block_x // fan, fan)
    order = np.concatenate(
        [
            cells[:, sum(sizes[:s]) : sum(sizes[: s + 1])].transpose(0, 2, 1).reshape(-1)
            for s in range(slabs)
        ]
    )
    factor, square = spline_factor(KX)
    tables = [*halves(cas), *halves(cas[:, order]), *halves(cas[order, :])]
    tables += [factor[None, :], factor[:, None], square[None, :], square[:, None]]
    tables = [jnp.asarray(table) for table in tables]
    vmem = pl.BlockSpec(memory_space=pltpu.VMEM)

    def held(*shape):
        return pltpu.VMEM(shape, jnp.float32)

    traffic = held(count, block_x // fan, 8, 128)
    dma = pltpu.SemaphoreType.DMA
    forces, energy = pl.pallas_call(
        functools.partial(whole_kernel, grp, pen, slots, sizes),
        out_shape=[
            jax.ShapeDtypeStruct((3, groups * width), jnp.float32),
            jax.ShapeDtypeStruct((1, 128), jnp.float32),
        ],
        in_specs=[vmem] * (4 + len(tables)),
        out_specs=[vmem] * 2,
        scratch_shapes=[
            held(block_x + 8, block_y + 8, KZ),
            held(block_x + 8, block_y + 8, KZ),
            *weight_scratch(groups, width),
            *weight_scratch(groups, width),
            traffic, traffic, traffic, traffic,
            held(16 * KX, 128),
            held(count, 1, 128),
            held(1, 128),
            held(block_x, 8, KZ), held(5, block_y, KZ), held(5, 8, KZ),
            held(block_x, 8, KZ), held(5, block_y, KZ), held(5, 8, KZ),
            dma((slabs,)), dma((slabs,)), dma((count,)), dma((slabs,)),
            dma((1,)), dma((1,)),
            dma((slabs,)), dma((slabs,)), dma((slabs,)), dma((slabs,)),
            dma((4,)), dma((4,)),
        ],
        compiler_params=pltpu.CompilerParams(
            collective_id=1, has_side_effects=True, vmem_limit_bytes=60 * 1024 * 1024
        ),
        name="whole",
    )(offsets, zcell, fracs, live_q, *tables)
    return (forces, energy[0, 0])


def slab_fits(grp, pen, sizes, block_x, block_y, per_row):
    fan = 128 // block_y
    return (
        grp * pen * 8 == KZ and KX == KY and KY == KZ and KZ == 256 and pen % fan == 0
        and block_x == fan * sum(sizes) and per_row * 8 == block_y and 8 % per_row == 0
    )


def local(cell_offsets, cell_z, frac, charges, tile_counts):
    block_x = KX // lax.axis_size("grp")
    block_y = KY // lax.axis_size("pen")
    tiles = tile_counts.shape[0]
    slots = charges.shape[0] // tiles
    width = 4 * slots
    groups = tiles // 4
    per_row = block_y // 8
    live = jnp.arange(slots, dtype=jnp.int32)[None, :] < tile_counts[:, None]
    live_q = (charges.reshape(tiles, slots) * live.astype(jnp.float32)).reshape(groups, width)
    offsets = cell_offsets.reshape(2, groups, width)
    zcell = cell_z.reshape(groups, width)
    fracs = frac.reshape(3, groups, width)
    grp, pen = lax.axis_size("grp"), lax.axis_size("pen")
    sizes = (6, 4, 4, 2)
    if slab_fits(grp, pen, sizes, block_x, block_y, per_row) and 128 % slots == 0:
        flat = tile_counts.reshape(-1, 128 // slots, 1)
        alive = jnp.arange(slots, dtype=jnp.int32) < flat
        live_q = charges.reshape(-1, 128) * alive.reshape(-1, 128).astype(jnp.float32)
        zcell = cell_z.reshape(-1, 128)
        forces, total = whole_program(offsets, zcell, fracs, live_q, slots, grp, pen, sizes)
        return (forces, total / ATOMS)
    vmem = pl.BlockSpec(memory_space=pltpu.VMEM)
    params = pltpu.CompilerParams(vmem_limit_bytes=60 * 1024 * 1024)
    padded = pl.pallas_call(
        functools.partial(spread_kernel, per_row, slots),
        out_shape=jax.ShapeDtypeStruct((block_x + 8, block_y + 8, KZ), jnp.float32),
        in_specs=[vmem] * 4,
        out_specs=vmem,
        scratch_shapes=weight_scratch(groups, width),
        compiler_params=params,
        name="spread",
    )(offsets, zcell, fracs, live_q)
    rim_y = shifted(padded[: block_x + 5, block_y : block_y + 5], "pen", 1)
    merged = padded[: block_x + 5, :block_y].at[:, :5].add(rim_y)
    rim_x = shifted(merged[block_x : block_x + 5], "grp", 1)
    grid = merged[:block_x] + jnp.pad(rim_x, ((0, block_x - 5), (0, 0), (0, 0)))
    potential, total = spectrum_of(grid, block_x, block_y)
    upper = shifted(potential[:5], "grp", -1)
    ext_x = jnp.concatenate([potential[:, :5], upper[:, :5]], axis=0)
    beside = shifted(ext_x, "pen", -1)
    beside = jnp.pad(beside, ((0, 0), (0, 3), (0, 0)))
    forces = pl.pallas_call(
        functools.partial(interp_kernel, per_row, slots),
        out_shape=jax.ShapeDtypeStruct((3, groups * width), jnp.float32),
        in_specs=[vmem] * 7,
        out_specs=vmem,
        scratch_shapes=[pltpu.VMEM((block_x + 8, block_y + 8, KZ), jnp.float32)]
        + 2 * weight_scratch(groups, width),
        compiler_params=params,
        name="interp",
    )(offsets, zcell, fracs, live_q, potential, upper, beside)
    return (forces, total / ATOMS)


def solution(mesh):
    in_specs = (
        P(None, ("grp", "pen")),
        P(("grp", "pen")),
        P(None, ("grp", "pen")),
        P(("grp", "pen")),
        P(("grp", "pen")),
    )
    out_specs = (P(None, ("grp", "pen")), P())
    return jax.shard_map(local, mesh=mesh, in_specs=in_specs, out_specs=out_specs, check_vma=False)
```
